32 devices in a mesh: dp: 32 (over z, y, x, core).
Axes of the slice: x: 2, y: 2, z: 4, core: 2. Of those that a mesh axis runs over, the one named last changes fastest.
Arguments:
- tokens: bfloat16 [4096, 2048], P('dp'), may hold values from -6 to 6
- seq_lengths: int32 [32, 2, 4], P('dp'), may hold values from 0 to 64, as said below
- attn_gain: bfloat16 [2048], P('dp'), may hold values from 0.5 to 1.5
- attn_shift: bfloat16 [2048], P('dp'), may hold values from -1 to 1
- query_weight: bfloat16 [2048, 2048], P('dp'), may hold values from -0.125 to 0.125
- key_weight: bfloat16 [2048, 2048], P('dp'), may hold values from -0.125 to 0.125
- value_weight: bfloat16 [2048, 4096], P('dp'), may hold values from -0.125 to 0.125
- gate_weight: bfloat16 [2048, 4096], P('dp'), may hold values from -0.125 to 0.125
- out_weight: bfloat16 [4096, 2048], P('dp'), may hold values from -0.09375 to 0.09375
- mlp_gain: bfloat16 [2048], P('dp'), may hold values from 0.5 to 1.5
- mlp_shift: bfloat16 [2048], P('dp'), may hold values from -1 to 1
- mlp_gate: bfloat16 [2048, 4096], P('dp'), may hold values from -0.125 to 0.125
- mlp_up: bfloat16 [2048, 4096], P('dp'), may hold values from -0.125 to 0.125
- mlp_down: bfloat16 [4096, 2048], P('dp'), may hold values from -0.09375 to 0.09375
- cotangent: bfloat16 [4096, 2048], P('dp'), may hold values from -6 to 6
Outputs:
- output: bfloat16 [4096, 2048], P('dp')
- tokens_grad: float32 [4096, 2048], P('dp')
- attn_gain_grad: float32 [2048], P('dp')
- attn_shift_grad: float32 [2048], P('dp')
- query_weight_grad: float32 [2048, 2048], P('dp')
- key_weight_grad: float32 [2048, 2048], P('dp')
- value_weight_grad: float32 [2048, 4096], P('dp')
- gate_weight_grad: float32 [2048, 4096], P('dp')
- out_weight_grad: float32 [4096, 2048], P('dp')
- mlp_gain_grad: float32 [2048], P('dp')
- mlp_shift_grad: float32 [2048], P('dp')
- mlp_gate_grad: float32 [2048, 4096], P('dp')
- mlp_up_grad: float32 [2048, 4096], P('dp')
- mlp_down_grad: float32 [4096, 2048], P('dp')
The draws below stay inside these ranges and needn't reach their ends.
Inputs may be any that keep to these rules, and one draw needn't show every extreme that they name: seq_lengths[d, m, :] lists the lengths of the sequences placed in micro-batch m of device d, packed from its first row in this order; 0 marks an unused slot; the lengths of one micro-batch add up to between 32 and 64; in every draw some micro-batch holds a single sequence of 64 tokens.
All inputs are finite; a program needn't handle non-finite values.
Results may differ from the reference program's by a relative error of at most 0.015.
Values may be sent and summed in bfloat16 or wider, within the bound.
A program may use at most 512 MiB of HBM per device.

```python
from functools import partial
import jax
import jax.numpy as jnp
from jax import lax

D = 2048
HEADS = 8
FF = 4096
MICRO = 2
MB_TOK = 64
SEQS = 4
QK = 2048
V = 4096
TOKENS = 4096
N_DP = 32


def draw_seq_lengths(key, part):
    fill_key, cut_key, pick_key = jax.random.split(key, 3)
    fill_rows = jax.random.randint(fill_key, (N_DP, MICRO, 1), MB_TOK // 2, MB_TOK + 1).astype(jnp.int32)
    raw_cuts = jax.random.randint(cut_key, (N_DP, MICRO, SEQS - 1), 0, 1048576).astype(jnp.int32)
    cut_points = jnp.sort(raw_cuts * (fill_rows + 1) // 1048576, axis=-1)
    zeros_col = jnp.zeros((N_DP, MICRO, 1), jnp.int32)
    boundaries = jnp.concatenate([zeros_col, cut_points, fill_rows], axis=-1)
    seq_sizes = boundaries[..., 1:] - boundaries[..., :-1]
    chosen = jax.random.randint(pick_key, (), 0, N_DP)
    whole_row = jnp.zeros((SEQS,), jnp.int32).at[0].set(MB_TOK)
    device_ids = jnp.arange(N_DP)[:, None, None]
    micro_ids = jnp.arange(MICRO)[None, :, None]
    special = (device_ids == chosen) & (micro_ids == 0)
    return jnp.where(special, whole_row[None, None, :], seq_sizes).astype(jnp.int32)


def steps_of(key, dims, cuts, low, largest):
    def one(axis_at, shards_of):
        heights = jax.random.uniform(jax.random.fold_in(jax.random.fold_in(key, 6), axis_at), (shards_of,), jnp.float32, low / len(cuts), largest / len(cuts))
        return jnp.repeat(jnp.exp(heights), dims[axis_at] // shards_of).reshape((-1,) + (1,) * (len(dims) - axis_at - 1))

    gain = one(*cuts[0])
    for cut in cuts[1:]:
        gain = gain * one(*cut)
    return gain


def noise(stream_key, dims, deviation, reach, cuts=(), kind=jnp.bfloat16):
    entries = jax.random.normal(stream_key, dims, jnp.float32) * deviation
    if len(cuts) > 0:
        entries = steps_of(stream_key, dims, cuts, -0.22, 0.18) * entries
    return jnp.clip(entries, min=-reach, max=reach).astype(kind)


def setup_inputs(seed: int = 0) -> dict:
    streams_of = jax.random.split(jax.random.key(seed), 16)
    tokens = noise(streams_of[0], (TOKENS, D), 1.0, 6.0, ((0, 32),))
    seq_lengths = draw_seq_lengths(jax.random.fold_in(streams_of[15], 71), 0)
    attn_gain = jnp.clip(1.0 + 0.1 * jax.random.normal(streams_of[2], (D,), jnp.float32), 0.5, 1.5).astype(jnp.bfloat16)
    attn_shift = noise(streams_of[3], (D,), 0.2, 1.0, ((0, 32),))
    query_weight = noise(streams_of[4], (D, QK), D ** -0.5, 0.125, ((0, 32),))
    key_weight = noise(streams_of[5], (D, QK), D ** -0.5, 0.125, ((0, 32),))
    value_weight = noise(streams_of[6], (D, V), D ** -0.5, 0.125, ((0, 32),))
    gate_weight = noise(streams_of[7], (D, V), D ** -0.5, 0.125, ((0, 32),))
    out_weight = noise(streams_of[8], (V, D), V ** -0.5, 0.09375, ((0, 32),))
    mlp_gain = jnp.clip(1.0 + 0.1 * jax.random.normal(streams_of[9], (D,), jnp.float32), 0.5, 1.5).astype(jnp.bfloat16)
    mlp_shift = noise(streams_of[10], (D,), 0.2, 1.0, ((0, 32),))
    mlp_gate = noise(streams_of[11], (D, FF), D ** -0.5, 0.125, ((0, 32),))
    mlp_up = noise(streams_of[12], (D, FF), D ** -0.5, 0.125, ((0, 32),))
    mlp_down = noise(streams_of[13], (FF, D), FF ** -0.5, 0.09375, ((0, 32),))
    cotangent = noise(streams_of[14], (TOKENS, D), 1.0, 6.0, ((0, 32),))
    return dict(tokens=tokens, seq_lengths=seq_lengths, attn_gain=attn_gain, attn_shift=attn_shift, query_weight=query_weight, key_weight=key_weight, value_weight=value_weight, gate_weight=gate_weight, out_weight=out_weight, mlp_gain=mlp_gain, mlp_shift=mlp_shift, mlp_gate=mlp_gate, mlp_up=mlp_up, mlp_down=mlp_down, cotangent=cotangent)


NORM_EPS = 1e-05
GROUP_EPS = 1.0

@jax.custom_vjp
def low(v):
    return lax.optimization_barrier(v.astype(jnp.bfloat16)).astype(jnp.float32)

@jax.custom_vjp
def low_back(v):
    return v

def low_keep(v):
    return (low(v), None)

def low_pass(kept, grad):
    return (grad,)

def back_keep(v):
    return (v, None)

def back_low(kept, grad):
    return (low(grad),)
low.defvjp(low_keep, low_pass)
low_back.defvjp(back_keep, back_low)

def matmul(left_side, right_side):
    return jnp.dot(left_side, right_side, precision=lax.Precision.HIGHEST, preferred_element_type=jnp.float32)

def seq_layout(seq_lens, row_count):
    row_ids = jnp.arange(row_count, dtype=jnp.int32)
    seq_ends = jnp.cumsum(seq_lens).astype(jnp.int32)
    passed = row_ids[:, None] >= seq_ends[None, :]
    segment = lax.optimization_barrier(jnp.sum(passed.astype(jnp.int32), axis=1)).astype(jnp.int32)
    seq_start = lax.optimization_barrier(jnp.sum(jnp.where(passed, seq_lens[None, :], 0), axis=1)).astype(jnp.int32)
    position = (row_ids - seq_start).astype(jnp.int32)
    live_rows = row_ids < seq_ends[-1]
    return (row_ids, segment, position, live_rows)

def decay_table(row_ids, segment, position, live_rows, head_count):
    same_seq = (segment[:, None] == segment[None, :]) & live_rows[:, None] & live_rows[None, :] & (row_ids[:, None] >= row_ids[None, :])
    distance = jnp.maximum(position[:, None] - position[None, :], 0).astype(jnp.float32)
    log_decay = jnp.log(1.0 - 2.0 ** (-5.0 - jnp.arange(head_count, dtype=jnp.float32)))
    return jnp.where(same_seq[None], jnp.exp(distance[None] * log_decay[:, None, None]), 0.0)

def rotary(position, key_size):
    half_size = key_size // 2
    pair_index = jnp.arange(half_size, dtype=jnp.float32)
    frequency = 10000.0 ** (-pair_index / half_size)
    row_place = position.astype(jnp.float32)[:, None]
    angles = row_place * frequency[None, :]
    growth = (pair_index * 2.0 / key_size + 0.4) / 1.4
    stretch = growth[None, :] ** (row_place / 512.0)
    return (jnp.cos(angles), jnp.sin(angles), stretch)

def rotate_pairs(values, cosine_table, sine_table, factor):
    half_size = values.shape[-1] // 2
    first_half = values[..., :half_size]
    second_half = values[..., half_size:]
    cosine_heads = cosine_table[:, None, :]
    sine_heads = sine_table[:, None, :]
    factor_heads = factor[:, None, :]
    return jnp.concatenate([(first_half * cosine_heads - second_half * sine_heads) * factor_heads, (second_half * cosine_heads + first_half * sine_heads) * factor_heads], axis=-1)

def layer_norm(values, gain_vec, shift_vec):
    center = values - lax.optimization_barrier(jnp.mean(values, axis=-1, keepdims=True))
    spread = lax.optimization_barrier(jnp.mean(center * center, axis=-1, keepdims=True))
    return center * lax.rsqrt(spread + NORM_EPS) * gain_vec + shift_vec

def group_norm(values, head_count):
    heads_view = values.reshape(values.shape[0], head_count, -1)
    center = heads_view - lax.optimization_barrier(jnp.mean(heads_view, axis=-1, keepdims=True))
    spread = lax.optimization_barrier(jnp.mean(center * center, axis=-1, keepdims=True))
    return (center * lax.rsqrt(spread + GROUP_EPS)).reshape(values.shape)

def forward(seq_table, x_input, attn_gain, attn_shift, query_weight, key_weight, value_weight, gate_weight, out_weight, mlp_gain, mlp_shift, mlp_gate, mlp_up, mlp_down):
    block_count = seq_table.shape[0]
    total_rows = x_input.shape[0]
    row_count = total_rows // block_count
    key_size = query_weight.shape[1] // HEADS
    value_size = value_weight.shape[1] // HEADS
    normed_one = low(layer_norm(x_input, attn_gain, attn_shift))
    query_raw = low_back(matmul(normed_one, query_weight))
    key_raw = low_back(matmul(normed_one, key_weight))
    value_both = low(low_back(matmul(normed_one, value_weight)))
    gate_raw = low_back(matmul(normed_one, gate_weight))

    def block_step(pieces):
        query_block, key_block, value_block, seq_lens = pieces
        row_ids, segment, position, live_rows = seq_layout(seq_lens, row_count)
        cosine_table, sine_table, stretch = rotary(position, key_size)
        query_turned = low(rotate_pairs(query_block, cosine_table, sine_table, stretch))
        key_turned = low(rotate_pairs(key_block, cosine_table, sine_table, key_size ** (-0.5) / stretch))
        scores = low_back(jnp.einsum('qhd,khd->hqk', query_turned, key_turned, precision=lax.Precision.HIGHEST))
        decay_mask = decay_table(row_ids, segment, position, live_rows, HEADS)
        weights_low = low(scores * decay_mask)
        return jnp.einsum('hqk,khe->qhe', weights_low, value_block, precision=lax.Precision.HIGHEST)
    retained = lax.map(jax.checkpoint(block_step), (query_raw.reshape(block_count, row_count, HEADS, key_size), key_raw.reshape(block_count, row_count, HEADS, key_size), value_both.reshape(block_count, row_count, HEADS, value_size), seq_table))
    retained = low_back(retained.reshape(total_rows, HEADS * value_size))
    mixed = low(jax.nn.silu(gate_raw) * group_norm(retained, HEADS))
    branch_one = low_back(matmul(mixed, out_weight))
    hidden = x_input + branch_one
    normed_two = low(layer_norm(hidden, mlp_gain, mlp_shift))
    up_gate = low_back(matmul(normed_two, mlp_gate))
    up_lin = low_back(matmul(normed_two, mlp_up))
    product = low(jax.nn.gelu(up_gate, approximate=True) * up_lin)
    branch_two = low_back(matmul(product, mlp_down))
    live_all = jax.vmap(lambda seq_lens: seq_layout(seq_lens, row_count)[3])(seq_table).reshape(total_rows)
    return (hidden + branch_two) * live_all.astype(jnp.float32)[:, None]

def reference(tokens, seq_lengths, attn_gain, attn_shift, query_weight, key_weight, value_weight, gate_weight, out_weight, mlp_gain, mlp_shift, mlp_gate, mlp_up, mlp_down, cotangent):
    seq_table = seq_lengths.reshape(-1, seq_lengths.shape[-1]).astype(jnp.int32)
    primals = (tokens.astype(jnp.float32), attn_gain.astype(jnp.float32), attn_shift.astype(jnp.float32), query_weight.astype(jnp.float32), key_weight.astype(jnp.float32), value_weight.astype(jnp.float32), gate_weight.astype(jnp.float32), out_weight.astype(jnp.float32), mlp_gain.astype(jnp.float32), mlp_shift.astype(jnp.float32), mlp_gate.astype(jnp.float32), mlp_up.astype(jnp.float32), mlp_down.astype(jnp.float32))
    output, pull_back = jax.vjp(partial(forward, seq_table), *primals)
    grads = pull_back(cotangent.astype(jnp.float32))
    return (output.astype(jnp.bfloat16), grads[0], grads[1], grads[2], grads[3], grads[4], grads[5], grads[6], grads[7], grads[8], grads[9], grads[10], grads[11], grads[12])
```

```python
import jax
import jax.numpy as jnp
from jax import lax
from jax.sharding import PartitionSpec as P

HEADS = 8
NORM_EPS = 1e-05
GROUP_EPS = 1.0
BF = jnp.bfloat16
F32 = jnp.float32


def xor_axis(values, axis, own):
    shape = values.shape
    size = shape[axis]
    bit = 1
    while bit < size:
        parts = values.reshape(shape[:axis] + (size // (2 * bit), 2, bit) + shape[axis + 1 :])
        parts = jnp.where((own & bit) != 0, jnp.flip(parts, axis + 1), parts)
        values = parts.reshape(shape)
        bit *= 2
    return values


def seq_layout(seq_lens, row_count):
    row_ids = jnp.arange(row_count, dtype=jnp.int32)
    seq_ends = jnp.cumsum(seq_lens)
    passed = row_ids[:, None] >= seq_ends[None, :]
    segment = jnp.sum(passed.astype(jnp.int32), axis=1)
    seq_start = jnp.sum(jnp.where(passed, seq_lens[None, :], 0), axis=1)
    position = row_ids - seq_start
    live_rows = row_ids < seq_ends[-1]
    return (segment, position, live_rows)


def layer_norm(values, gain_vec, shift_vec):
    center = values - jnp.mean(values, axis=-1, keepdims=True)
    spread = jnp.mean(center * center, axis=-1, keepdims=True)
    return center * lax.rsqrt(spread + NORM_EPS) * gain_vec + shift_vec


def group_norm(values):
    center = values - jnp.mean(values, axis=-1, keepdims=True)
    spread = jnp.mean(center * center, axis=-1, keepdims=True)
    return center * lax.rsqrt(spread + GROUP_EPS)


def dot(left, right):
    return jnp.dot(left, right, preferred_element_type=F32)


def dot_nt(left, right):
    return lax.dot_general(left, right, (((1,), (1,)), ((), ())), preferred_element_type=F32)


def dot_tn(left, right):
    return lax.dot_general(left, right, (((0,), (0,)), ((), ())), preferred_element_type=F32)


def make_body(count):
    reps = count // 8
    hi_count = count // 16

    def flip_bit(values, bit):
        return lax.ppermute(values, "dp", [(i, i ^ (1 << bit)) for i in range(count)])

    def rep_bit(rel):
        low = 0
        while not (rel >> low) & 1:
            low += 1
        return low, (2 if low == 0 else 3 + low)

    groups = [
        [(r >> 1) * 16 + (t >> 2) * 8 + (r & 1) * 4 + (t & 3) for t in range(8)]
        for r in range(reps)
    ]
    head_perm = [(d, groups[d % reps][d // reps]) for d in range(count)]
    head_back = [(b, a) for a, b in head_perm]

    def gather_reps(block):
        blocks = [block]
        for rel in range(1, reps):
            low, bit = rep_bit(rel)
            blocks.append(flip_bit(blocks[rel & ~(1 << low)], bit))
        return blocks

    def scatter_reps(parts):
        parts = list(parts)
        for rel in range(reps - 1, 0, -1):
            low, bit = rep_bit(rel)
            got = flip_bit(parts[rel].astype(BF), bit)
            parts[rel & ~(1 << low)] = parts[rel & ~(1 << low)] + got.astype(F32)
        return parts[0]

    def gather_rows(block):
        half = block.shape[0] // 2
        a0, b0 = block[:half], block[half:]
        ax, bx, az, bz = flip_bit(a0, 1), flip_bit(b0, 1), flip_bit(a0, 3), flip_bit(b0, 3)
        axz, bxz = flip_bit(ax, 3), flip_bit(bz, 1)
        own_c = flip_bit(block, 0)
        first = jnp.concatenate([ax, bx, az, bz], axis=0)
        first_c = flip_bit(first, 0)
        last = jnp.concatenate([axz, bxz], axis=0)
        last_c = flip_bit(last, 0)
        return jnp.concatenate([block, first, last, own_c, first_c, last_c], axis=0)

    def scatter_rows(parts):
        rows = parts.shape[0]
        half = rows // 16
        even, odd = parts[: rows // 2], parts[rows // 2 :].astype(BF)
        cut = 6 * half
        got_last = flip_bit(odd[cut:], 0)
        got_first = flip_bit(odd[:cut], 0)
        last = even[cut:] + got_last.astype(F32)
        axz, bxz = last[:half], last[half:]
        first = even[:cut] + got_first.astype(F32)
        a0, b0, ax, bx, az, bz = (first[i * half : (i + 1) * half] for i in range(6))
        ax = ax + flip_bit(axz.astype(BF), 3).astype(F32)
        bz = bz + flip_bit(bxz.astype(BF), 1).astype(F32)
        a0 = a0 + flip_bit(az.astype(BF), 3).astype(F32)
        b0 = b0 + flip_bit(bx.astype(BF), 1).astype(F32)
        a0 = a0 + flip_bit(ax.astype(BF), 1).astype(F32)
        b0 = b0 + flip_bit(bz.astype(BF), 3).astype(F32)
        return jnp.concatenate([a0, b0], axis=0)

    def to_group(values):
        return lax.all_to_all(
            values, "dp", split_axis=0, concat_axis=0, axis_index_groups=groups, tiled=True
        )

    def on_device(
        tokens,
        seq_lengths,
        attn_gain,
        attn_shift,
        query_weight,
        key_weight,
        value_weight,
        gate_weight,
        out_weight,
        mlp_gain,
        mlp_shift,
        mlp_gate,
        mlp_up,
        mlp_down,
        cotangent,
    ):
        device = lax.axis_index("dp")
        rep = (device >> 4) * 2 + ((device >> 2) & 1)
        pos_t = ((device >> 3) & 1) * 4 + (device & 3)
        local_rows, width = tokens.shape
        micro_count, seq_slots = seq_lengths.shape[1:]
        row_count = local_rows // micro_count
        shard = width // count
        key_size = query_weight.shape[1] // HEADS
        value_size = value_weight.shape[1] // HEADS
        hidden_size = mlp_gate.shape[1]
        ff_block = hidden_size // count
        group_rows = 8 * local_rows

        def features_to_rel(values):
            v = values.reshape(local_rows, hi_count, 2, 2, 4 * shard)
            v = v.transpose(0, 1, 3, 2, 4).reshape(local_rows, reps, 8 * shard)
            return xor_axis(v, 1, rep).reshape(local_rows, width)

        def features_from_rel(values):
            v = xor_axis(values.reshape(local_rows, reps, 8 * shard), 1, rep)
            v = v.reshape(local_rows, hi_count, 2, 2, 4 * shard).transpose(0, 1, 3, 2, 4)
            return v.reshape(local_rows, width)

        def heads_first(weight):
            return weight.reshape(shard, HEADS, -1).transpose(1, 0, 2)

        def ff_first(weight):
            v = weight.reshape(shard, hi_count, 2, 2, 4, ff_block)
            return v.transpose(2, 4, 0, 1, 3, 5).reshape(8, shard, reps * ff_block)

        def ff_back(grad):
            v = grad.reshape(2, 4, shard, hi_count, 2, ff_block)
            return v.transpose(2, 3, 0, 4, 1, 5).reshape(shard, hidden_size)

        def heads_back(grad):
            return grad.transpose(1, 0, 2).reshape(shard, -1)

        small = jnp.concatenate(
            [attn_gain, attn_shift, mlp_gain, mlp_shift, seq_lengths.reshape(-1).astype(BF)]
        )
        small = lax.all_gather(small, "dp", axis=0, tiled=False)
        gain_one, shift_one, gain_two, shift_two = (
            small[:, i * shard : (i + 1) * shard].reshape(-1).astype(F32) for i in range(4)
        )
        lens = small[:, 4 * shard :].astype(jnp.int32).reshape(hi_count, 2, 2, 4, -1)
        lens = lens.transpose(0, 2, 1, 3, 4).reshape(reps, 8, -1)
        lens = lax.dynamic_index_in_dim(lens, rep, 0, keepdims=False)
        lens = xor_axis(lens, 0, pos_t).reshape(4, 2, micro_count, seq_slots)
        lens = lens.transpose(1, 0, 2, 3).reshape(8 * micro_count, seq_slots)

        attn_cols = to_group(
            jnp.concatenate(
                [
                    heads_first(query_weight),
                    heads_first(key_weight),
                    heads_first(value_weight),
                    heads_first(gate_weight),
                ],
                axis=2,
            )
        ).reshape(8 * shard, -1)
        attn_blocks = gather_reps(attn_cols)
        out_own = lax.ppermute(out_weight, "dp", head_perm)
        out_blocks = gather_reps(out_own)
        mlp_cols = to_group(
            jnp.concatenate([ff_first(mlp_gate), ff_first(mlp_up)], axis=2)
        ).reshape(8 * shard, -1)
        mlp_blocks = gather_reps(mlp_cols)
        down_blocks = gather_reps(mlp_down)

        def natural_rows(blocks):
            stacked = xor_axis(jnp.stack(blocks), 0, rep)
            return stacked.reshape(-1, stacked.shape[-1])

        def feature_dot(values, blocks):
            size = values.shape[1] // reps
            total = None
            for j, block in enumerate(blocks):
                term = dot(values[:, j * size : (j + 1) * size], block)
                total = term if total is None else total + term
            return total

        def feature_dot_back(grads, blocks):
            return jnp.concatenate([dot_nt(grads, block) for block in blocks], axis=1)

        def weight_grad_parts(values, grads):
            size = values.shape[1] // reps
            return [
                dot_tn(values[:, j * size : (j + 1) * size], grads) for j in range(reps)
            ]

        segment, position, live = jax.vmap(lambda s: seq_layout(s, row_count))(lens)
        head_log = jnp.log(1.0 - 2.0 ** (-5.0 - jnp.arange(HEADS, dtype=F32)))
        head_log = lax.dynamic_index_in_dim(head_log, pos_t, 0, keepdims=False)
        ids = jnp.arange(row_count, dtype=jnp.int32)
        same_seq = (
            (segment[:, :, None] == segment[:, None, :])
            & live[:, :, None]
            & live[:, None, :]
            & (ids[:, None] >= ids[None, :])[None]
        )
        distance = jnp.maximum(position[:, :, None] - position[:, None, :], 0).astype(F32)
        decay = jnp.where(same_seq, jnp.exp(distance * head_log), 0.0)
        half_size = key_size // 2
        pair_index = jnp.arange(half_size, dtype=F32)
        frequency = 10000.0 ** (-pair_index / half_size)
        row_place = position.reshape(-1).astype(F32)[:, None]
        angles = row_place * frequency[None, :]
        growth = (pair_index * 2.0 / key_size + 0.4) / 1.4
        stretch = growth[None, :] ** (row_place / 512.0)
        cosine, sine = jnp.cos(angles), jnp.sin(angles)
        key_factor = key_size ** (-0.5) / stretch

        def rotate(values, factor):
            a, b = values[:, :half_size], values[:, half_size:]
            return jnp.concatenate(
                [(a * cosine - b * sine) * factor, (b * cosine + a * sine) * factor], axis=1
            )

        def rotate_back(grads, factor):
            a, b = grads[:, :half_size] * factor, grads[:, half_size:] * factor
            return jnp.concatenate([a * cosine + b * sine, b * cosine - a * sine], axis=1)

        def micro(values):
            return values.reshape(-1, row_count, values.shape[-1])

        x_local = tokens.astype(F32)
        normed_one_local = layer_norm(x_local, gain_one, shift_one).astype(BF)
        normed_one = gather_rows(features_to_rel(normed_one_local))
        own_live = live.reshape(8, local_rows)[0].astype(F32)[:, None]
        out_grad = cotangent.astype(F32) * own_live
        cot_all = gather_rows(out_grad.astype(BF))

        qkvg = feature_dot(normed_one, attn_blocks)
        query_raw = qkvg[:, :key_size]
        key_raw = qkvg[:, key_size : 2 * key_size]
        value_low = qkvg[:, 2 * key_size : 2 * key_size + value_size].astype(BF)
        gate_raw = qkvg[:, 2 * key_size + value_size :]
        query_turned = micro(rotate(query_raw, stretch).astype(BF))
        key_turned = micro(rotate(key_raw, key_factor).astype(BF))
        value_m = micro(value_low)
        scores = jnp.einsum("mqd,mkd->mqk", query_turned, key_turned, preferred_element_type=F32)
        weights_low = (scores * decay).astype(BF)
        retained = jnp.einsum("mqk,mke->mqe", weights_low, value_m, preferred_element_type=F32)
        retained = retained.reshape(group_rows, value_size)

        def mix(gate_in, retained_in):
            return jax.nn.silu(gate_in) * group_norm(retained_in)

        mixed = mix(gate_raw, retained).astype(BF)
        out_full = natural_rows(out_blocks)
        branch_one = scatter_rows(dot(mixed, out_full))
        hidden = x_local + branch_one
        normed_two_local = layer_norm(hidden, gain_two, shift_two).astype(BF)
        normed_two = gather_rows(features_to_rel(normed_two_local))

        ups = feature_dot(normed_two, mlp_blocks)
        up_gate, up_lin = ups[:, : ups.shape[1] // 2], ups[:, ups.shape[1] // 2 :]

        def act(gate_in, up_in):
            return jax.nn.gelu(gate_in, approximate=True) * up_in

        product, pull_act = jax.vjp(act, up_gate, up_lin)
        product = product.astype(BF)
        down_full = natural_rows(down_blocks)
        product_grad = dot_nt(cot_all, down_full)
        gate_up_grad = jnp.concatenate([g.astype(BF) for g in pull_act(product_grad)], axis=1)
        normed_two_grad = features_from_rel(
            scatter_rows(feature_dot_back(gate_up_grad, mlp_blocks))
        )
        _, pull_two = jax.vjp(layer_norm, hidden, gain_two, shift_two)
        hidden_part, mlp_gain_part, mlp_shift_part = pull_two(normed_two_grad)
        hidden_grad = out_grad + hidden_part
        branch_one_grad = gather_rows(hidden_grad.astype(BF))

        def down_parts(values, grads):
            full = dot_tn(values, grads).reshape(reps, -1, grads.shape[1])
            full = xor_axis(full, 0, rep)
            return [full[j] for j in range(reps)]

        mlp_down_grad = scatter_reps(down_parts(product, cot_all))
        mlp_cols_grad = scatter_reps(weight_grad_parts(normed_two, gate_up_grad))
        mlp_cols_grad = to_group(mlp_cols_grad.astype(BF).reshape(8, shard, -1)).astype(F32)
        ff_cols = mlp_cols_grad.shape[2] // 2
        mlp_gate_grad = ff_back(mlp_cols_grad[:, :, :ff_cols])
        mlp_up_grad = ff_back(mlp_cols_grad[:, :, ff_cols:])

        branch_two = scatter_rows(dot(product, down_full))
        output = ((hidden + branch_two) * own_live).astype(BF)

        mixed_grad = dot_nt(branch_one_grad, out_full)
        _, pull_mix = jax.vjp(mix, gate_raw, retained)
        gate_grad, retained_grad = pull_mix(mixed_grad)
        gate_low = gate_grad.astype(BF)
        retained_low = micro(retained_grad.astype(BF))
        weights_grad = jnp.einsum("mqe,mke->mqk", retained_low, value_m, preferred_element_type=F32)
        value_grad = jnp.einsum("mqk,mqe->mke", weights_low, retained_low, preferred_element_type=F32)
        value_grad = value_grad.reshape(group_rows, value_size).astype(BF)
        score_low = (weights_grad * decay).astype(BF)
        query_turn_grad = jnp.einsum("mqk,mkd->mqd", score_low, key_turned, preferred_element_type=F32)
        key_turn_grad = jnp.einsum("mqk,mqd->mkd", score_low, query_turned, preferred_element_type=F32)
        query_low = rotate_back(query_turn_grad.reshape(group_rows, key_size), stretch).astype(BF)
        key_low = rotate_back(key_turn_grad.reshape(group_rows, key_size), key_factor).astype(BF)
        attn_grads = jnp.concatenate([query_low, key_low, value_grad, gate_low], axis=1)
        attn_cols_grad = scatter_reps(weight_grad_parts(normed_one, attn_grads))
        attn_cols_grad = to_group(attn_cols_grad.astype(BF).reshape(8, shard, -1)).astype(F32)
        edges = (0, key_size, 2 * key_size, 2 * key_size + value_size, 2 * (key_size + value_size))
        q_grad, k_grad, v_grad, g_grad = (
            heads_back(attn_cols_grad[:, :, a:b]) for a, b in zip(edges[:-1], edges[1:])
        )
        out_own_grad = scatter_reps(down_parts(mixed, branch_one_grad))
        out_weight_grad = lax.ppermute(out_own_grad.astype(BF), "dp", head_back).astype(F32)

        normed_one_grad = features_from_rel(
            scatter_rows(feature_dot_back(attn_grads, attn_blocks))
        )
        _, pull_one = jax.vjp(layer_norm, x_local, gain_one, shift_one)
        input_part, attn_gain_part, attn_shift_part = pull_one(normed_one_grad)
        tokens_grad = hidden_grad + input_part

        vectors = jnp.stack([attn_gain_part, attn_shift_part, mlp_gain_part, mlp_shift_part])
        vectors = vectors.reshape(4, count, shard).transpose(1, 0, 2).reshape(count, 4 * shard)
        vectors = lax.psum_scatter(vectors, "dp", scatter_dimension=0, tiled=False)
        attn_gain_grad, attn_shift_grad, mlp_gain_grad, mlp_shift_grad = (
            vectors[i * shard : (i + 1) * shard] for i in range(4)
        )
        return (
            output,
            tokens_grad,
            attn_gain_grad,
            attn_shift_grad,
            q_grad,
            k_grad,
            v_grad,
            g_grad,
            out_weight_grad,
            mlp_gain_grad,
            mlp_shift_grad,
            mlp_gate_grad,
            mlp_up_grad,
            mlp_down_grad,
        )

    return on_device


def solution(mesh):
    rows = P("dp", None)
    vec = P("dp")
    placed = (
        rows, P("dp", None, None), vec, vec, rows, rows, rows, rows, rows,
        vec, vec, rows, rows, rows, rows,
    )
    outs = (rows, rows, vec, vec, rows, rows, rows, rows, rows, vec, vec, rows, rows, rows)
    return jax.shard_map(
        make_body(mesh.shape["dp"]), mesh=mesh, in_specs=placed, out_specs=outs, check_vma=False
    )
```

```python
import functools

import jax
import jax.numpy as jnp
from jax import lax
from jax.experimental import pallas as pl
from jax.experimental.pallas import tpu as pltpu
from jax.sharding import PartitionSpec as P

HEADS = 8
NORM_EPS = 1e-05
GROUP_EPS = 1.0
BF = jnp.bfloat16
F32 = jnp.float32
MESH = pl.DeviceIdType.MESH
LANES = 128


CORE, NEAR = 1, 2
TILE = 16


class Layout:
    def __init__(self, count, shard):
        self.count, self.shard = count, shard
        self.far_bit = 3 if (4 * shard) % LANES == 0 and count >= 32 else 2
        self.far = 1 << self.far_bit
        self.bits = count.bit_length() - 1
        self.rep_bits = [b for b in range(2, self.bits) if b != self.far_bit]
        self.reps = count // 8
        self.team = (CORE, NEAR, self.far, CORE | NEAR, CORE | self.far, NEAR | self.far,
                     CORE | NEAR | self.far)
        self.masks = self.team + tuple(
            1 << b for b in range(self.bits) if (1 << b) not in self.team
        )

    def place(self, device):
        return ((device // self.far) % 2) * 4 + device % 4

    def rep(self, device):
        total = 0
        for i, b in enumerate(self.rep_bits):
            total = total + ((device // (1 << b)) % 2) * (1 << i)
        return total

    def device(self, rep, place):
        total = place % 4 + (place // 4) * self.far
        for i, b in enumerate(self.rep_bits):
            total += ((rep >> i) & 1) << b
        return total

    def low(self, rel):
        return (rel & -rel).bit_length() - 1 if rel else len(self.rep_bits)

    def mask(self, rel):
        return 1 << self.rep_bits[self.low(rel)]

    def sources(self, rel):
        return [rel | (1 << i) for i in range(self.low(rel))]

    def pieces(self, width):
        if self.far_bit == 2:
            return [(0, width)]
        size = 4 * self.shard
        order = []
        for hi in range(self.count // 16):
            for b2 in range(2):
                for b3 in range(2):
                    order.append(((hi * 4 + b3 * 2 + b2) * size, size))
        return order


def flip_device(device, mask):
    other, bit = device, 0
    while mask >> bit:
        if (mask >> bit) & 1:
            other = other + (1 - 2 * ((device // (1 << bit)) % 2)) * (1 << bit)
        bit += 1
    return other


def xor_index(static, own, size):
    total, bit = 0, 1
    while bit < size:
        own_bit = (own // bit) % 2
        total = total + bit * (1 - own_bit if static & bit else own_bit)
        bit *= 2
    return total


def layer_norm(values, gain_vec, shift_vec):
    center = values - jnp.mean(values, axis=-1, keepdims=True)
    spread = jnp.mean(center * center, axis=-1, keepdims=True)
    return center * lax.rsqrt(spread + NORM_EPS) * gain_vec + shift_vec


def layer_norm_back(values, gain_vec, grads):
    center = values - jnp.mean(values, axis=-1, keepdims=True)
    scale = lax.rsqrt(jnp.mean(center * center, axis=-1, keepdims=True) + NORM_EPS)
    z = center * scale
    e = grads * gain_vec
    part = scale * (
        e - jnp.mean(e, axis=-1, keepdims=True) - z * jnp.mean(e * z, axis=-1, keepdims=True)
    )
    gain_part = jnp.sum(grads * z, axis=0, keepdims=True)
    shift_part = jnp.sum(grads, axis=0, keepdims=True)
    return part, gain_part, shift_part


def to_weight_order(values, pieces):
    return jnp.concatenate([values[:, at : at + size] for at, size in pieces], axis=1)


def from_weight_order(values, pieces):
    size = pieces[0][1]
    where = {at: i * size for i, (at, _) in enumerate(pieces)}
    return jnp.concatenate([values[:, where[at] : where[at] + size] for at in sorted(where)], axis=1)


class Links:
    def __init__(self, layout, send_sems, recv_sems, local_sems):
        self.layout = layout
        self.device = lax.axis_index("dp")
        self.send_sems, self.recv_sems, self.local_sems = send_sems, recv_sems, local_sems
        self.made, self.locals, self.sent = [], [], []

    def greet(self, masks):
        barrier = pltpu.get_barrier_semaphore()
        for mask in masks:
            pl.semaphore_signal(
                barrier, inc=1, device_id=(flip_device(self.device, mask),), device_id_type=MESH
            )
        pl.semaphore_wait(barrier, len(masks))

    def send(self, source, target, mask):
        index = len(self.made)
        copy = pltpu.make_async_remote_copy(
            src_ref=source,
            dst_ref=target,
            send_sem=self.send_sems.at[index],
            recv_sem=self.recv_sems.at[index],
            device_id=(flip_device(self.device, mask),),
            device_id_type=MESH,
        )
        copy.start()
        self.made.append(copy)
        return copy

    def local(self, source, target):
        copy = pltpu.make_async_copy(source, target, self.local_sems.at[len(self.locals)])
        copy.start()
        self.locals.append(copy)
        return copy

    def swap_done(self, copy):
        copy.wait()
        self.sent.append(copy)

    def finish(self):
        for copy in self.made:
            if not any(copy is other for other in self.sent):
                copy.wait_send()


def gather_steps(links, own, out):
    got = {}
    far = links.layout.far

    def begin():
        got["an"] = links.send(own.at[0], out.at[2], NEAR)
        got["bf"] = links.send(own.at[1], out.at[5], far)
        got["bn"] = links.send(own.at[1], out.at[3], NEAR)
        got["af"] = links.send(own.at[0], out.at[4], far)
        got["c"] = [links.send(own.at[i], out.at[8 + i], CORE) for i in range(2)]

    def relay():
        got["an"].wait_recv()
        got["anf"] = links.send(out.at[2], out.at[6], far)
        got["c"].append(links.send(out.at[2], out.at[10], CORE))
        got["bf"].wait_recv()
        got["bnf"] = links.send(out.at[5], out.at[7], NEAR)
        got["c"].append(links.send(out.at[5], out.at[13], CORE))
        got["bn"].wait_recv()
        got["c"].append(links.send(out.at[3], out.at[11], CORE))
        got["af"].wait_recv()
        got["c"].append(links.send(out.at[4], out.at[12], CORE))

    def end():
        got["anf"].wait_recv()
        got["c"].append(links.send(out.at[6], out.at[14], CORE))
        got["bnf"].wait_recv()
        got["c"].append(links.send(out.at[7], out.at[15], CORE))
        for copy in got["c"]:
            copy.wait_recv()

    return [begin, relay, end]


GATHER_COPIES = 14


def scatter_steps(links, parts, even, cores, taken, finish):
    got = {}
    far = links.layout.far

    def total(block):
        return even[block].astype(F32) + cores[block].astype(F32)

    def begin():
        got["load"] = links.local(parts.at[pl.ds(0, 8)], even)
        got["last"] = links.send(parts.at[pl.ds(14, 2)], cores.at[pl.ds(6, 2)], CORE)
        got["mid"] = links.send(parts.at[pl.ds(10, 4)], cores.at[pl.ds(2, 4)], CORE)
        got["own"] = links.send(parts.at[pl.ds(8, 2)], cores.at[pl.ds(0, 2)], CORE)

    def corners():
        got["load"].wait()
        got["last"].wait_recv()
        even[6] = total(6).astype(BF)
        got["anf"] = links.send(even.at[6], taken.at[0], far)
        even[7] = total(7).astype(BF)
        got["bnf"] = links.send(even.at[7], taken.at[1], NEAR)
        got["mid"].wait_recv()
        even[4] = total(4).astype(BF)
        got["af"] = links.send(even.at[4], taken.at[2], far)
        even[3] = total(3).astype(BF)
        got["bn"] = links.send(even.at[3], taken.at[3], NEAR)

    def relay():
        got["anf"].wait_recv()
        even[2] = (total(2) + taken[0].astype(F32)).astype(BF)
        got["an"] = links.send(even.at[2], taken.at[4], NEAR)
        got["bnf"].wait_recv()
        even[5] = (total(5) + taken[1].astype(F32)).astype(BF)
        got["bf"] = links.send(even.at[5], taken.at[5], far)

    def end():
        got["own"].wait_recv()
        for name in ("af", "an"):
            got[name].wait_recv()
        finish(0, total(0) + taken[2].astype(F32) + taken[4].astype(F32))
        for name in ("bn", "bf"):
            got[name].wait_recv()
        finish(1, total(1) + taken[3].astype(F32) + taken[5].astype(F32))

    return [begin, corners, relay, end]


SCATTER_COPIES = 9


def scatter_scratch(half, width):
    return [
        pltpu.VMEM((8, half, width), BF),
        pltpu.VMEM((8, half, width), BF),
        pltpu.VMEM((6, half, width), BF),
    ]


def gather_stream(links, items, lag):
    layout = links.layout
    made = [{} for _ in items]

    def spread(i, rel, source):
        slot = items[i][2]
        for bit in range(layout.low(rel)):
            goal = rel | (1 << bit)
            made[i][goal] = links.send(source, slot(rel), layout.mask(1 << bit))

    def step(k):
        def run():
            if k < len(items):
                ready, own, _ = items[k]
                ready()
                spread(k, 0, own)
            if k >= lag:
                i = k - lag
                for rel in range(2, layout.reps, 2):
                    made[i][rel].wait_recv()
                    spread(i, rel, items[i][2](rel))

        return run

    def end():
        for copies in made:
            for rel in range(1, layout.reps, 2):
                copies[rel].wait_recv()

    return [step(k) for k in range(len(items) + lag)], end


def scatter_stream(links, items, window, lag):
    layout = links.layout
    made = [{} for _ in items]
    loads = [None for _ in items]
    stay = range(0, layout.reps, 2)

    def begin(i):
        part, keep, taken, _ = items[i]
        loads[i] = [links.local(part(rel), keep(rel // 2)) for rel in stay]
        for rel in range(layout.reps - 1, 0, -2):
            made[i][rel] = links.send(part(rel), taken(rel - 1), layout.mask(rel))

    def total(i, rel):
        _, keep, taken, _ = items[i]
        for source in layout.sources(rel):
            made[i][source].wait_recv()
        value = keep(rel // 2)[...].astype(F32)
        for source in layout.sources(rel):
            value = value + taken(source - 1)[...].astype(F32)
        return value

    def pass_on(i):
        _, keep, taken, _ = items[i]
        for load in loads[i]:
            load.wait()
        for rel in stay[:0:-1]:
            keep(rel // 2)[...] = total(i, rel).astype(BF)
            made[i][rel] = links.send(keep(rel // 2), taken(rel - 1), layout.mask(rel))

    def step(k):
        def run():
            if k < len(items):
                begin(k)
            if window <= k < len(items) + window:
                pass_on(k - window)
            if k >= window + lag:
                items[k - window - lag][3](total(k - window - lag, 0))

        return run

    return [step(k) for k in range(len(items) + window + lag)]


def interleave(stream, acts, first=1):
    acts = list(acts)
    for k, step in enumerate(stream):
        step()
        if k >= first and acts:
            acts.pop(0)()
    for act in acts:
        act()


def semaphores(copies, local_copies):
    return [
        pltpu.SemaphoreType.DMA((copies,)),
        pltpu.SemaphoreType.DMA((copies,)),
        pltpu.SemaphoreType.DMA((local_copies,)),
    ]


VMEM = pl.BlockSpec(memory_space=pltpu.VMEM)
HBM = pl.BlockSpec(memory_space=pl.ANY)


def kernel_params(call_id):
    return pltpu.CompilerParams(collective_id=call_id, has_side_effects=True)


def opening_kernel(
    layout, small, tokens, cot, query_w, key_w, value_w, gate_w, gate_src, up_src, out_src, down_src,
    small_all, x_all, cot_all, attn_w, gate_in, up_in, out_w, down_w,
    small_buf, gain_buf, normed_buf, attn_own, out_own, down_own, gate_own, up_own, send_sems, recv_sems, local_sems,
):
    links = Links(layout, send_sems, recv_sems, local_sems)
    device = links.device
    place, rep = layout.place(device), layout.rep(device)
    _, half, width = tokens.shape
    shard = layout.shard

    def place_at(mask):
        return layout.place(flip_device(device, mask)) if mask else place

    edges, columns = 0, []
    for weight in (query_w, key_w, value_w, gate_w):
        size = weight.shape[1] // HEADS
        columns.append((weight, size, edges))
        edges += size

    def column(weight, size, where):
        return weight.at[:, pl.ds(pl.multiple_of(where * size, LANES), size)]

    mine = links.local(small, small_buf.at[pl.ds(device, 1)])
    own_loads = [
        links.local(column(weight, size, place), attn_own.at[:, pl.ds(at, size)])
        for weight, size, at in columns
    ]
    out_load, down_load = links.local(out_src, out_own), links.local(down_src, down_own)
    gate_load = links.local(gate_src.at[place], gate_own)
    up_load = links.local(up_src.at[place], up_own)
    links.greet(layout.masks)
    mine.wait()

    def small_step(b):
        size = 1 << b
        part = small_buf.at[pl.ds((device // size) * size, size)]
        return links.send(part, part, size)

    attn_in, later_in = {}, []

    def attn_exchange(mask):
        attn_in[mask] = [
            links.send(
                column(weight, size, place_at(mask)),
                attn_w.at[rep, place, :, pl.ds(at, size)],
                mask,
            )
            for weight, size, at in columns
        ]

    def hidden_exchange(mask):
        for source, target in ((gate_src, gate_in), (up_src, up_in)):
            later_in.append(links.send(source.at[place_at(mask)], target.at[place], mask))

    small_copy = small_step(0)
    for mask in layout.team[:3]:
        attn_exchange(mask)
    for load in own_loads:
        load.wait()
    keeps = [links.local(attn_own, attn_w.at[rep, place])]

    def attn_item(mask):
        at = place_at(mask)

        def ready():
            for copy in attn_in.get(mask, ()):
                copy.wait_recv()

        own = attn_w.at[rep, at] if mask else attn_own
        return ready, own, lambda rel: attn_w.at[xor_index(rel, rep, layout.reps), at]

    def row_item(own, target, part):
        return (
            lambda: None,
            own.at[part],
            lambda rel: target.at[xor_index(rel, rep, layout.reps), part],
        )

    items = [attn_item(mask) for mask in (0,) + layout.team]
    items += [row_item(out_own, out_w, part) for part in range(4)]
    items += [row_item(down_own, down_w, part) for part in range(4)]
    out_load.wait()
    down_load.wait()
    keeps.append(links.local(out_own, out_w.at[rep]))
    keeps.append(links.local(down_own, down_w.at[rep]))
    steps, stream_end = gather_stream(links, items, 3)
    steps[0]()
    for b in range(1, layout.bits):
        small_copy.wait_recv()
        small_copy = small_step(b)
        if b < 5:
            attn_exchange(layout.team[2 + b])
        if b == 2:
            steps[1]()
    steps[2]()
    small_copy.wait_recv()
    keeps.append(links.local(small_buf, small_all))

    per = LANES // shard
    for k in range(width // LANES):
        rows = small_buf[k * per].astype(F32)
        for i in range(1, per):
            rows = rows + small_buf[k * per + i].astype(F32)
        gain_buf[:, k * LANES : (k + 1) * LANES] = rows
    gain, shift = gain_buf[0:1, :], gain_buf[1:2, :]
    pieces = layout.pieces(width)

    def norm_rows(i, carry):
        part = i // (half // TILE)
        at = pl.ds(pl.multiple_of((i % (half // TILE)) * TILE, TILE), TILE)
        normed = layer_norm(tokens[part, at, :].astype(F32), gain, shift)
        normed_buf[part, at, :] = to_weight_order(normed, pieces).astype(BF)
        return carry

    lax.fori_loop(0, 2 * half // TILE, norm_rows, 0)
    keeps.append(links.local(normed_buf, x_all.at[pl.ds(0, 2)]))
    keeps.append(links.local(cot, cot_all.at[pl.ds(0, 2)]))
    for own, target, load in ((gate_own, gate_in, gate_load), (up_own, up_in, up_load)):
        load.wait()
        keeps.append(links.local(own, target.at[place]))

    def exchange_some(masks):
        return lambda: [hidden_exchange(mask) for mask in masks]

    x_steps = gather_steps(links, normed_buf, x_all)
    cot_steps = gather_steps(links, cot, cot_all)
    acts = x_steps[:1] + [lambda: None] + x_steps[1:2] + [lambda: None] + x_steps[2:]
    acts += [exchange_some(layout.team[:2]), exchange_some(layout.team[2:4])]
    acts += cot_steps[:1] + [exchange_some(layout.team[4:6])] + cot_steps[1:2]
    acts += [exchange_some(layout.team[6:])] + cot_steps[2:]
    interleave(steps[3:], acts, 0)
    stream_end()
    for copy in later_in:
        copy.wait_recv()
    for copy in keeps:
        copy.wait()
    links.finish()


def opening_call(layout, small, tokens, cot, attn_weights, gate_src, up_src, out_src, down_src):
    reps, shard = layout.reps, layout.shard
    rows, width = tokens.shape
    half = rows // 2
    attn_cols = sum(w.shape[1] for w in attn_weights) // HEADS
    ff_cols = gate_src.shape[2]
    down_rows, down_cols = down_src.shape
    down_shape = (4, down_rows // 4, down_cols)
    copies = 7 * 4 + 7 * 2 + 16 * (reps - 1) + 2 * GATHER_COPIES + layout.bits
    return pl.pallas_call(
        functools.partial(opening_kernel, layout),
        out_shape=(
            jax.ShapeDtypeStruct((layout.count, 8, LANES), BF),
            jax.ShapeDtypeStruct((16, half, width), BF),
            jax.ShapeDtypeStruct((16, half, width), BF),
            jax.ShapeDtypeStruct((reps, 8, shard, attn_cols), BF),
            jax.ShapeDtypeStruct((8, shard, ff_cols), BF),
            jax.ShapeDtypeStruct((8, shard, ff_cols), BF),
            jax.ShapeDtypeStruct((reps,) + down_shape, BF),
            jax.ShapeDtypeStruct((reps,) + down_shape, BF),
        ),
        in_specs=[HBM, VMEM] + [HBM] * 9,
        out_specs=(HBM,) * 8,
        scratch_shapes=[
            pltpu.VMEM((layout.count, 8, LANES), BF),
            pltpu.VMEM((8, width), F32),
            pltpu.VMEM((2, half, width), BF),
            pltpu.VMEM((shard, attn_cols), BF),
            pltpu.VMEM(down_shape, BF),
            pltpu.VMEM(down_shape, BF),
            pltpu.VMEM((shard, ff_cols), BF),
            pltpu.VMEM((shard, ff_cols), BF),
        ]
        + semaphores(copies, 18),
        compiler_params=kernel_params(0),
        name="opening",
    )(
        small, tokens.reshape(2, half, width), cot.reshape(2, half, width), *attn_weights,
        gate_src, up_src, out_src.reshape(down_shape), down_src.reshape(down_shape),
    )


def turn_kernel(
    layout, parts, tokens, gains, gate_in, up_in,
    hidden, all_rows, gate_w, up_w,
    even, cores, taken, normed_buf, send_sems, recv_sems, local_sems,
):
    links = Links(layout, send_sems, recv_sems, local_sems)
    rep = layout.rep(links.device)
    _, half, width = tokens.shape
    links.greet((CORE, NEAR, layout.far) + tuple(1 << b for b in layout.rep_bits))
    keeps = [links.local(gate_in, gate_w.at[rep]), links.local(up_in, up_w.at[rep])]

    def item(own, target, part):
        at = pl.ds(part * 2, 2)
        return (
            lambda: None,
            own.at[at],
            lambda rel: target.at[xor_index(rel, rep, layout.reps), at],
        )

    items = [item(gate_in, gate_w, part) for part in range(4)]
    items += [item(up_in, up_w, part) for part in range(4)]
    steps, stream_end = gather_stream(links, items, 2)
    pieces = layout.pieces(width)

    def finish(part, value):
        hidden[part] = value + tokens[part].astype(F32)

        def norm_rows(i, carry):
            at = pl.ds(pl.multiple_of(i * TILE, TILE), TILE)
            normed = layer_norm(hidden[part, at, :], gains[0:1, :], gains[1:2, :])
            normed_buf[part, at, :] = to_weight_order(normed, pieces).astype(BF)
            return carry

        lax.fori_loop(0, half // TILE, norm_rows, 0)

    acts = scatter_steps(links, parts, even, cores, taken, finish)
    acts.append(lambda: keeps.append(links.local(normed_buf, all_rows.at[pl.ds(0, 2)])))
    acts += gather_steps(links, normed_buf, all_rows)
    acts.pop(0)()
    interleave(steps, acts, 0)
    stream_end()
    for copy in keeps:
        copy.wait()
    links.finish()


def turn_call(layout, parts, tokens, gains, gate_in, up_in):
    rows, width = tokens.shape
    half = rows // 2
    block = gate_in.shape
    return pl.pallas_call(
        functools.partial(turn_kernel, layout),
        out_shape=(
            jax.ShapeDtypeStruct((2, half, width), F32),
            jax.ShapeDtypeStruct((16, half, width), BF),
            jax.ShapeDtypeStruct((layout.reps,) + block, BF),
            jax.ShapeDtypeStruct((layout.reps,) + block, BF),
        ),
        in_specs=[HBM, VMEM, VMEM, VMEM, VMEM],
        out_specs=(VMEM, HBM, HBM, HBM),
        scratch_shapes=scatter_scratch(half, width)
        + [pltpu.VMEM((2, half, width), BF)]
        + semaphores(8 * (layout.reps - 1) + SCATTER_COPIES + GATHER_COPIES, 5),
        compiler_params=kernel_params(1),
        name="turn",
    )(parts.reshape(16, half, width), tokens.reshape(2, half, width), gains, gate_in, up_in)


def turn_back_kernel(
    layout, parts, hidden, out_grad, gains, down_p, gate_p,
    hidden_grad, all_rows, vectors, down_sum, gate_sum,
    even, cores, taken, low_buf, sum_buf, down_l, down_y, gate_l, gate_y,
    send_sems, recv_sems, local_sems,
):
    links = Links(layout, send_sems, recv_sems, local_sems)
    rep = layout.rep(links.device)
    _, half, width = hidden.shape
    links.greet((CORE, NEAR, layout.far) + tuple(1 << b for b in layout.rep_bits))
    items = replica_items(layout, rep, down_p, down_l, down_y, range(4), down_sum)
    pairs = [pl.ds(2 * part, 2) for part in range(4)]
    items += replica_items(layout, rep, gate_p, gate_l, gate_y, pairs, gate_sum)
    steps = scatter_stream(links, items, 2, 2)
    pieces = layout.pieces(width)
    vectors[...] = jnp.zeros_like(vectors)

    def finish(part, value):
        sum_buf[...] = value

        def rows(i, carry):
            at = pl.ds(pl.multiple_of(i * TILE, TILE), TILE)
            grads = from_weight_order(sum_buf[at, :], pieces)
            back, gain_part, shift_part = layer_norm_back(
                hidden[part, at, :], gains[0:1, :], grads
            )
            total = out_grad[part, at, :].astype(F32) + back
            hidden_grad[part, at, :] = total
            low_buf[part, at, :] = total.astype(BF)
            vectors[0:1, :] += gain_part
            vectors[1:2, :] += shift_part
            return carry

        lax.fori_loop(0, half // TILE, rows, 0)

    keeps = []
    acts = scatter_steps(links, parts, even, cores, taken, finish)
    acts.append(lambda: keeps.append(links.local(low_buf, all_rows.at[pl.ds(0, 2)])))
    acts += gather_steps(links, low_buf, all_rows)
    acts.pop(0)()
    interleave(steps, acts, 0)
    for copy in keeps:
        copy.wait()
    links.finish()


def replica_items(layout, rep, part, keep, taken, places, sums):
    def item(at):
        def finish(value):
            sums[at] = value.astype(sums.dtype)

        return (
            lambda rel: part.at[xor_index(rel, rep, layout.reps), at],
            lambda i: keep.at[i, at],
            lambda i: taken.at[i, at],
            finish,
        )

    return [item(at) for at in places]


def turn_back_call(layout, parts, hidden, out_grad, gains, down_p, gate_p):
    half, width = hidden.shape[1:]
    reps = layout.reps
    down_block, gate_block = down_p.shape[1:], gate_p.shape[1:]
    return pl.pallas_call(
        functools.partial(turn_back_kernel, layout),
        out_shape=(
            jax.ShapeDtypeStruct((2, half, width), F32),
            jax.ShapeDtypeStruct((16, half, width), BF),
            jax.ShapeDtypeStruct((8, width), F32),
            jax.ShapeDtypeStruct(down_block, F32),
            jax.ShapeDtypeStruct(gate_block, BF),
        ),
        in_specs=[HBM, VMEM, VMEM, VMEM, HBM, HBM],
        out_specs=(VMEM, HBM, VMEM, VMEM, VMEM),
        scratch_shapes=scatter_scratch(half, width)
        + [
            pltpu.VMEM((2, half, width), BF),
            pltpu.VMEM((half, width), F32),
            pltpu.VMEM((reps // 2,) + down_block, BF),
            pltpu.VMEM((reps - 1,) + down_block, BF),
            pltpu.VMEM((reps // 2,) + gate_block, BF),
            pltpu.VMEM((reps - 1,) + gate_block, BF),
        ]
        + semaphores(8 * (reps - 1) + SCATTER_COPIES + GATHER_COPIES, 4 * reps + 2),
        compiler_params=kernel_params(2),
        name="turn_back",
    )(
        parts.reshape(16, half, width), hidden, out_grad.reshape(2, half, width), gains,
        down_p, gate_p,
    )


def closing_kernel(
    layout, attn_p, up_p, out_p, gate_sum, one_parts, two_parts, tokens, hidden_grad, gains, vectors,
    query_back, key_back, value_back, swish_back, gate_back, up_back, out_sum, branch_two,
    tokens_grad, vector_sum,
    even_1, cores_1, taken_1, even_2, cores_2, taken_2, sum_buf, rows_buf, vec_l, vec_y,
    attn_l, attn_y, attn_s, up_l, up_y, up_s, out_l, out_y, send_sems, recv_sems, local_sems,
):
    links = Links(layout, send_sems, recv_sems, local_sems)
    device = links.device
    place, rep = layout.place(device), layout.rep(device)
    _, half, width = tokens.shape
    links.greet(layout.masks)
    backs, kept = [], []

    def place_at(mask):
        return layout.place(flip_device(device, mask)) if mask else place

    def give(source, target, mask):
        if mask:
            backs.append(links.send(source, target, mask))
        else:
            kept.append(links.local(source, target))

    edges, columns = 0, []
    for target in (query_back, key_back, value_back, swish_back):
        size = target.shape[1] // HEADS
        columns.append((target, size, edges))
        edges += size

    def with_return(item, mask, give_back):
        part, keep, taken, finish = item

        def finish_and_give(value):
            finish(value)
            give_back(mask)

        return part, keep, taken, finish_and_give

    def attn_return(mask):
        for target, size, at in columns:
            goal = pl.ds(pl.multiple_of(place * size, LANES), size)
            give(attn_s.at[place_at(mask), :, pl.ds(at, size)], target.at[:, goal], mask)

    def up_return(mask):
        give(up_s.at[place_at(mask)], up_back.at[place], mask)

    order = layout.team[::-1] + (0,)
    items = []
    for part, keep, taken, sums, give_back in (
        (attn_p, attn_l, attn_y, attn_s, attn_return),
        (up_p, up_l, up_y, up_s, up_return),
    ):
        plain = replica_items(layout, rep, part, keep, taken, [place_at(m) for m in order], sums)
        items += [with_return(item, m, give_back) for item, m in zip(plain, order)]
    items += replica_items(layout, rep, out_p, out_l, out_y, range(4), out_sum)
    steps = scatter_stream(links, items, 2, 2)

    pieces = layout.pieces(width)
    rows_buf[...] = jnp.zeros_like(rows_buf)
    rows_buf[2:4, :] = vectors[0:2, :]

    def finish_one(part, value):
        sum_buf[...] = value

        def rows(i, carry):
            at = pl.ds(pl.multiple_of(i * TILE, TILE), TILE)
            grads = from_weight_order(sum_buf[at, :], pieces)
            back, gain_part, shift_part = layer_norm_back(
                tokens[part, at, :].astype(F32), gains[0:1, :], grads
            )
            tokens_grad[part, at, :] = hidden_grad[part, at, :] + back
            rows_buf[0:1, :] += gain_part
            rows_buf[1:2, :] += shift_part
            return carry

        lax.fori_loop(0, half // TILE, rows, 0)

    def finish_two(part, value):
        branch_two[part] = value

    per = LANES // layout.shard
    own_bits = per.bit_length() - 1
    slots = layout.count // per
    flight = {}

    def vector_begin():
        for slot in range(slots):
            vec_l[slot] = rows_buf[:, slot * LANES : (slot + 1) * LANES]

    def vector_send(b):
        def run():
            peer = flip_device(device, 1 << b)
            if b >= own_bits:
                size = 1 << (b - own_bits)
                source = vec_l.at[pl.ds((peer // (1 << b)) * size, size)]
                target = vec_y.at[pl.ds(size, size)]
            else:
                source = vec_l.at[pl.ds(device // per, 1)]
                target = vec_y.at[pl.ds(slots + b, 1)]
            flight[b] = links.send(source, target, 1 << b)

        return run

    def vector_add(b):
        def run():
            if b >= own_bits:
                size = 1 << (b - own_bits)
                flight[b].wait_recv()
                mine = pl.ds((device // (1 << b)) * size, size)
                vec_l[mine] = vec_l[mine] + vec_y[size : 2 * size]
            else:
                links.swap_done(flight[b])
                mine = pl.ds(device // per, 1)
                vec_l[mine] = vec_l[mine] + vec_y[slots + b : slots + b + 1]

        return run

    def gate_return():
        for mask in layout.team + (0,):
            give(gate_sum.at[place_at(mask)], gate_back.at[place], mask)

    one = scatter_steps(links, one_parts, even_1, cores_1, taken_1, finish_one)
    two = scatter_steps(links, two_parts, even_2, cores_2, taken_2, finish_two)
    acts = one[1:] + [vector_begin]
    down_bits = list(range(layout.bits))[::-1]
    together = [(lambda b=b, a=a: ((a() if a else None), vector_send(b)())) for a, b in zip(
        [None] + [vector_add(b) for b in down_bits[:-1]], down_bits)]
    acts += [lambda: (together[0](), two[0](), gate_return())]
    for k in range(1, layout.bits):
        extra = two[k] if k < len(two) else (lambda: None)
        acts.append(lambda k=k, extra=extra: (together[k](), extra()))
    acts += two[layout.bits :] + [vector_add(down_bits[-1])]
    one[0]()
    interleave(steps, acts, 0)
    vector_sum[...] = vec_l[device // per]
    for copy in backs:
        copy.wait_recv()
    for copy in kept:
        copy.wait()
    links.finish()


def closing_call(layout, attn_p, up_p, out_p, gate_sum, one_parts, two_parts, tokens, hidden_grad,
                 gains, vectors, back_widths):
    reps, shard = layout.reps, layout.shard
    half, width = hidden_grad.shape[1:]
    attn_block, up_block, out_block = attn_p.shape[1:], up_p.shape[1:], out_p.shape[1:]
    per = LANES // shard
    slots = layout.count // per
    stay = reps // 2
    rows = jax.ShapeDtypeStruct((2, half, width), F32)
    copies = 20 * (reps - 1) + 7 * 6 + 2 * SCATTER_COPIES + layout.bits
    return pl.pallas_call(
        functools.partial(closing_kernel, layout),
        out_shape=tuple(jax.ShapeDtypeStruct((shard, w), BF) for w in back_widths)
        + (
            jax.ShapeDtypeStruct(up_block, BF),
            jax.ShapeDtypeStruct(up_block, BF),
            jax.ShapeDtypeStruct(out_block, F32),
            rows,
            rows,
            jax.ShapeDtypeStruct((8, LANES), F32),
        ),
        in_specs=[HBM, HBM, HBM, VMEM, HBM, HBM, VMEM, VMEM, VMEM, VMEM],
        out_specs=(HBM,) * 6 + (VMEM,) * 4,
        scratch_shapes=scatter_scratch(half, width)
        + scatter_scratch(half, width)
        + [
            pltpu.VMEM((half, width), F32),
            pltpu.VMEM((8, width), F32),
            pltpu.VMEM((slots, 8, LANES), F32),
            pltpu.VMEM((slots + per, 8, LANES), F32),
            pltpu.VMEM((stay,) + attn_block, BF),
            pltpu.VMEM((reps - 1,) + attn_block, BF),
            pltpu.VMEM(attn_block, BF),
            pltpu.VMEM((stay,) + up_block, BF),
            pltpu.VMEM((reps - 1,) + up_block, BF),
            pltpu.VMEM(up_block, BF),
            pltpu.VMEM((stay,) + out_block, BF),
            pltpu.VMEM((reps - 1,) + out_block, BF),
        ]
        + semaphores(copies, 20 * stay + 8),
        compiler_params=kernel_params(3),
        name="closing",
    )(
        attn_p, up_p, out_p, gate_sum, one_parts.reshape(16, half, width),
        two_parts.reshape(16, half, width), tokens.reshape(2, half, width), hidden_grad, gains, vectors,
    )


def seq_layout(seq_lens, row_count):
    row_ids = jnp.arange(row_count, dtype=jnp.int32)
    seq_ends = jnp.cumsum(seq_lens)
    passed = row_ids[:, None] >= seq_ends[None, :]
    segment = jnp.sum(passed.astype(jnp.int32), axis=1)
    seq_start = jnp.sum(jnp.where(passed, seq_lens[None, :], 0), axis=1)
    position = row_ids - seq_start
    live_rows = row_ids < seq_ends[-1]
    return (segment, position, live_rows)


def group_norm(values):
    center = values - jnp.mean(values, axis=-1, keepdims=True)
    spread = jnp.mean(center * center, axis=-1, keepdims=True)
    return center * lax.rsqrt(spread + GROUP_EPS)


def dot(left, right):
    return jnp.dot(left, right, preferred_element_type=F32)


def dot_nt(left, right):
    return lax.dot_general(left, right, (((1,), (1,)), ((), ())), preferred_element_type=F32)


def dot_tn(left, right):
    return lax.dot_general(left, right, (((0,), (0,)), ((), ())), preferred_element_type=F32)


def make_body(count):
    def on_device(
        tokens,
        seq_lengths,
        attn_gain,
        attn_shift,
        query_weight,
        key_weight,
        value_weight,
        gate_weight,
        out_weight,
        mlp_gain,
        mlp_shift,
        mlp_gate,
        mlp_up,
        mlp_down,
        cotangent,
    ):
        local_rows, width = tokens.shape
        shard = width // count
        layout = Layout(count, shard)
        reps = layout.reps
        device = lax.axis_index("dp")
        rep, pos_t = layout.rep(device), layout.place(device)
        micro_count, seq_slots = seq_lengths.shape[1:]
        row_count = local_rows // micro_count
        key_size = query_weight.shape[1] // HEADS
        value_size = value_weight.shape[1] // HEADS
        hidden_size = mlp_gate.shape[1]
        ff_block = hidden_size // count
        group_rows = 8 * local_rows
        half = local_rows // 2
        home = [layout.device(d % reps, d // reps) for d in range(count)]
        head_perm = [(d, home[d]) for d in range(count)]
        head_back = [(b, a) for a, b in head_perm]

        high, mid = 1 << (layout.bits - 1 - layout.far_bit), 1 << (layout.far_bit - 2)

        def ff_first(weight):
            v = weight.reshape(shard, high, 2, mid, 4, ff_block)
            return v.transpose(2, 4, 0, 1, 3, 5).reshape(8, shard, reps * ff_block)

        def ff_back(grad):
            v = grad.reshape(2, 4, shard, high, mid, ff_block)
            return v.transpose(2, 3, 0, 4, 1, 5).reshape(shard, hidden_size)

        per = LANES // shard
        lane_on = jnp.arange(LANES, dtype=jnp.int32) // shard == device % per

        def in_lanes(values):
            return jnp.where(lane_on, jnp.tile(values, per), jnp.zeros((), BF))[None]

        own_lens = seq_lengths.reshape(-1).astype(BF)
        small = jnp.concatenate(
            [in_lanes(v) for v in (attn_gain, attn_shift, mlp_gain, mlp_shift)]
            + [jnp.pad(own_lens, (0, LANES - own_lens.shape[0]))[None], jnp.zeros((3, LANES), BF)]
        )
        own_live = jax.vmap(lambda v: seq_layout(v, row_count)[2])(seq_lengths[0])
        own_live = own_live.reshape(local_rows).astype(F32)[:, None]
        out_grad_low = (cotangent.astype(F32) * own_live).astype(BF)

        out_own = lax.ppermute(out_weight, "dp", head_perm)
        small, normed_one, cot_all, attn_w, gate_in, up_in, out_w, down_w = opening_call(
            layout, small[None], tokens, out_grad_low,
            (query_weight, key_weight, value_weight, gate_weight),
            ff_first(mlp_gate), ff_first(mlp_up), out_own, mlp_down,
        )
        normed_one = normed_one.reshape(group_rows, width)
        cot_all = cot_all.reshape(group_rows, width)
        attn_w = attn_w.reshape(width, -1)
        out_w = out_w.reshape(-1, width)
        down_w = down_w.reshape(-1, width)

        vecs = small[:, :4, :].astype(F32).reshape(-1, per, 4, LANES).sum(1)
        vecs = vecs.transpose(1, 0, 2).reshape(4, width)
        gains_one = jnp.pad(vecs[:2], ((0, 6), (0, 0)))
        gains_two = jnp.pad(vecs[2:], ((0, 6), (0, 0)))
        lens = small[:, 4, : own_lens.shape[0]].astype(jnp.int32)
        order = [c + 2 * n + 4 * f for c in range(2) for f in range(2) for n in range(2)]
        members = jnp.stack(
            [flip_device(device, (j & 3) + (j >> 2) * layout.far) for j in order]
        )
        lens = jnp.take(lens, members, axis=0).reshape(8 * micro_count, seq_slots)

        segment, position, live = jax.vmap(lambda s: seq_layout(s, row_count))(lens)
        head_log = jnp.log(1.0 - 2.0 ** (-5.0 - jnp.arange(HEADS, dtype=F32)))
        head_log = lax.dynamic_index_in_dim(head_log, pos_t, 0, keepdims=False)
        ids = jnp.arange(row_count, dtype=jnp.int32)
        same_seq = (
            (segment[:, :, None] == segment[:, None, :])
            & live[:, :, None]
            & live[:, None, :]
            & (ids[:, None] >= ids[None, :])[None]
        )
        distance = jnp.maximum(position[:, :, None] - position[:, None, :], 0).astype(F32)
        decay = jnp.where(same_seq, jnp.exp(distance * head_log), 0.0)
        half_size = key_size // 2
        pair_index = jnp.arange(half_size, dtype=F32)
        frequency = 10000.0 ** (-pair_index / half_size)
        row_place = position.reshape(-1).astype(F32)[:, None]
        angles = row_place * frequency[None, :]
        growth = (pair_index * 2.0 / key_size + 0.4) / 1.4
        stretch = growth[None, :] ** (row_place / 512.0)
        cosine, sine = jnp.cos(angles), jnp.sin(angles)
        key_factor = key_size ** (-0.5) / stretch

        def rotate(values, factor):
            a, b = values[:, :half_size], values[:, half_size:]
            return jnp.concatenate(
                [(a * cosine - b * sine) * factor, (b * cosine + a * sine) * factor], axis=1
            )

        def rotate_back(grads, factor):
            a, b = grads[:, :half_size] * factor, grads[:, half_size:] * factor
            return jnp.concatenate([a * cosine + b * sine, b * cosine - a * sine], axis=1)

        def micro(values):
            return values.reshape(-1, row_count, values.shape[-1])

        qkvg = dot(normed_one, attn_w)
        query_raw = qkvg[:, :key_size]
        key_raw = qkvg[:, key_size : 2 * key_size]
        value_low = qkvg[:, 2 * key_size : 2 * key_size + value_size].astype(BF)
        gate_raw = qkvg[:, 2 * key_size + value_size :]
        query_turned = micro(rotate(query_raw, stretch).astype(BF))
        key_turned = micro(rotate(key_raw, key_factor).astype(BF))
        value_m = micro(value_low)
        scores = jnp.einsum("mqd,mkd->mqk", query_turned, key_turned, preferred_element_type=F32)
        weights_low = (scores * decay).astype(BF)
        retained = jnp.einsum("mqk,mke->mqe", weights_low, value_m, preferred_element_type=F32)
        retained = retained.reshape(group_rows, value_size)

        def mix(gate_in, retained_in):
            return jax.nn.silu(gate_in) * group_norm(retained_in)

        mixed = mix(gate_raw, retained).astype(BF)
        hidden, normed_two, gate_w, up_w = turn_call(
            layout, dot(mixed, out_w).astype(BF), tokens, gains_two, gate_in, up_in
        )
        normed_two = normed_two.reshape(group_rows, width)
        gate_w, up_w = gate_w.reshape(width, -1), up_w.reshape(width, -1)

        def act(gate_in, up_in):
            return jax.nn.gelu(gate_in, approximate=True) * up_in

        product, pull_act = jax.vjp(act, dot(normed_two, gate_w), dot(normed_two, up_w))
        product = product.astype(BF)
        gate_low, up_low = (g.astype(BF) for g in pull_act(dot_nt(cot_all, down_w)))
        two_parts = dot(product, down_w).astype(BF)
        down_parts = dot_tn(product, cot_all).astype(BF)
        gate_parts = dot_tn(normed_two, gate_low).astype(BF)
        up_parts = dot_tn(normed_two, up_low).astype(BF)
        normed_parts = (dot_nt(gate_low, gate_w) + dot_nt(up_low, up_w)).astype(BF)
        hidden_grad, branch_one_grad, vectors, mlp_down_grad, gate_sum = turn_back_call(
            layout, normed_parts, hidden, out_grad_low, gains_two,
            down_parts.reshape(reps, 4, -1, width), gate_parts.reshape(reps, 8, shard, -1),
        )
        branch_one_grad = branch_one_grad.reshape(group_rows, width)

        mixed_grad = dot_nt(branch_one_grad, out_w)
        _, pull_mix = jax.vjp(mix, gate_raw, retained)
        gate_grad, retained_grad = pull_mix(mixed_grad)
        gate_grad = gate_grad.astype(BF)
        retained_low = micro(retained_grad.astype(BF))
        weights_grad = jnp.einsum("mqe,mke->mqk", retained_low, value_m, preferred_element_type=F32)
        value_grad = jnp.einsum("mqk,mqe->mke", weights_low, retained_low, preferred_element_type=F32)
        value_grad = value_grad.reshape(group_rows, value_size).astype(BF)
        score_low = (weights_grad * decay).astype(BF)
        query_turn_grad = jnp.einsum("mqk,mkd->mqd", score_low, key_turned, preferred_element_type=F32)
        key_turn_grad = jnp.einsum("mqk,mqd->mkd", score_low, query_turned, preferred_element_type=F32)
        query_grad = rotate_back(query_turn_grad.reshape(group_rows, key_size), stretch).astype(BF)
        key_grad = rotate_back(key_turn_grad.reshape(group_rows, key_size), key_factor).astype(BF)
        attn_grads = jnp.concatenate([query_grad, key_grad, value_grad, gate_grad], axis=1)
        attn_parts = dot_tn(normed_one, attn_grads).astype(BF)
        out_parts = dot_tn(mixed, branch_one_grad).astype(BF)
        one_parts = dot_nt(attn_grads, attn_w).astype(BF)
        q_back, k_back, v_back, g_back, gate_back, up_back, out_sum, branch_two, tokens_grad, vectors = (
            closing_call(
                layout,
                attn_parts.reshape(reps, 8, shard, -1),
                up_parts.reshape(reps, 8, shard, -1),
                out_parts.reshape(reps, 4, -1, width),
                gate_sum, one_parts, two_parts, tokens, hidden_grad, gains_one, vectors,
                [w.shape[1] for w in (query_weight, key_weight, value_weight, gate_weight)],
            )
        )
        out_sum = out_sum.reshape(out_weight.shape).astype(BF)
        out_weight_grad = lax.ppermute(out_sum, "dp", head_back).astype(F32)
        output = ((hidden + branch_two).reshape(local_rows, width) * own_live).astype(BF)
        vectors = lax.dynamic_slice_in_dim(vectors, (device % per) * shard, shard, axis=1)
        return (
            output,
            tokens_grad.reshape(local_rows, width),
            vectors[0],
            vectors[1],
            q_back.astype(F32),
            k_back.astype(F32),
            v_back.astype(F32),
            g_back.astype(F32),
            out_weight_grad,
            vectors[2],
            vectors[3],
            ff_back(gate_back.astype(F32)),
            ff_back(up_back.astype(F32)),
            mlp_down_grad.reshape(mlp_down.shape),
        )

    return on_device


def solution(mesh):
    rows = P("dp", None)
    vec = P("dp")
    placed = (
        rows, P("dp", None, None), vec, vec, rows, rows, rows, rows, rows,
        vec, vec, rows, rows, rows, rows,
    )
    outs = (rows, rows, vec, vec, rows, rows, rows, rows, rows, vec, vec, rows, rows, rows)
    return jax.shard_map(
        make_body(mesh.shape["dp"]), mesh=mesh, in_specs=placed, out_specs=outs, check_vma=False
    )
```

```python
import functools

import jax
import jax.numpy as jnp
from jax import lax
from jax.experimental import pallas as pl
from jax.experimental.pallas import tpu as pltpu
from jax.sharding import PartitionSpec as P


HEADS = 8
NORM_EPS = 1e-05
GROUP_EPS = 1.0
BF = jnp.bfloat16
F32 = jnp.float32
MESH = pl.DeviceIdType.MESH
LANES = 128


CORE, NEAR = 1, 2
TILE = 16


class Layout:
    def __init__(self, count, shard):
        self.count, self.shard = count, shard
        self.far_bit = 3 if (4 * shard) % LANES == 0 and count >= 32 else 2
        self.far = 1 << self.far_bit
        self.bits = count.bit_length() - 1
        self.rep_bits = [b for b in range(2, self.bits) if b != self.far_bit]
        self.reps = count // 8
        self.team = (CORE, NEAR, self.far, CORE | NEAR, CORE | self.far, NEAR | self.far,
                     CORE | NEAR | self.far)
        self.masks = self.team + tuple(
            1 << b for b in range(self.bits) if (1 << b) not in self.team
        )

    def place(self, device):
        return ((device // self.far) % 2) * 4 + device % 4

    def rep(self, device):
        total = 0
        for i, b in enumerate(self.rep_bits):
            total = total + ((device // (1 << b)) % 2) * (1 << i)
        return total

    def device(self, rep, place):
        total = place % 4 + (place // 4) * self.far
        for i, b in enumerate(self.rep_bits):
            total += ((rep >> i) & 1) << b
        return total

    def low(self, rel):
        return (rel & -rel).bit_length() - 1 if rel else len(self.rep_bits)

    def mask(self, rel):
        return 1 << self.rep_bits[self.low(rel)]

    def sources(self, rel):
        return [rel | (1 << i) for i in range(self.low(rel))]

    def pieces(self, width):
        if self.far_bit == 2:
            return [(0, width)]
        size = 4 * self.shard
        order = []
        for hi in range(self.count // 16):
            for b2 in range(2):
                for b3 in range(2):
                    order.append(((hi * 4 + b3 * 2 + b2) * size, size))
        return order


def flip_device(device, mask):
    other, bit = device, 0
    while mask >> bit:
        if (mask >> bit) & 1:
            other = other + (1 - 2 * ((device // (1 << bit)) % 2)) * (1 << bit)
        bit += 1
    return other


def xor_index(static, own, size):
    total, bit = 0, 1
    while bit < size:
        own_bit = (own // bit) % 2
        total = total + bit * (1 - own_bit if static & bit else own_bit)
        bit *= 2
    return total


def layer_norm(values, gain_vec, shift_vec):
    center = values - jnp.mean(values, axis=-1, keepdims=True)
    spread = jnp.mean(center * center, axis=-1, keepdims=True)
    return center * lax.rsqrt(spread + NORM_EPS) * gain_vec + shift_vec


def layer_norm_back(values, gain_vec, grads):
    center = values - jnp.mean(values, axis=-1, keepdims=True)
    scale = lax.rsqrt(jnp.mean(center * center, axis=-1, keepdims=True) + NORM_EPS)
    z = center * scale
    e = grads * gain_vec
    part = scale * (
        e - jnp.mean(e, axis=-1, keepdims=True) - z * jnp.mean(e * z, axis=-1, keepdims=True)
    )
    gain_part = jnp.sum(grads * z, axis=0, keepdims=True)
    shift_part = jnp.sum(grads, axis=0, keepdims=True)
    return part, gain_part, shift_part


def to_weight_order(values, pieces):
    return jnp.concatenate([values[:, at : at + size] for at, size in pieces], axis=1)


def from_weight_order(values, pieces):
    size = pieces[0][1]
    where = {at: i * size for i, (at, _) in enumerate(pieces)}
    return jnp.concatenate([values[:, where[at] : where[at] + size] for at in sorted(where)], axis=1)


class Links:
    def __init__(self, layout, send_sems, recv_sems, local_sems):
        self.layout = layout
        self.device = lax.axis_index("dp")
        self.send_sems, self.recv_sems, self.local_sems = send_sems, recv_sems, local_sems
        self.made, self.locals, self.sent = [], [], []

    def greet(self, masks):
        barrier = pltpu.get_barrier_semaphore()
        for mask in masks:
            pl.semaphore_signal(
                barrier, inc=1, device_id=(flip_device(self.device, mask),), device_id_type=MESH
            )
        pl.semaphore_wait(barrier, len(masks))

    def send(self, source, target, mask):
        index = len(self.made)
        copy = pltpu.make_async_remote_copy(
            src_ref=source,
            dst_ref=target,
            send_sem=self.send_sems.at[index],
            recv_sem=self.recv_sems.at[index],
            device_id=(flip_device(self.device, mask),),
            device_id_type=MESH,
        )
        copy.start()
        self.made.append(copy)
        return copy

    def local(self, source, target):
        copy = pltpu.make_async_copy(source, target, self.local_sems.at[len(self.locals)])
        copy.start()
        self.locals.append(copy)
        return copy

    def swap_done(self, copy):
        copy.wait()
        self.sent.append(copy)

    def finish(self):
        for copy in self.made:
            if not any(copy is other for other in self.sent):
                copy.wait_send()


def gather_steps(links, own, out):
    got = {}
    far = links.layout.far

    def begin():
        got["an"] = links.send(own.at[0], out.at[2], NEAR)
        got["bf"] = links.send(own.at[1], out.at[5], far)
        got["bn"] = links.send(own.at[1], out.at[3], NEAR)
        got["af"] = links.send(own.at[0], out.at[4], far)
        got["c"] = [links.send(own.at[i], out.at[8 + i], CORE) for i in range(2)]

    def relay():
        got["an"].wait_recv()
        got["anf"] = links.send(out.at[2], out.at[6], far)
        got["c"].append(links.send(out.at[2], out.at[10], CORE))
        got["bf"].wait_recv()
        got["bnf"] = links.send(out.at[5], out.at[7], NEAR)
        got["c"].append(links.send(out.at[5], out.at[13], CORE))
        got["bn"].wait_recv()
        got["c"].append(links.send(out.at[3], out.at[11], CORE))
        got["af"].wait_recv()
        got["c"].append(links.send(out.at[4], out.at[12], CORE))

    def end():
        got["anf"].wait_recv()
        got["c"].append(links.send(out.at[6], out.at[14], CORE))
        got["bnf"].wait_recv()
        got["c"].append(links.send(out.at[7], out.at[15], CORE))
        for copy in got["c"]:
            copy.wait_recv()

    return [begin, relay, end]


def gather_steps_light(links, own, out):
    got = {}
    far = links.layout.far

    def begin():
        got["af"] = links.send(own.at[0], out.at[4], far)
        got["bf"] = links.send(own.at[1], out.at[5], far)
        got["an"] = links.send(own.at[0], out.at[2], NEAR)
        got["bn"] = links.send(own.at[1], out.at[3], NEAR)
        got["c"] = [links.send(own.at[i], out.at[8 + i], CORE) for i in range(2)]

    def relay():
        for i, name in enumerate(("af", "bf")):
            got[name].wait_recv()
            got[name + "n"] = links.send(out.at[4 + i], out.at[6 + i], NEAR)
            got["c"].append(links.send(out.at[4 + i], out.at[12 + i], CORE))
        for i, name in enumerate(("an", "bn")):
            got[name].wait_recv()
            got["c"].append(links.send(out.at[2 + i], out.at[10 + i], CORE))

    def end():
        for i, name in enumerate(("afn", "bfn")):
            got[name].wait_recv()
            got["c"].append(links.send(out.at[6 + i], out.at[14 + i], CORE))
        for copy in got["c"]:
            copy.wait_recv()

    return [begin, relay, end]


GATHER_COPIES = 14


def scatter_steps(links, parts, even, cores, taken, finish):
    got = {}
    far = links.layout.far

    def total(block):
        return even[block].astype(F32) + cores[block].astype(F32)

    def begin():
        got["load"] = links.local(parts.at[pl.ds(0, 8)], even)
        got["last"] = links.send(parts.at[pl.ds(14, 2)], cores.at[pl.ds(6, 2)], CORE)
        got["mid"] = links.send(parts.at[pl.ds(10, 4)], cores.at[pl.ds(2, 4)], CORE)
        got["own"] = links.send(parts.at[pl.ds(8, 2)], cores.at[pl.ds(0, 2)], CORE)

    def corners():
        got["load"].wait()
        got["last"].wait_recv()
        even[6] = total(6).astype(BF)
        got["anf"] = links.send(even.at[6], taken.at[0], far)
        even[7] = total(7).astype(BF)
        got["bnf"] = links.send(even.at[7], taken.at[1], NEAR)
        got["mid"].wait_recv()
        even[4] = total(4).astype(BF)
        got["af"] = links.send(even.at[4], taken.at[2], far)
        even[3] = total(3).astype(BF)
        got["bn"] = links.send(even.at[3], taken.at[3], NEAR)

    def relay():
        got["anf"].wait_recv()
        even[2] = (total(2) + taken[0].astype(F32)).astype(BF)
        got["an"] = links.send(even.at[2], taken.at[4], NEAR)
        got["bnf"].wait_recv()
        even[5] = (total(5) + taken[1].astype(F32)).astype(BF)
        got["bf"] = links.send(even.at[5], taken.at[5], far)

    def end():
        got["own"].wait_recv()
        for name in ("af", "an"):
            got[name].wait_recv()
        finish(0, total(0) + taken[2].astype(F32) + taken[4].astype(F32))
        for name in ("bn", "bf"):
            got[name].wait_recv()
        finish(1, total(1) + taken[3].astype(F32) + taken[5].astype(F32))

    return [begin, corners, relay, end]


def scatter_steps_light(links, parts, even, cores, taken, finish):
    got = {}
    far = links.layout.far

    def total(block):
        return even[block].astype(F32) + cores[block].astype(F32)

    def begin():
        got["load"] = links.local(parts.at[pl.ds(0, 8)], even)
        got["last"] = links.send(parts.at[pl.ds(14, 2)], cores.at[pl.ds(6, 2)], CORE)
        got["mid"] = links.send(parts.at[pl.ds(10, 4)], cores.at[pl.ds(2, 4)], CORE)
        got["own"] = links.send(parts.at[pl.ds(8, 2)], cores.at[pl.ds(0, 2)], CORE)

    def corners():
        got["load"].wait()
        got["last"].wait_recv()
        for i in range(2):
            even[6 + i] = total(6 + i).astype(BF)
            got["nf", i] = links.send(even.at[6 + i], taken.at[i], NEAR)
        got["mid"].wait_recv()
        for i in range(2):
            even[2 + i] = total(2 + i).astype(BF)
            got["n", i] = links.send(even.at[2 + i], taken.at[2 + i], NEAR)

    def relay():
        for i in range(2):
            got["nf", i].wait_recv()
            even[4 + i] = (total(4 + i) + taken[i].astype(F32)).astype(BF)
            got["f", i] = links.send(even.at[4 + i], taken.at[4 + i], far)

    def end():
        got["own"].wait_recv()
        for i in range(2):
            got["n", i].wait_recv()
            got["f", i].wait_recv()
            finish(i, total(i) + taken[2 + i].astype(F32) + taken[4 + i].astype(F32))

    return [begin, corners, relay, end]


SCATTER_COPIES = 9


def scatter_scratch(half, width):
    return [
        pltpu.VMEM((8, half, width), BF),
        pltpu.VMEM((8, half, width), BF),
        pltpu.VMEM((6, half, width), BF),
    ]


def gather_stream(links, items, lag):
    layout = links.layout
    made = [{} for _ in items]

    def spread(i, rel, source):
        slot = items[i][2]
        for bit in range(layout.low(rel)):
            goal = rel | (1 << bit)
            made[i][goal] = links.send(source, slot(rel), layout.mask(1 << bit))

    def step(k):
        def run():
            if k < len(items):
                ready, own, _ = items[k]
                ready()
                spread(k, 0, own)
            if k >= lag:
                i = k - lag
                for rel in range(2, layout.reps, 2):
                    made[i][rel].wait_recv()
                    spread(i, rel, items[i][2](rel))

        return run

    def end():
        for copies in made:
            for rel in range(1, layout.reps, 2):
                copies[rel].wait_recv()

    return [step(k) for k in range(len(items) + lag)], end


def scatter_stream(links, items, window, lag):
    layout = links.layout
    made = [{} for _ in items]
    loads = [None for _ in items]
    stay = range(0, layout.reps, 2)

    def begin(i):
        part, keep, taken, _, paired = items[i]
        loads[i] = [links.local(part(rel), keep(rel // 2)) for rel in stay]
        for rel in range(layout.reps - 1, 0, -2):
            if not paired:
                made[i][rel] = links.send(part(rel), taken(rel - 1), layout.mask(rel))

    def total(i, rel):
        _, keep, taken, _, paired = items[i]
        sources = [source for source in layout.sources(rel) if not (paired and source & 1)]
        for source in sources:
            made[i][source].wait_recv()
        value = keep(rel // 2)[...].astype(F32)
        for source in sources:
            value = value + taken(source - 1)[...].astype(F32)
        return value

    def pass_on(i):
        _, keep, taken, _, paired = items[i]
        for load in loads[i]:
            load.wait()
        for rel in stay[:0:-1]:
            if not (paired and layout.low(rel) == 1):
                keep(rel // 2)[...] = total(i, rel).astype(BF)
            made[i][rel] = links.send(keep(rel // 2), taken(rel - 1), layout.mask(rel))

    def step(k):
        def run():
            if k < len(items):
                begin(k)
            if window <= k < len(items) + window:
                pass_on(k - window)
            if k >= window + lag:
                items[k - window - lag][3](total(k - window - lag, 0))

        return run

    return [step(k) for k in range(len(items) + window + lag)]


def pair_stream(links, items, window):
    layout = links.layout
    made = [{} for _ in items]

    def begin(i):
        part, keep, taken, _ = items[i]
        for k in range(layout.reps // 2):
            made[i][k] = (
                links.local(part(2 * k), keep(k)),
                links.send(part(2 * k + 1), taken(k), layout.mask(1)),
            )

    def end(i):
        _, keep, taken, finish = items[i]
        for k, (load, copy) in made[i].items():
            load.wait()
            copy.wait_recv()
            finish(k, keep(k)[...].astype(F32) + taken(k)[...].astype(F32))

    def step(k):
        def run():
            if k < len(items):
                begin(k)
            if k >= window:
                end(k - window)

        return run

    return [step(k) for k in range(len(items) + window)]


def interleave(stream, acts, first=1):
    acts = list(acts)
    for k, step in enumerate(stream):
        step()
        if k >= first and acts:
            acts.pop(0)()
    for act in acts:
        act()


def semaphores(copies, local_copies):
    return [
        pltpu.SemaphoreType.DMA((copies,)),
        pltpu.SemaphoreType.DMA((copies,)),
        pltpu.SemaphoreType.DMA((local_copies,)),
    ]


VMEM = pl.BlockSpec(memory_space=pltpu.VMEM)
HBM = pl.BlockSpec(memory_space=pl.ANY)


def kernel_params(call_id):
    return pltpu.CompilerParams(collective_id=call_id, has_side_effects=True)


def opening_kernel(
    layout, small, tokens, cot, query_w, key_w, value_w, gate_w, gate_src, up_src, out_src,
    small_all, x_all, cot_all, attn_w, gate_in, up_in, out_w,
    small_buf, gain_buf, normed_buf, attn_own, out_own, gate_own, up_own, send_sems, recv_sems, local_sems,
):
    links = Links(layout, send_sems, recv_sems, local_sems)
    device = links.device
    place, rep = layout.place(device), layout.rep(device)
    _, half, width = tokens.shape
    shard = layout.shard

    def place_at(mask):
        return layout.place(flip_device(device, mask)) if mask else place

    edges, columns = 0, []
    for weight in (query_w, key_w, value_w, gate_w):
        size = weight.shape[1] // HEADS
        columns.append((weight, size, edges))
        edges += size

    def column(weight, size, where):
        return weight.at[:, pl.ds(pl.multiple_of(where * size, LANES), size)]

    mine = links.local(small, small_buf.at[pl.ds(device, 1)])
    own_loads = [
        links.local(column(weight, size, place), attn_own.at[:, pl.ds(at, size)])
        for weight, size, at in columns
    ]
    out_load = links.local(out_src, out_own)
    gate_load = links.local(gate_src.at[place], gate_own)
    up_load = links.local(up_src.at[place], up_own)
    links.greet(layout.masks)
    mine.wait()

    def small_step(b):
        size = 1 << b
        part = small_buf.at[pl.ds((device // size) * size, size)]
        return links.send(part, part, size)

    attn_in, later_in = {}, []

    def attn_exchange(mask):
        attn_in[mask] = [
            links.send(
                column(weight, size, place_at(mask)),
                attn_w.at[rep, place, :, pl.ds(at, size)],
                mask,
            )
            for weight, size, at in columns
        ]

    def hidden_exchange(mask):
        for source, target in ((gate_src, gate_in), (up_src, up_in)):
            later_in.append(links.send(source.at[place_at(mask)], target.at[place], mask))

    small_copy = small_step(0)
    for mask in layout.team[:3]:
        attn_exchange(mask)
    for load in own_loads:
        load.wait()
    keeps = [links.local(attn_own, attn_w.at[rep, place])]

    def attn_item(mask):
        at = place_at(mask)

        def ready():
            for copy in attn_in.get(mask, ()):
                copy.wait_recv()

        own = attn_w.at[rep, at] if mask else attn_own
        return ready, own, lambda rel: attn_w.at[xor_index(rel, rep, layout.reps), at]

    def row_item(own, target, part):
        return (
            lambda: None,
            own.at[part],
            lambda rel: target.at[xor_index(rel, rep, layout.reps), part],
        )

    items = [attn_item(0)] + [row_item(out_own, out_w, part) for part in range(4)]
    items += [attn_item(mask) for mask in layout.team]
    out_load.wait()
    keeps.append(links.local(out_own, out_w.at[rep]))
    steps, stream_end = gather_stream(links, items, 3)
    steps[0]()
    for b in range(1, layout.bits):
        small_copy.wait_recv()
        small_copy = small_step(b)
        if b < 5:
            attn_exchange(layout.team[2 + b])
        if b == 2:
            steps[1]()
    steps[2]()
    small_copy.wait_recv()
    keeps.append(links.local(small_buf, small_all))

    per = LANES // shard
    for k in range(width // LANES):
        rows = small_buf[k * per].astype(F32)
        for i in range(1, per):
            rows = rows + small_buf[k * per + i].astype(F32)
        gain_buf[:, k * LANES : (k + 1) * LANES] = rows
    gain, shift = gain_buf[0:1, :], gain_buf[1:2, :]
    pieces = layout.pieces(width)

    def norm_rows(i, carry):
        part = i // (half // TILE)
        at = pl.ds(pl.multiple_of((i % (half // TILE)) * TILE, TILE), TILE)
        normed = layer_norm(tokens[part, at, :].astype(F32), gain, shift)
        normed_buf[part, at, :] = to_weight_order(normed, pieces).astype(BF)
        return carry

    lax.fori_loop(0, 2 * half // TILE, norm_rows, 0)
    keeps.append(links.local(normed_buf, x_all.at[pl.ds(0, 2)]))
    keeps.append(links.local(cot, cot_all.at[pl.ds(0, 2)]))
    for own, target, load in ((gate_own, gate_in, gate_load), (up_own, up_in, up_load)):
        load.wait()
        keeps.append(links.local(own, target.at[place]))

    def exchange_some(masks):
        return lambda: [hidden_exchange(mask) for mask in masks]

    x_steps = gather_steps_light(links, normed_buf, x_all)
    cot_steps = gather_steps_light(links, cot, cot_all)
    acts = x_steps[:1] + [lambda: None] + x_steps[1:2] + [lambda: None] + x_steps[2:]
    acts += [exchange_some(layout.team[:2]), exchange_some(layout.team[2:4])]
    acts += cot_steps[:1] + [exchange_some(layout.team[4:6])] + cot_steps[1:2]
    acts += [exchange_some(layout.team[6:])] + cot_steps[2:]
    interleave(steps[3:], acts, 0)
    stream_end()
    for copy in later_in:
        copy.wait_recv()
    for copy in keeps:
        copy.wait()
    links.finish()


def opening_call(layout, small, tokens, cot, attn_weights, gate_src, up_src, out_src):
    reps, shard = layout.reps, layout.shard
    rows, width = tokens.shape
    half = rows // 2
    attn_cols = sum(w.shape[1] for w in attn_weights) // HEADS
    ff_cols = gate_src.shape[2]
    out_shape = (4, out_src.shape[0] // 4, out_src.shape[1])
    copies = 7 * 4 + 7 * 2 + 12 * (reps - 1) + 2 * GATHER_COPIES + layout.bits
    return pl.pallas_call(
        functools.partial(opening_kernel, layout),
        out_shape=(
            jax.ShapeDtypeStruct((layout.count, 8, LANES), BF),
            jax.ShapeDtypeStruct((16, half, width), BF),
            jax.ShapeDtypeStruct((16, half, width), BF),
            jax.ShapeDtypeStruct((reps, 8, shard, attn_cols), BF),
            jax.ShapeDtypeStruct((8, shard, ff_cols), BF),
            jax.ShapeDtypeStruct((8, shard, ff_cols), BF),
            jax.ShapeDtypeStruct((reps,) + out_shape, BF),
        ),
        in_specs=[HBM, VMEM] + [HBM] * 8,
        out_specs=(HBM,) * 7,
        scratch_shapes=[
            pltpu.VMEM((layout.count, 8, LANES), BF),
            pltpu.VMEM((8, width), F32),
            pltpu.VMEM((2, half, width), BF),
            pltpu.VMEM((shard, attn_cols), BF),
            pltpu.VMEM(out_shape, BF),
            pltpu.VMEM((shard, ff_cols), BF),
            pltpu.VMEM((shard, ff_cols), BF),
        ]
        + semaphores(copies, 18),
        compiler_params=kernel_params(0),
        name="opening",
    )(
        small, tokens.reshape(2, half, width), cot.reshape(2, half, width), *attn_weights,
        gate_src, up_src, out_src.reshape(out_shape),
    )


def turn_kernel(
    layout, parts, tokens, gains, gate_in, up_in, down_in,
    hidden, all_rows, gate_w, up_w, down_w,
    even, cores, taken, normed_buf, send_sems, recv_sems, local_sems,
):
    links = Links(layout, send_sems, recv_sems, local_sems)
    rep = layout.rep(links.device)
    _, half, width = tokens.shape
    links.greet((CORE, NEAR, layout.far) + tuple(1 << b for b in layout.rep_bits))
    keeps = [links.local(gate_in, gate_w.at[rep]), links.local(up_in, up_w.at[rep])]
    downs = []
    for i in range(layout.reps // 2):
        slot = down_w.at[xor_index(2 * i, rep, layout.reps)]
        keeps.append(links.local(down_in.at[i], slot))
        downs.append(links.send(down_in.at[i], slot, layout.mask(1)))

    def item(own, target, part):
        at = pl.ds(part * 2, 2)
        return (
            lambda: None,
            own.at[at],
            lambda rel: target.at[xor_index(rel, rep, layout.reps), at],
        )

    items = [item(gate_in, gate_w, part) for part in range(4)]
    items += [item(up_in, up_w, part) for part in range(4)]
    steps, stream_end = gather_stream(links, items, 2)
    pieces = layout.pieces(width)

    def finish(part, value):
        hidden[part] = value + tokens[part].astype(F32)

        def norm_rows(i, carry):
            at = pl.ds(pl.multiple_of(i * TILE, TILE), TILE)
            normed = layer_norm(hidden[part, at, :], gains[0:1, :], gains[1:2, :])
            normed_buf[part, at, :] = to_weight_order(normed, pieces).astype(BF)
            return carry

        lax.fori_loop(0, half // TILE, norm_rows, 0)

    acts = scatter_steps_light(links, parts, even, cores, taken, finish)
    acts.append(lambda: keeps.append(links.local(normed_buf, all_rows.at[pl.ds(0, 2)])))
    acts += gather_steps_light(links, normed_buf, all_rows)
    acts.pop(0)()
    interleave(steps, acts, 0)
    stream_end()
    for copy in downs:
        copy.wait_recv()
    for copy in keeps:
        copy.wait()
    links.finish()


def turn_call(layout, parts, tokens, gains, gate_in, up_in, down_in):
    rows, width = tokens.shape
    half = rows // 2
    block = gate_in.shape
    return pl.pallas_call(
        functools.partial(turn_kernel, layout),
        out_shape=(
            jax.ShapeDtypeStruct((2, half, width), F32),
            jax.ShapeDtypeStruct((16, half, width), BF),
            jax.ShapeDtypeStruct((layout.reps,) + block, BF),
            jax.ShapeDtypeStruct((layout.reps,) + block, BF),
            jax.ShapeDtypeStruct((layout.reps,) + down_in.shape[1:], BF),
        ),
        in_specs=[HBM, VMEM, VMEM, VMEM, VMEM, VMEM],
        out_specs=(VMEM, HBM, HBM, HBM, HBM),
        scratch_shapes=scatter_scratch(half, width)
        + [pltpu.VMEM((2, half, width), BF)]
        + semaphores(
            8 * (layout.reps - 1) + layout.reps // 2 + SCATTER_COPIES + GATHER_COPIES,
            5 + layout.reps // 2,
        ),
        compiler_params=kernel_params(1),
        name="turn",
    )(parts.reshape(16, half, width), tokens.reshape(2, half, width), gains, gate_in, up_in, down_in)


def turn_back_kernel(
    layout, parts, hidden, out_grad, gains, down_p, gate_p,
    hidden_grad, all_rows, vectors, down_first, down_rest, gate_first, gate_rest,
    even, cores, taken, low_buf, sum_buf, down_l, down_y, gate_l, gate_y,
    send_sems, recv_sems, local_sems,
):
    links = Links(layout, send_sems, recv_sems, local_sems)
    rep = layout.rep(links.device)
    _, half, width = hidden.shape
    links.greet((CORE, NEAR, layout.far) + tuple(1 << b for b in layout.rep_bits))

    def item(part, keep, taken, at, first, rest):
        def finish(k, value):
            if k:
                rest[k - 1, at] = value.astype(rest.dtype)
            else:
                first[at] = value.astype(first.dtype)

        return (
            lambda rel: part.at[xor_index(rel, rep, layout.reps), at],
            lambda k: keep.at[k, at],
            lambda k: taken.at[k, at],
            finish,
        )

    pairs = [pl.ds(2 * part, 2) for part in range(4)]
    items = [item(down_p, down_l, down_y, at, down_first, down_rest) for at in range(4)]
    items += [item(gate_p, gate_l, gate_y, at, gate_first, gate_rest) for at in pairs]
    steps = pair_stream(links, items, 3)
    pieces = layout.pieces(width)
    vectors[...] = jnp.zeros_like(vectors)

    def finish(part, value):
        sum_buf[...] = value

        def rows(i, carry):
            at = pl.ds(pl.multiple_of(i * TILE, TILE), TILE)
            grads = from_weight_order(sum_buf[at, :], pieces)
            back, gain_part, shift_part = layer_norm_back(
                hidden[part, at, :], gains[0:1, :], grads
            )
            total = out_grad[part, at, :].astype(F32) + back
            hidden_grad[part, at, :] = total
            low_buf[part, at, :] = total.astype(BF)
            vectors[0:1, :] += gain_part
            vectors[1:2, :] += shift_part
            return carry

        lax.fori_loop(0, half // TILE, rows, 0)

    keeps = []
    acts = scatter_steps(links, parts, even, cores, taken, finish)
    acts.append(lambda: keeps.append(links.local(low_buf, all_rows.at[pl.ds(0, 2)])))
    acts += gather_steps(links, low_buf, all_rows)
    acts.pop(0)()
    interleave(steps, acts, 0)
    for copy in keeps:
        copy.wait()
    links.finish()


def replica_items(layout, rep, part, keep, taken, places, sums, paired=False):
    def item(at):
        def finish(value):
            sums[at] = value.astype(sums.dtype)

        return (
            lambda rel: part.at[rel // 2 if paired else xor_index(rel, rep, layout.reps), at],
            lambda i: keep.at[i, at],
            lambda i: taken.at[i, at],
            finish,
            paired,
        )

    return [item(at) for at in places]


def turn_back_call(layout, parts, hidden, out_grad, gains, down_p, gate_p):
    half, width = hidden.shape[1:]
    reps = layout.reps
    down_block, gate_block = down_p.shape[1:], gate_p.shape[1:]
    return pl.pallas_call(
        functools.partial(turn_back_kernel, layout),
        out_shape=(
            jax.ShapeDtypeStruct((2, half, width), F32),
            jax.ShapeDtypeStruct((16, half, width), BF),
            jax.ShapeDtypeStruct((8, width), F32),
            jax.ShapeDtypeStruct(down_block, F32),
            jax.ShapeDtypeStruct((reps // 2 - 1,) + down_block, BF),
            jax.ShapeDtypeStruct(gate_block, F32),
            jax.ShapeDtypeStruct((reps // 2 - 1,) + gate_block, BF),
        ),
        in_specs=[HBM, VMEM, VMEM, VMEM, HBM, HBM],
        out_specs=(VMEM, HBM, VMEM, VMEM, VMEM, VMEM, VMEM),
        scratch_shapes=scatter_scratch(half, width)
        + [
            pltpu.VMEM((2, half, width), BF),
            pltpu.VMEM((half, width), F32),
            pltpu.VMEM((reps // 2,) + down_block, BF),
            pltpu.VMEM((reps // 2,) + down_block, BF),
            pltpu.VMEM((reps // 2,) + gate_block, BF),
            pltpu.VMEM((reps // 2,) + gate_block, BF),
        ]
        + semaphores(4 * reps + SCATTER_COPIES + GATHER_COPIES, 4 * reps + 2),
        compiler_params=kernel_params(2),
        name="turn_back",
    )(
        parts.reshape(16, half, width), hidden, out_grad.reshape(2, half, width), gains,
        down_p, gate_p,
    )


def closing_kernel(
    layout, attn_p, up_p, out_p, gate_sum, one_parts, two_parts, tokens, hidden_grad, gains, vectors,
    query_back, key_back, value_back, swish_back, gate_back, up_back, out_sum, branch_two,
    tokens_grad, vector_sum,
    even_1, cores_1, taken_1, even_2, cores_2, taken_2, sum_buf, rows_buf, vec_l, vec_y,
    attn_l, attn_y, attn_s, up_l, up_y, up_s, out_l, out_y, send_sems, recv_sems, local_sems,
):
    links = Links(layout, send_sems, recv_sems, local_sems)
    device = links.device
    place, rep = layout.place(device), layout.rep(device)
    _, half, width = tokens.shape
    links.greet(layout.masks)
    backs, kept = [], []

    def place_at(mask):
        return layout.place(flip_device(device, mask)) if mask else place

    def give(source, target, mask):
        if mask:
            backs.append(links.send(source, target, mask))
        else:
            kept.append(links.local(source, target))

    edges, columns = 0, []
    for target in (query_back, key_back, value_back, swish_back):
        size = target.shape[1] // HEADS
        columns.append((target, size, edges))
        edges += size

    def with_return(item, mask, give_back):
        part, keep, taken, finish, paired = item

        def finish_and_give(value):
            finish(value)
            give_back(mask)

        return part, keep, taken, finish_and_give, paired

    def attn_return(mask):
        for target, size, at in columns:
            goal = pl.ds(pl.multiple_of(place * size, LANES), size)
            give(attn_s.at[place_at(mask), :, pl.ds(at, size)], target.at[:, goal], mask)

    def up_return(mask):
        give(up_s.at[place_at(mask)], up_back.at[place], mask)

    order = layout.team[::-1] + (0,)
    items = []
    for part, keep, taken, sums, give_back, paired in (
        (attn_p, attn_l, attn_y, attn_s, attn_return, False),
        (up_p, up_l, up_y, up_s, up_return, False),
    ):
        places = [place_at(m) for m in order]
        plain = replica_items(layout, rep, part, keep, taken, places, sums, paired)
        items += [with_return(item, m, give_back) for item, m in zip(plain, order)]
    items += replica_items(layout, rep, out_p, out_l, out_y, range(4), out_sum)
    steps = scatter_stream(links, items, 2, 2)

    pieces = layout.pieces(width)
    rows_buf[...] = jnp.zeros_like(rows_buf)
    rows_buf[2:4, :] = vectors[0:2, :]

    def finish_one(part, value):
        sum_buf[...] = value

        def rows(i, carry):
            at = pl.ds(pl.multiple_of(i * TILE, TILE), TILE)
            grads = from_weight_order(sum_buf[at, :], pieces)
            back, gain_part, shift_part = layer_norm_back(
                tokens[part, at, :].astype(F32), gains[0:1, :], grads
            )
            tokens_grad[part, at, :] = hidden_grad[part, at, :] + back
            rows_buf[0:1, :] += gain_part
            rows_buf[1:2, :] += shift_part
            return carry

        lax.fori_loop(0, half // TILE, rows, 0)

    def finish_two(part, value):
        branch_two[part] = value

    per = LANES // layout.shard
    own_bits = per.bit_length() - 1
    slots = layout.count // per
    flight = {}

    def vector_begin():
        for slot in range(slots):
            vec_l[slot] = rows_buf[:, slot * LANES : (slot + 1) * LANES]

    def vector_send(b):
        def run():
            peer = flip_device(device, 1 << b)
            if b >= own_bits:
                size = 1 << (b - own_bits)
                source = vec_l.at[pl.ds((peer // (1 << b)) * size, size)]
                target = vec_y.at[pl.ds(size, size)]
            else:
                source = vec_l.at[pl.ds(device // per, 1)]
                target = vec_y.at[pl.ds(slots + b, 1)]
            flight[b] = links.send(source, target, 1 << b)

        return run

    def vector_add(b):
        def run():
            if b >= own_bits:
                size = 1 << (b - own_bits)
                flight[b].wait_recv()
                mine = pl.ds((device // (1 << b)) * size, size)
                vec_l[mine] = vec_l[mine] + vec_y[size : 2 * size]
            else:
                links.swap_done(flight[b])
                mine = pl.ds(device // per, 1)
                vec_l[mine] = vec_l[mine] + vec_y[slots + b : slots + b + 1]

        return run

    def gate_return():
        for mask in layout.team + (0,):
            give(gate_sum.at[place_at(mask)], gate_back.at[place], mask)

    one = scatter_steps_light(links, one_parts, even_1, cores_1, taken_1, finish_one)
    two = scatter_steps_light(links, two_parts, even_2, cores_2, taken_2, finish_two)
    acts = one[1:] + [vector_begin]
    down_bits = list(range(layout.bits))[::-1]
    together = [(lambda b=b, a=a: ((a() if a else None), vector_send(b)())) for a, b in zip(
        [None] + [vector_add(b) for b in down_bits[:-1]], down_bits)]
    acts += [lambda: (together[0](), two[0](), gate_return())]
    for k in range(1, layout.bits):
        extra = two[k] if k < len(two) else (lambda: None)
        acts.append(lambda k=k, extra=extra: (together[k](), extra()))
    acts += two[layout.bits :] + [vector_add(down_bits[-1])]
    one[0]()
    interleave(steps, acts, 0)
    vector_sum[...] = vec_l[device // per]
    for copy in backs:
        copy.wait_recv()
    for copy in kept:
        copy.wait()
    links.finish()


def closing_call(layout, attn_p, up_p, out_p, gate_sum, one_parts, two_parts, tokens, hidden_grad,
                 gains, vectors, back_widths):
    reps, shard = layout.reps, layout.shard
    half, width = hidden_grad.shape[1:]
    attn_block, up_block, out_block = attn_p.shape[1:], up_p.shape[1:], out_p.shape[1:]
    per = LANES // shard
    slots = layout.count // per
    stay = reps // 2
    rows = jax.ShapeDtypeStruct((2, half, width), F32)
    copies = 20 * (reps - 1) + 7 * 6 + 2 * SCATTER_COPIES + layout.bits
    return pl.pallas_call(
        functools.partial(closing_kernel, layout),
        out_shape=tuple(jax.ShapeDtypeStruct((shard, w), BF) for w in back_widths)
        + (
            jax.ShapeDtypeStruct(up_block, BF),
            jax.ShapeDtypeStruct(up_block, BF),
            jax.ShapeDtypeStruct(out_block, F32),
            rows,
            rows,
            jax.ShapeDtypeStruct((8, LANES), F32),
        ),
        in_specs=[HBM, HBM, HBM, VMEM, HBM, HBM, VMEM, VMEM, VMEM, VMEM],
        out_specs=(HBM,) * 6 + (VMEM,) * 4,
        scratch_shapes=scatter_scratch(half, width)
        + scatter_scratch(half, width)
        + [
            pltpu.VMEM((half, width), F32),
            pltpu.VMEM((8, width), F32),
            pltpu.VMEM((slots, 8, LANES), F32),
            pltpu.VMEM((slots + per, 8, LANES), F32),
            pltpu.VMEM((stay,) + attn_block, BF),
            pltpu.VMEM((reps - 1,) + attn_block, BF),
            pltpu.VMEM(attn_block, BF),
            pltpu.VMEM((stay,) + up_block, BF),
            pltpu.VMEM((reps - 1,) + up_block, BF),
            pltpu.VMEM(up_block, BF),
            pltpu.VMEM((stay,) + out_block, BF),
            pltpu.VMEM((reps - 1,) + out_block, BF),
        ]
        + semaphores(copies, 20 * stay + 8),
        compiler_params=kernel_params(3),
        name="closing",
    )(
        attn_p, up_p, out_p, gate_sum, one_parts.reshape(16, half, width),
        two_parts.reshape(16, half, width), tokens.reshape(2, half, width), hidden_grad, gains, vectors,
    )


def seq_layout(seq_lens, row_count):
    row_ids = jnp.arange(row_count, dtype=jnp.int32)
    seq_ends = jnp.cumsum(seq_lens)
    passed = row_ids[:, None] >= seq_ends[None, :]
    segment = jnp.sum(passed.astype(jnp.int32), axis=1)
    seq_start = jnp.sum(jnp.where(passed, seq_lens[None, :], 0), axis=1)
    position = row_ids - seq_start
    live_rows = row_ids < seq_ends[-1]
    return (segment, position, live_rows)


def group_norm(values):
    center = values - jnp.mean(values, axis=-1, keepdims=True)
    spread = jnp.mean(center * center, axis=-1, keepdims=True)
    return center * lax.rsqrt(spread + GROUP_EPS)


def dot(left, right):
    return jnp.dot(left, right, preferred_element_type=F32)


def dot_nt(left, right):
    return lax.dot_general(left, right, (((1,), (1,)), ((), ())), preferred_element_type=F32)


def dot_tn(left, right):
    return lax.dot_general(left, right, (((0,), (0,)), ((), ())), preferred_element_type=F32)


def make_body(count):
    def on_device(
        tokens,
        seq_lengths,
        attn_gain,
        attn_shift,
        query_weight,
        key_weight,
        value_weight,
        gate_weight,
        out_weight,
        mlp_gain,
        mlp_shift,
        mlp_gate,
        mlp_up,
        mlp_down,
        cotangent,
    ):
        local_rows, width = tokens.shape
        shard = width // count
        layout = Layout(count, shard)
        reps = layout.reps
        device = lax.axis_index("dp")
        rep, pos_t = layout.rep(device), layout.place(device)
        micro_count, seq_slots = seq_lengths.shape[1:]
        row_count = local_rows // micro_count
        key_size = query_weight.shape[1] // HEADS
        value_size = value_weight.shape[1] // HEADS
        hidden_size = mlp_gate.shape[1]
        ff_block = hidden_size // count
        group_rows = 8 * local_rows
        home = [layout.device(d % reps, d // reps) for d in range(count)]
        head_perm = [(d, home[d]) for d in range(count)]
        head_back = [(b, a) for a, b in head_perm]

        high, mid = 1 << (layout.bits - 1 - layout.far_bit), 1 << (layout.far_bit - 2)

        def ff_first(weight):
            v = weight.reshape(shard, high, 2, mid, 4, ff_block)
            return v.transpose(2, 4, 0, 1, 3, 5).reshape(8, shard, reps * ff_block)

        def ff_back(grad):
            v = grad.reshape(2, 4, shard, high, mid, ff_block)
            return v.transpose(2, 3, 0, 4, 1, 5).reshape(shard, hidden_size)

        per = LANES // shard
        lane_on = jnp.arange(LANES, dtype=jnp.int32) // shard == device % per

        def in_lanes(values):
            return jnp.where(lane_on, jnp.tile(values, per), jnp.zeros((), BF))[None]

        own_lens = seq_lengths.reshape(-1).astype(BF)
        small = jnp.concatenate(
            [in_lanes(v) for v in (attn_gain, attn_shift, mlp_gain, mlp_shift)]
            + [jnp.pad(own_lens, (0, LANES - own_lens.shape[0]))[None], jnp.zeros((3, LANES), BF)]
        )
        own_live = jax.vmap(lambda v: seq_layout(v, row_count)[2])(seq_lengths[0])
        own_live = own_live.reshape(local_rows).astype(F32)[:, None]
        out_grad_low = (cotangent.astype(F32) * own_live).astype(BF)

        out_own = lax.ppermute(out_weight, "dp", head_perm)
        small, normed_one, cot_all, attn_w, gate_in, up_in, out_w = opening_call(
            layout, small[None], tokens, out_grad_low,
            (query_weight, key_weight, value_weight, gate_weight),
            ff_first(mlp_gate), ff_first(mlp_up), out_own,
        )
        normed_one = normed_one.reshape(group_rows, width)
        cot_all = cot_all.reshape(group_rows, width)
        attn_w = attn_w.reshape(width, -1)
        out_w = out_w.reshape(-1, width)

        def flip_rep(values, bit):
            mask = 1 << layout.rep_bits[bit]
            return lax.ppermute(values, "dp", [(d, d ^ mask) for d in range(count)])

        down_even = [lax.optimization_barrier((mlp_down, small))[0]]
        for k in range(1, reps // 2):
            low = layout.low(k)
            down_even.append(flip_rep(down_even[k & ~(1 << low)], low + 1))

        def finish_pairs(first, rest):
            sums = [first] + [rest[k] for k in range(reps // 2 - 1)]
            for k in range(reps // 2 - 1, 0, -1):
                low = layout.low(k)
                got = flip_rep(sums[k].astype(BF), low + 1).astype(F32)
                sums[k & ~(1 << low)] = sums[k & ~(1 << low)].astype(F32) + got
            return sums[0]

        vecs = small[:, :4, :].astype(F32).reshape(-1, per, 4, LANES).sum(1)
        vecs = vecs.transpose(1, 0, 2).reshape(4, width)
        gains_one = jnp.pad(vecs[:2], ((0, 6), (0, 0)))
        gains_two = jnp.pad(vecs[2:], ((0, 6), (0, 0)))
        lens = small[:, 4, : own_lens.shape[0]].astype(jnp.int32)
        order = [c + 2 * n + 4 * f for c in range(2) for f in range(2) for n in range(2)]
        members = jnp.stack(
            [flip_device(device, (j & 3) + (j >> 2) * layout.far) for j in order]
        )
        lens = jnp.take(lens, members, axis=0).reshape(8 * micro_count, seq_slots)

        segment, position, live = jax.vmap(lambda s: seq_layout(s, row_count))(lens)
        head_log = jnp.log(1.0 - 2.0 ** (-5.0 - jnp.arange(HEADS, dtype=F32)))
        head_log = lax.dynamic_index_in_dim(head_log, pos_t, 0, keepdims=False)
        ids = jnp.arange(row_count, dtype=jnp.int32)
        same_seq = (
            (segment[:, :, None] == segment[:, None, :])
            & live[:, :, None]
            & live[:, None, :]
            & (ids[:, None] >= ids[None, :])[None]
        )
        distance = jnp.maximum(position[:, :, None] - position[:, None, :], 0).astype(F32)
        decay = jnp.where(same_seq, jnp.exp(distance * head_log), 0.0)
        half_size = key_size // 2
        pair_index = jnp.arange(half_size, dtype=F32)
        frequency = 10000.0 ** (-pair_index / half_size)
        row_place = position.reshape(-1).astype(F32)[:, None]
        angles = row_place * frequency[None, :]
        growth = (pair_index * 2.0 / key_size + 0.4) / 1.4
        stretch = growth[None, :] ** (row_place / 512.0)
        key_factor = key_size ** (-0.5) / stretch
        cosine, sine, stretch, key_factor = lax.optimization_barrier(
            (jnp.cos(angles), jnp.sin(angles), stretch, key_factor)
        )

        def rotate(values, factor):
            a, b = values[:, :half_size], values[:, half_size:]
            return jnp.concatenate(
                [(a * cosine - b * sine) * factor, (b * cosine + a * sine) * factor], axis=1
            )

        def rotate_back(grads, factor):
            a, b = grads[:, :half_size] * factor, grads[:, half_size:] * factor
            return jnp.concatenate([a * cosine + b * sine, b * cosine - a * sine], axis=1)

        def micro(values):
            return values.reshape(-1, row_count, values.shape[-1])

        qkvg = dot(normed_one, attn_w)
        query_raw = qkvg[:, :key_size]
        key_raw = qkvg[:, key_size : 2 * key_size]
        value_low = qkvg[:, 2 * key_size : 2 * key_size + value_size].astype(BF)
        gate_raw = qkvg[:, 2 * key_size + value_size :]
        query_turned = micro(rotate(query_raw, stretch).astype(BF))
        key_turned = micro(rotate(key_raw, key_factor).astype(BF))
        value_m = micro(value_low)
        scores = jnp.einsum("mqd,mkd->mqk", query_turned, key_turned, preferred_element_type=F32)
        weights_low = (scores * decay).astype(BF)
        retained = jnp.einsum("mqk,mke->mqe", weights_low, value_m, preferred_element_type=F32)
        retained = retained.reshape(group_rows, value_size)

        def mix(gate_in, retained_in):
            return jax.nn.silu(gate_in) * group_norm(retained_in)

        mixed = mix(gate_raw, retained).astype(BF)
        hidden, normed_two, gate_w, up_w, down_w = turn_call(
            layout, dot(mixed, out_w).astype(BF), tokens, gains_two, gate_in, up_in,
            jnp.stack(down_even),
        )
        down_w = down_w.reshape(-1, width)
        normed_two = normed_two.reshape(group_rows, width)
        gate_w, up_w = gate_w.reshape(width, -1), up_w.reshape(width, -1)

        def act(gate_in, up_in):
            return jax.nn.gelu(gate_in, approximate=True) * up_in

        product, pull_act = jax.vjp(act, dot(normed_two, gate_w), dot(normed_two, up_w))
        product = product.astype(BF)
        gate_low, up_low = (g.astype(BF) for g in pull_act(dot_nt(cot_all, down_w)))
        two_parts = dot(product, down_w).astype(BF)
        down_parts = dot_tn(product, cot_all).astype(BF)
        gate_parts = dot_tn(normed_two, gate_low).astype(BF)
        up_parts = dot_tn(normed_two, up_low).astype(BF)
        normed_parts = (dot_nt(gate_low, gate_w) + dot_nt(up_low, up_w)).astype(BF)
        hidden_grad, branch_one_grad, vectors, down_first, down_rest, gate_first, gate_rest = turn_back_call(
            layout, normed_parts, hidden, out_grad_low, gains_two,
            down_parts.reshape(reps, 4, -1, width), gate_parts.reshape(reps, 8, shard, -1),
        )
        branch_one_grad = branch_one_grad.reshape(group_rows, width)
        gate_sum = finish_pairs(gate_first, gate_rest).astype(BF)
        mlp_down_grad = finish_pairs(down_first, down_rest)

        mixed_grad = dot_nt(branch_one_grad, out_w)
        _, pull_mix = jax.vjp(mix, gate_raw, retained)
        gate_grad, retained_grad = pull_mix(mixed_grad)
        gate_grad = gate_grad.astype(BF)
        retained_low = micro(retained_grad.astype(BF))
        weights_grad = jnp.einsum("mqe,mke->mqk", retained_low, value_m, preferred_element_type=F32)
        value_grad = jnp.einsum(
            "mqk,mqe->mke", weights_low, retained_low, preferred_element_type=F32
        )
        value_grad = value_grad.reshape(group_rows, value_size).astype(BF)
        score_low = (weights_grad * decay).astype(BF)
        query_turn_grad = jnp.einsum("mqk,mkd->mqd", score_low, key_turned, preferred_element_type=F32)
        key_turn_grad = jnp.einsum("mqk,mqd->mkd", score_low, query_turned, preferred_element_type=F32)
        query_grad = rotate_back(query_turn_grad.reshape(group_rows, key_size), stretch).astype(BF)
        key_grad = rotate_back(key_turn_grad.reshape(group_rows, key_size), key_factor).astype(BF)
        attn_grads = jnp.concatenate([query_grad, key_grad, value_grad, gate_grad], axis=1)
        attn_parts = dot_tn(normed_one, attn_grads).astype(BF)
        out_parts = dot_tn(mixed, branch_one_grad).astype(BF)
        one_parts = dot_nt(attn_grads, attn_w).astype(BF)
        q_back, k_back, v_back, g_back, gate_back, up_back, out_sum, branch_two, tokens_grad, vectors = (
            closing_call(
                layout,
                attn_parts.reshape(reps, 8, shard, -1),
                up_parts.reshape(reps, 8, shard, -1),
                out_parts.reshape(reps, 4, -1, width),
                gate_sum, one_parts, two_parts, tokens, hidden_grad, gains_one, vectors,
                [w.shape[1] for w in (query_weight, key_weight, value_weight, gate_weight)],
            )
        )
        out_sum = out_sum.reshape(out_weight.shape).astype(BF)
        out_weight_grad = lax.ppermute(out_sum, "dp", head_back).astype(F32)
        output = ((hidden + branch_two).reshape(local_rows, width) * own_live).astype(BF)
        vectors = lax.dynamic_slice_in_dim(vectors, (device % per) * shard, shard, axis=1)
        return (
            output,
            tokens_grad.reshape(local_rows, width),
            vectors[0],
            vectors[1],
            q_back.astype(F32),
            k_back.astype(F32),
            v_back.astype(F32),
            g_back.astype(F32),
            out_weight_grad,
            vectors[2],
            vectors[3],
            ff_back(gate_back.astype(F32)),
            ff_back(up_back.astype(F32)),
            mlp_down_grad.reshape(mlp_down.shape),
        )

    return on_device


def solution(mesh):
    rows = P("dp", None)
    vec = P("dp")
    placed = (
        rows, P("dp", None, None), vec, vec, rows, rows, rows, rows, rows,
        vec, vec, rows, rows, rows, rows,
    )
    outs = (rows, rows, vec, vec, rows, rows, rows, rows, rows, vec, vec, rows, rows, rows)
    return jax.shard_map(
        make_body(mesh.shape["dp"]), mesh=mesh, in_specs=placed, out_specs=outs, check_vma=False
    )
```

```python
import functools

import jax
import jax.numpy as jnp
from jax import lax
from jax.experimental import pallas as pl
from jax.experimental.pallas import tpu as pltpu
from jax.sharding import PartitionSpec as P


HEADS = 8
NORM_EPS = 1e-05
GROUP_EPS = 1.0
BF = jnp.bfloat16
F32 = jnp.float32
MESH = pl.DeviceIdType.MESH
LANES = 128


CORE, NEAR = 1, 2
TILE = 16


class Layout:
    def __init__(self, count, shard):
        self.count, self.shard = count, shard
        self.far_bit = 3 if (4 * shard) % LANES == 0 and count >= 32 else 2
        self.far = 1 << self.far_bit
        self.bits = count.bit_length() - 1
        self.rep_bits = [b for b in range(2, self.bits) if b != self.far_bit]
        self.reps = count // 8
        self.team = (CORE, NEAR, self.far, CORE | NEAR, CORE | self.far, NEAR | self.far,
                     CORE | NEAR | self.far)
        self.masks = self.team + tuple(
            1 << b for b in range(self.bits) if (1 << b) not in self.team
        )

    def place(self, device):
        return ((device // self.far) % 2) * 4 + device % 4

    def rep(self, device):
        total = 0
        for i, b in enumerate(self.rep_bits):
            total = total + ((device // (1 << b)) % 2) * (1 << i)
        return total

    def device(self, rep, place):
        total = place % 4 + (place // 4) * self.far
        for i, b in enumerate(self.rep_bits):
            total += ((rep >> i) & 1) << b
        return total

    def low(self, rel):
        return (rel & -rel).bit_length() - 1 if rel else len(self.rep_bits)

    def mask(self, rel):
        return 1 << self.rep_bits[self.low(rel)]

    def sources(self, rel):
        return [rel | (1 << i) for i in range(self.low(rel))]

    def pieces(self, width):
        if self.far_bit == 2:
            return [(0, width)]
        size = 4 * self.shard
        order = []
        for hi in range(self.count // 16):
            for b2 in range(2):
                for b3 in range(2):
                    order.append(((hi * 4 + b3 * 2 + b2) * size, size))
        return order


def flip_device(device, mask):
    other, bit = device, 0
    while mask >> bit:
        if (mask >> bit) & 1:
            other = other + (1 - 2 * ((device // (1 << bit)) % 2)) * (1 << bit)
        bit += 1
    return other


def xor_index(static, own, size):
    total, bit = 0, 1
    while bit < size:
        own_bit = (own // bit) % 2
        total = total + bit * (1 - own_bit if static & bit else own_bit)
        bit *= 2
    return total


def layer_norm(values, gain_vec, shift_vec):
    center = values - jnp.mean(values, axis=-1, keepdims=True)
    spread = jnp.mean(center * center, axis=-1, keepdims=True)
    return center * lax.rsqrt(spread + NORM_EPS) * gain_vec + shift_vec


def layer_norm_back(values, gain_vec, grads):
    center = values - jnp.mean(values, axis=-1, keepdims=True)
    scale = lax.rsqrt(jnp.mean(center * center, axis=-1, keepdims=True) + NORM_EPS)
    z = center * scale
    e = grads * gain_vec
    part = scale * (
        e - jnp.mean(e, axis=-1, keepdims=True) - z * jnp.mean(e * z, axis=-1, keepdims=True)
    )
    gain_part = jnp.sum(grads * z, axis=0, keepdims=True)
    shift_part = jnp.sum(grads, axis=0, keepdims=True)
    return part, gain_part, shift_part


def to_weight_order(values, pieces):
    return jnp.concatenate([values[:, at : at + size] for at, size in pieces], axis=1)


def from_weight_order(values, pieces):
    size = pieces[0][1]
    where = {at: i * size for i, (at, _) in enumerate(pieces)}
    return jnp.concatenate([values[:, where[at] : where[at] + size] for at in sorted(where)], axis=1)


class Links:
    def __init__(self, layout, send_sems, recv_sems, local_sems):
        self.layout = layout
        self.device = lax.axis_index("dp")
        self.send_sems, self.recv_sems, self.local_sems = send_sems, recv_sems, local_sems
        self.made, self.locals, self.sent = [], [], []

    def greet(self, masks):
        barrier = pltpu.get_barrier_semaphore()
        for mask in masks:
            pl.semaphore_signal(
                barrier, inc=1, device_id=(flip_device(self.device, mask),), device_id_type=MESH
            )
        pl.semaphore_wait(barrier, len(masks))

    def send(self, source, target, mask):
        index = len(self.made)
        copy = pltpu.make_async_remote_copy(
            src_ref=source,
            dst_ref=target,
            send_sem=self.send_sems.at[index],
            recv_sem=self.recv_sems.at[index],
            device_id=(flip_device(self.device, mask),),
            device_id_type=MESH,
        )
        copy.start()
        self.made.append(copy)
        return copy

    def local(self, source, target):
        copy = pltpu.make_async_copy(source, target, self.local_sems.at[len(self.locals)])
        copy.start()
        self.locals.append(copy)
        return copy

    def swap_done(self, copy):
        copy.wait()
        self.sent.append(copy)

    def finish(self):
        for copy in self.made:
            if not any(copy is other for other in self.sent):
                copy.wait_send()


def gather_steps(links, own, out):
    got = {}
    far = links.layout.far

    def begin():
        got["an"] = links.send(own.at[0], out.at[2], NEAR)
        got["bf"] = links.send(own.at[1], out.at[5], far)
        got["bn"] = links.send(own.at[1], out.at[3], NEAR)
        got["af"] = links.send(own.at[0], out.at[4], far)
        got["c"] = [links.send(own.at[i], out.at[8 + i], CORE) for i in range(2)]

    def relay():
        got["an"].wait_recv()
        got["anf"] = links.send(out.at[2], out.at[6], far)
        got["c"].append(links.send(out.at[2], out.at[10], CORE))
        got["bf"].wait_recv()
        got["bnf"] = links.send(out.at[5], out.at[7], NEAR)
        got["c"].append(links.send(out.at[5], out.at[13], CORE))
        got["bn"].wait_recv()
        got["c"].append(links.send(out.at[3], out.at[11], CORE))
        got["af"].wait_recv()
        got["c"].append(links.send(out.at[4], out.at[12], CORE))

    def end():
        got["anf"].wait_recv()
        got["c"].append(links.send(out.at[6], out.at[14], CORE))
        got["bnf"].wait_recv()
        got["c"].append(links.send(out.at[7], out.at[15], CORE))
        for copy in got["c"]:
            copy.wait_recv()

    return [begin, relay, end]


def gather_steps_light(links, own, out):
    got = {}
    far = links.layout.far

    def begin():
        got["af"] = links.send(own.at[0], out.at[4], far)
        got["bf"] = links.send(own.at[1], out.at[5], far)
        got["an"] = links.send(own.at[0], out.at[2], NEAR)
        got["bn"] = links.send(own.at[1], out.at[3], NEAR)
        got["c"] = [links.send(own.at[i], out.at[8 + i], CORE) for i in range(2)]

    def relay():
        for i, name in enumerate(("af", "bf")):
            got[name].wait_recv()
            got[name + "n"] = links.send(out.at[4 + i], out.at[6 + i], NEAR)
            got["c"].append(links.send(out.at[4 + i], out.at[12 + i], CORE))
        for i, name in enumerate(("an", "bn")):
            got[name].wait_recv()
            got["c"].append(links.send(out.at[2 + i], out.at[10 + i], CORE))

    def end():
        for i, name in enumerate(("afn", "bfn")):
            got[name].wait_recv()
            got["c"].append(links.send(out.at[6 + i], out.at[14 + i], CORE))
        for copy in got["c"]:
            copy.wait_recv()

    return [begin, relay, end]


GATHER_COPIES = 14


def scatter_steps(links, parts, even, cores, taken, finish):
    got = {}
    far = links.layout.far

    def total(block):
        return even[block].astype(F32) + cores[block].astype(F32)

    def begin():
        got["load"] = links.local(parts.at[pl.ds(0, 8)], even)
        got["last"] = links.send(parts.at[pl.ds(14, 2)], cores.at[pl.ds(6, 2)], CORE)
        got["mid"] = links.send(parts.at[pl.ds(10, 4)], cores.at[pl.ds(2, 4)], CORE)
        got["own"] = links.send(parts.at[pl.ds(8, 2)], cores.at[pl.ds(0, 2)], CORE)

    def corners():
        got["load"].wait()
        got["last"].wait_recv()
        even[6] = total(6).astype(BF)
        got["anf"] = links.send(even.at[6], taken.at[0], far)
        even[7] = total(7).astype(BF)
        got["bnf"] = links.send(even.at[7], taken.at[1], NEAR)
        got["mid"].wait_recv()
        even[4] = total(4).astype(BF)
        got["af"] = links.send(even.at[4], taken.at[2], far)
        even[3] = total(3).astype(BF)
        got["bn"] = links.send(even.at[3], taken.at[3], NEAR)

    def relay():
        got["anf"].wait_recv()
        even[2] = (total(2) + taken[0].astype(F32)).astype(BF)
        got["an"] = links.send(even.at[2], taken.at[4], NEAR)
        got["bnf"].wait_recv()
        even[5] = (total(5) + taken[1].astype(F32)).astype(BF)
        got["bf"] = links.send(even.at[5], taken.at[5], far)

    def end():
        got["own"].wait_recv()
        for name in ("af", "an"):
            got[name].wait_recv()
        finish(0, total(0) + taken[2].astype(F32) + taken[4].astype(F32))
        for name in ("bn", "bf"):
            got[name].wait_recv()
        finish(1, total(1) + taken[3].astype(F32) + taken[5].astype(F32))

    return [begin, corners, relay, end]


def scatter_steps_light(links, parts, even, cores, taken, finish):
    got = {}
    far = links.layout.far

    def total(block):
        return even[block].astype(F32) + cores[block].astype(F32)

    def begin():
        got["load"] = links.local(parts.at[pl.ds(0, 8)], even)
        got["last"] = links.send(parts.at[pl.ds(14, 2)], cores.at[pl.ds(6, 2)], CORE)
        got["mid"] = links.send(parts.at[pl.ds(10, 4)], cores.at[pl.ds(2, 4)], CORE)
        got["own"] = links.send(parts.at[pl.ds(8, 2)], cores.at[pl.ds(0, 2)], CORE)

    def corners():
        got["load"].wait()
        got["last"].wait_recv()
        for i in range(2):
            even[6 + i] = total(6 + i).astype(BF)
            got["nf", i] = links.send(even.at[6 + i], taken.at[i], NEAR)
        got["mid"].wait_recv()
        for i in range(2):
            even[2 + i] = total(2 + i).astype(BF)
            got["n", i] = links.send(even.at[2 + i], taken.at[2 + i], NEAR)

    def relay():
        for i in range(2):
            got["nf", i].wait_recv()
            even[4 + i] = (total(4 + i) + taken[i].astype(F32)).astype(BF)
            got["f", i] = links.send(even.at[4 + i], taken.at[4 + i], far)

    def end():
        got["own"].wait_recv()
        for i in range(2):
            got["n", i].wait_recv()
            got["f", i].wait_recv()
            finish(i, total(i) + taken[2 + i].astype(F32) + taken[4 + i].astype(F32))

    return [begin, corners, relay, end]


SCATTER_COPIES = 9


def scatter_scratch(half, width):
    return [
        pltpu.VMEM((8, half, width), BF),
        pltpu.VMEM((8, half, width), BF),
        pltpu.VMEM((6, half, width), BF),
    ]


def gather_stream(links, items, lag):
    layout = links.layout
    made = [{} for _ in items]

    def spread(i, rel, source):
        slot = items[i][2]
        for bit in range(layout.low(rel)):
            goal = rel | (1 << bit)
            made[i][goal] = links.send(source, slot(rel), layout.mask(1 << bit))

    def step(k):
        def run():
            if k < len(items):
                ready, own, _ = items[k]
                ready()
                spread(k, 0, own)
            if k >= lag:
                i = k - lag
                for rel in range(2, layout.reps, 2):
                    made[i][rel].wait_recv()
                    spread(i, rel, items[i][2](rel))

        return run

    def end():
        for copies in made:
            for rel in range(1, layout.reps, 2):
                copies[rel].wait_recv()

    return [step(k) for k in range(len(items) + lag)], end


def scatter_stream(links, items, window, lag):
    layout = links.layout
    made = [{} for _ in items]
    loads = [None for _ in items]
    stay = range(0, layout.reps, 2)

    def begin(i):
        part, keep, taken, _, paired = items[i]
        loads[i] = [links.local(part(rel), keep(rel // 2)) for rel in stay]
        for rel in range(layout.reps - 1, 0, -2):
            if not paired:
                made[i][rel] = links.send(part(rel), taken(rel - 1), layout.mask(rel))

    def total(i, rel):
        _, keep, taken, _, paired = items[i]
        sources = [source for source in layout.sources(rel) if not (paired and source & 1)]
        for source in sources:
            made[i][source].wait_recv()
        value = keep(rel // 2)[...].astype(F32)
        for source in sources:
            value = value + taken(source - 1)[...].astype(F32)
        return value

    def pass_on(i):
        _, keep, taken, _, paired = items[i]
        for load in loads[i]:
            load.wait()
        for rel in stay[:0:-1]:
            if not (paired and layout.low(rel) == 1):
                keep(rel // 2)[...] = total(i, rel).astype(BF)
            made[i][rel] = links.send(keep(rel // 2), taken(rel - 1), layout.mask(rel))

    def step(k):
        def run():
            if k < len(items):
                begin(k)
            if window <= k < len(items) + window:
                pass_on(k - window)
            if k >= window + lag:
                items[k - window - lag][3](total(k - window - lag, 0))

        return run

    return [step(k) for k in range(len(items) + window + lag)]


def pair_stream(links, items, window):
    layout = links.layout
    made = [{} for _ in items]

    def begin(i):
        part, keep, taken, _ = items[i]
        for k in range(layout.reps // 2):
            made[i][k] = (
                links.local(part(2 * k), keep(k)),
                links.send(part(2 * k + 1), taken(k), layout.mask(1)),
            )

    def end(i):
        _, keep, taken, finish = items[i]
        for k, (load, copy) in made[i].items():
            load.wait()
            copy.wait_recv()
            finish(k, keep(k)[...].astype(F32) + taken(k)[...].astype(F32))

    def step(k):
        def run():
            if k < len(items):
                begin(k)
            if k >= window:
                end(k - window)

        return run

    return [step(k) for k in range(len(items) + window)]


def both(first, second):
    def run():
        first()
        second()

    return run


def interleave(stream, acts, first=1):
    acts = list(acts)
    for k, step in enumerate(stream):
        step()
        if k >= first and acts:
            acts.pop(0)()
    for act in acts:
        act()


def semaphores(copies, local_copies):
    return [
        pltpu.SemaphoreType.DMA((copies,)),
        pltpu.SemaphoreType.DMA((copies,)),
        pltpu.SemaphoreType.DMA((local_copies,)),
    ]


VMEM = pl.BlockSpec(memory_space=pltpu.VMEM)
HBM = pl.BlockSpec(memory_space=pl.ANY)


def kernel_params(call_id):
    return pltpu.CompilerParams(collective_id=call_id, has_side_effects=True)


def opening_kernel(
    layout, small, tokens, cot, query_w, key_w, value_w, gate_w, gate_src, up_src, out_src,
    small_all, x_all, cot_all, attn_w, gate_in, up_in, out_w,
    small_buf, gain_buf, normed_buf, attn_own, out_own, gate_own, up_own, send_sems, recv_sems, local_sems,
):
    links = Links(layout, send_sems, recv_sems, local_sems)
    device = links.device
    place, rep = layout.place(device), layout.rep(device)
    _, half, width = tokens.shape
    shard = layout.shard

    def place_at(mask):
        return layout.place(flip_device(device, mask)) if mask else place

    edges, columns = 0, []
    for weight in (query_w, key_w, value_w, gate_w):
        size = weight.shape[1] // HEADS
        columns.append((weight, size, edges))
        edges += size

    def column(weight, size, where):
        return weight.at[:, pl.ds(pl.multiple_of(where * size, LANES), size)]

    mine = links.local(small, small_buf.at[pl.ds(device, 1)])
    own_loads = [
        links.local(column(weight, size, place), attn_own.at[:, pl.ds(at, size)])
        for weight, size, at in columns
    ]
    out_load = links.local(out_src, out_own)
    gate_load = links.local(gate_src.at[place], gate_own)
    up_load = links.local(up_src.at[place], up_own)
    links.greet(layout.masks)
    mine.wait()

    def small_step(b):
        size = 1 << b
        part = small_buf.at[pl.ds((device // size) * size, size)]
        return links.send(part, part, size)

    attn_in, later_in = {}, []

    def attn_exchange(mask):
        attn_in[mask] = [
            links.send(
                column(weight, size, place_at(mask)),
                attn_w.at[rep, place, :, pl.ds(at, size)],
                mask,
            )
            for weight, size, at in columns
        ]

    def hidden_exchange(mask):
        for source, target in ((gate_src, gate_in), (up_src, up_in)):
            later_in.append(links.send(source.at[place_at(mask)], target.at[place], mask))

    small_copy = small_step(0)
    for mask in layout.team[:3]:
        attn_exchange(mask)
    for load in own_loads:
        load.wait()
    keeps = [links.local(attn_own, attn_w.at[rep, place])]

    def attn_item(mask):
        at = place_at(mask)

        def ready():
            for copy in attn_in.get(mask, ()):
                copy.wait_recv()

        own = attn_w.at[rep, at] if mask else attn_own
        return ready, own, lambda rel: attn_w.at[xor_index(rel, rep, layout.reps), at]

    def row_item(own, target, part):
        return (
            lambda: None,
            own.at[part],
            lambda rel: target.at[xor_index(rel, rep, layout.reps), part],
        )

    items = [attn_item(0)] + [row_item(out_own, out_w, part) for part in range(4)]
    items += [attn_item(mask) for mask in layout.team]
    out_load.wait()
    keeps.append(links.local(out_own, out_w.at[rep]))
    steps, stream_end = gather_stream(links, items, 3)
    steps[0]()
    for b in range(1, layout.bits):
        small_copy.wait_recv()
        small_copy = small_step(b)
        if b < 5:
            attn_exchange(layout.team[2 + b])
        if b == 2:
            steps[1]()
    steps[2]()
    small_copy.wait_recv()
    keeps.append(links.local(small_buf, small_all))

    per = LANES // shard
    for k in range(width // LANES):
        rows = small_buf[k * per].astype(F32)
        for i in range(1, per):
            rows = rows + small_buf[k * per + i].astype(F32)
        gain_buf[:, k * LANES : (k + 1) * LANES] = rows
    gain, shift = gain_buf[0:1, :], gain_buf[1:2, :]
    pieces = layout.pieces(width)

    def norm_rows(i, carry):
        part = i // (half // TILE)
        at = pl.ds(pl.multiple_of((i % (half // TILE)) * TILE, TILE), TILE)
        normed = layer_norm(tokens[part, at, :].astype(F32), gain, shift)
        normed_buf[part, at, :] = to_weight_order(normed, pieces).astype(BF)
        return carry

    lax.fori_loop(0, 2 * half // TILE, norm_rows, 0)
    keeps.append(links.local(normed_buf, x_all.at[pl.ds(0, 2)]))
    keeps.append(links.local(cot, cot_all.at[pl.ds(0, 2)]))
    for own, target, load in ((gate_own, gate_in, gate_load), (up_own, up_in, up_load)):
        load.wait()
        keeps.append(links.local(own, target.at[place]))

    def exchange_some(masks):
        return lambda: [hidden_exchange(mask) for mask in masks]

    x_steps = gather_steps_light(links, normed_buf, x_all)
    cot_steps = gather_steps_light(links, cot, cot_all)
    acts = x_steps[:1] + [lambda: None] + x_steps[1:2] + [lambda: None] + x_steps[2:]
    acts += [exchange_some(layout.team[:2]), exchange_some(layout.team[2:4])]
    acts += cot_steps[:1] + [exchange_some(layout.team[4:6])] + cot_steps[1:2]
    acts += [exchange_some(layout.team[6:])] + cot_steps[2:]
    interleave(steps[3:], acts, 0)
    stream_end()
    for copy in later_in:
        copy.wait_recv()
    for copy in keeps:
        copy.wait()
    links.finish()


def opening_call(layout, small, tokens, cot, attn_weights, gate_src, up_src, out_src):
    reps, shard = layout.reps, layout.shard
    rows, width = tokens.shape
    half = rows // 2
    attn_cols = sum(w.shape[1] for w in attn_weights) // HEADS
    ff_cols = gate_src.shape[2]
    out_shape = (4, out_src.shape[0] // 4, out_src.shape[1])
    copies = 7 * 4 + 7 * 2 + 12 * (reps - 1) + 2 * GATHER_COPIES + layout.bits
    return pl.pallas_call(
        functools.partial(opening_kernel, layout),
        out_shape=(
            jax.ShapeDtypeStruct((layout.count, 8, LANES), BF),
            jax.ShapeDtypeStruct((16, half, width), BF),
            jax.ShapeDtypeStruct((16, half, width), BF),
            jax.ShapeDtypeStruct((reps, 8, shard, attn_cols), BF),
            jax.ShapeDtypeStruct((8, shard, ff_cols), BF),
            jax.ShapeDtypeStruct((8, shard, ff_cols), BF),
            jax.ShapeDtypeStruct((reps,) + out_shape, BF),
        ),
        in_specs=[HBM, VMEM] + [HBM] * 8,
        out_specs=(HBM,) * 7,
        scratch_shapes=[
            pltpu.VMEM((layout.count, 8, LANES), BF),
            pltpu.VMEM((8, width), F32),
            pltpu.VMEM((2, half, width), BF),
            pltpu.VMEM((shard, attn_cols), BF),
            pltpu.VMEM(out_shape, BF),
            pltpu.VMEM((shard, ff_cols), BF),
            pltpu.VMEM((shard, ff_cols), BF),
        ]
        + semaphores(copies, 18),
        compiler_params=kernel_params(0),
        name="opening",
    )(
        small, tokens.reshape(2, half, width), cot.reshape(2, half, width), *attn_weights,
        gate_src, up_src, out_src.reshape(out_shape),
    )


def turn_kernel(
    layout, parts, tokens, gains, gate_in, up_in, down_in,
    hidden, all_rows, gate_w, up_w, down_w,
    even, cores, taken, normed_buf, send_sems, recv_sems, local_sems,
):
    links = Links(layout, send_sems, recv_sems, local_sems)
    rep = layout.rep(links.device)
    _, half, width = tokens.shape
    links.greet((CORE, NEAR, layout.far) + tuple(1 << b for b in layout.rep_bits))
    keeps = [links.local(gate_in, gate_w.at[rep]), links.local(up_in, up_w.at[rep])]
    downs = []
    for i in range(layout.reps // 2):
        slot = down_w.at[xor_index(2 * i, rep, layout.reps)]
        keeps.append(links.local(down_in.at[i], slot))
        downs.append(links.send(down_in.at[i], slot, layout.mask(1)))

    def item(own, target, part):
        at = pl.ds(part * 2, 2)
        return (
            lambda: None,
            own.at[at],
            lambda rel: target.at[xor_index(rel, rep, layout.reps), at],
        )

    items = [item(gate_in, gate_w, part) for part in range(4)]
    items += [item(up_in, up_w, part) for part in range(4)]
    steps, stream_end = gather_stream(links, items, 2)
    pieces = layout.pieces(width)

    def finish(part, value):
        hidden[part] = value + tokens[part].astype(F32)

        def norm_rows(i, carry):
            at = pl.ds(pl.multiple_of(i * TILE, TILE), TILE)
            normed = layer_norm(hidden[part, at, :], gains[0:1, :], gains[1:2, :])
            normed_buf[part, at, :] = to_weight_order(normed, pieces).astype(BF)
            return carry

        lax.fori_loop(0, half // TILE, norm_rows, 0)

    acts = scatter_steps_light(links, parts, even, cores, taken, finish)
    acts.append(lambda: keeps.append(links.local(normed_buf, all_rows.at[pl.ds(0, 2)])))
    acts += gather_steps_light(links, normed_buf, all_rows)
    acts.pop(0)()
    interleave(steps, acts, 0)
    stream_end()
    for copy in downs:
        copy.wait_recv()
    for copy in keeps:
        copy.wait()
    links.finish()


def turn_call(layout, parts, tokens, gains, gate_in, up_in, down_in):
    rows, width = tokens.shape
    half = rows // 2
    block = gate_in.shape
    return pl.pallas_call(
        functools.partial(turn_kernel, layout),
        out_shape=(
            jax.ShapeDtypeStruct((2, half, width), F32),
            jax.ShapeDtypeStruct((16, half, width), BF),
            jax.ShapeDtypeStruct((layout.reps,) + block, BF),
            jax.ShapeDtypeStruct((layout.reps,) + block, BF),
            jax.ShapeDtypeStruct((layout.reps,) + down_in.shape[1:], BF),
        ),
        in_specs=[HBM, VMEM, VMEM, VMEM, VMEM, VMEM],
        out_specs=(VMEM, HBM, HBM, HBM, HBM),
        scratch_shapes=scatter_scratch(half, width)
        + [pltpu.VMEM((2, half, width), BF)]
        + semaphores(
            8 * (layout.reps - 1) + layout.reps // 2 + SCATTER_COPIES + GATHER_COPIES,
            5 + layout.reps // 2,
        ),
        compiler_params=kernel_params(1),
        name="turn",
    )(parts.reshape(16, half, width), tokens.reshape(2, half, width), gains, gate_in, up_in, down_in)


def turn_back_kernel(
    layout, parts, hidden, out_grad, gains, down_p, gate_p, up_p,
    hidden_grad, all_rows, vectors, down_sum, gate_sum, up_first, up_rest,
    even, cores, taken, low_buf, sum_buf, down_l, down_y, gate_l, gate_y, up_l, up_y,
    send_sems, recv_sems, local_sems,
):
    links = Links(layout, send_sems, recv_sems, local_sems)
    rep = layout.rep(links.device)
    _, half, width = hidden.shape
    links.greet((CORE, NEAR, layout.far) + tuple(1 << b for b in layout.rep_bits))

    def item(part, keep, taken, at, first, rest):
        def finish(k, value):
            if k:
                rest[k - 1, at] = value.astype(rest.dtype)
            else:
                first[at] = value.astype(first.dtype)

        return (
            lambda rel: part.at[xor_index(rel, rep, layout.reps), at],
            lambda k: keep.at[k, at],
            lambda k: taken.at[k, at],
            finish,
        )

    pairs = [pl.ds(2 * part, 2) for part in range(4)]
    items = replica_items(layout, rep, down_p, down_l, down_y, range(4), down_sum)
    items += replica_items(layout, rep, gate_p, gate_l, gate_y, pairs, gate_sum)
    steps = scatter_stream(links, items, 2, 2)
    late = pair_stream(links, [item(up_p, up_l, up_y, at, up_first, up_rest) for at in pairs], 2)
    for k, more in enumerate(late):
        steps[min(k + 5, 11)] = both(steps[min(k + 5, 11)], more)
    pieces = layout.pieces(width)
    vectors[...] = jnp.zeros_like(vectors)

    def finish(part, value):
        sum_buf[...] = value

        def rows(i, carry):
            at = pl.ds(pl.multiple_of(i * TILE, TILE), TILE)
            grads = from_weight_order(sum_buf[at, :], pieces)
            back, gain_part, shift_part = layer_norm_back(
                hidden[part, at, :], gains[0:1, :], grads
            )
            total = out_grad[part, at, :].astype(F32) + back
            hidden_grad[part, at, :] = total
            low_buf[part, at, :] = total.astype(BF)
            vectors[0:1, :] += gain_part
            vectors[1:2, :] += shift_part
            return carry

        lax.fori_loop(0, half // TILE, rows, 0)

    keeps = []
    acts = scatter_steps(links, parts, even, cores, taken, finish)
    acts.append(lambda: keeps.append(links.local(low_buf, all_rows.at[pl.ds(0, 2)])))
    acts += gather_steps(links, low_buf, all_rows)
    acts.pop(0)()
    interleave(steps, acts, 0)
    for copy in keeps:
        copy.wait()
    links.finish()


def replica_items(layout, rep, part, keep, taken, places, sums, paired=False):
    def item(at):
        def finish(value):
            sums[at] = value.astype(sums.dtype)

        return (
            lambda rel: part.at[rel // 2 if paired else xor_index(rel, rep, layout.reps), at],
            lambda i: keep.at[i, at],
            lambda i: taken.at[i, at],
            finish,
            paired,
        )

    return [item(at) for at in places]


def turn_back_call(layout, parts, hidden, out_grad, gains, down_p, gate_p, up_p):
    half, width = hidden.shape[1:]
    reps = layout.reps
    down_block, gate_block = down_p.shape[1:], gate_p.shape[1:]
    return pl.pallas_call(
        functools.partial(turn_back_kernel, layout),
        out_shape=(
            jax.ShapeDtypeStruct((2, half, width), F32),
            jax.ShapeDtypeStruct((16, half, width), BF),
            jax.ShapeDtypeStruct((8, width), F32),
            jax.ShapeDtypeStruct(down_block, F32),
            jax.ShapeDtypeStruct(gate_block, BF),
            jax.ShapeDtypeStruct(gate_block, F32),
            jax.ShapeDtypeStruct((reps // 2 - 1,) + gate_block, BF),
        ),
        in_specs=[HBM, VMEM, VMEM, VMEM, HBM, HBM, HBM],
        out_specs=(VMEM, HBM, VMEM, VMEM, VMEM, VMEM, VMEM),
        scratch_shapes=scatter_scratch(half, width)
        + [
            pltpu.VMEM((2, half, width), BF),
            pltpu.VMEM((half, width), F32),
            pltpu.VMEM((reps // 2,) + down_block, BF),
            pltpu.VMEM((reps - 1,) + down_block, BF),
            pltpu.VMEM((reps // 2,) + gate_block, BF),
            pltpu.VMEM((reps - 1,) + gate_block, BF),
            pltpu.VMEM((reps // 2,) + gate_block, BF),
            pltpu.VMEM((reps // 2,) + gate_block, BF),
        ]
        + semaphores(
            8 * (reps - 1) + 2 * reps + SCATTER_COPIES + GATHER_COPIES, 4 * reps + 2 * reps + 2
        ),
        compiler_params=kernel_params(2),
        name="turn_back",
    )(
        parts.reshape(16, half, width), hidden, out_grad.reshape(2, half, width), gains,
        down_p, gate_p, up_p,
    )


def closing_kernel(
    layout, attn_p, out_q, gate_sum, up_sum, one_parts, two_parts, tokens, hidden_grad, gains, vectors,
    query_back, key_back, value_back, swish_back, gate_back, up_back, out_sum, branch_two,
    tokens_grad, vector_sum,
    even_1, cores_1, taken_1, even_2, cores_2, taken_2, sum_buf, rows_buf, vec_l, vec_y,
    attn_l, attn_y, attn_s, out_l, out_y, send_sems, recv_sems, local_sems,
):
    links = Links(layout, send_sems, recv_sems, local_sems)
    device = links.device
    place, rep = layout.place(device), layout.rep(device)
    _, half, width = tokens.shape
    links.greet(layout.masks)
    backs, kept = [], []

    def place_at(mask):
        return layout.place(flip_device(device, mask)) if mask else place

    def give(source, target, mask):
        if mask:
            backs.append(links.send(source, target, mask))
        else:
            kept.append(links.local(source, target))

    edges, columns = 0, []
    for target in (query_back, key_back, value_back, swish_back):
        size = target.shape[1] // HEADS
        columns.append((target, size, edges))
        edges += size

    def with_return(item, mask, give_back):
        part, keep, taken, finish, paired = item

        def finish_and_give(value):
            finish(value)
            give_back(mask)

        return part, keep, taken, finish_and_give, paired

    def attn_return(mask):
        for target, size, at in columns:
            goal = pl.ds(pl.multiple_of(place * size, LANES), size)
            give(attn_s.at[place_at(mask), :, pl.ds(at, size)], target.at[:, goal], mask)

    order = layout.team[::-1] + (0,)
    items = replica_items(layout, rep, out_q, out_l, out_y, range(4), out_sum, True)
    places = [place_at(m) for m in order]
    plain = replica_items(layout, rep, attn_p, attn_l, attn_y, places, attn_s)
    items += [with_return(item, m, attn_return) for item, m in zip(plain, order)]
    steps = scatter_stream(links, items, 2, 2)

    pieces = layout.pieces(width)
    rows_buf[...] = jnp.zeros_like(rows_buf)
    rows_buf[2:4, :] = vectors[0:2, :]

    def finish_one(part, value):
        sum_buf[...] = value

        def rows(i, carry):
            at = pl.ds(pl.multiple_of(i * TILE, TILE), TILE)
            grads = from_weight_order(sum_buf[at, :], pieces)
            back, gain_part, shift_part = layer_norm_back(
                tokens[part, at, :].astype(F32), gains[0:1, :], grads
            )
            tokens_grad[part, at, :] = hidden_grad[part, at, :] + back
            rows_buf[0:1, :] += gain_part
            rows_buf[1:2, :] += shift_part
            return carry

        lax.fori_loop(0, half // TILE, rows, 0)

    def finish_two(part, value):
        branch_two[part] = value

    per = LANES // layout.shard
    own_bits = per.bit_length() - 1
    slots = layout.count // per
    flight = {}

    def vector_begin():
        for slot in range(slots):
            vec_l[slot] = rows_buf[:, slot * LANES : (slot + 1) * LANES]

    def vector_send(b):
        def run():
            peer = flip_device(device, 1 << b)
            if b >= own_bits:
                size = 1 << (b - own_bits)
                source = vec_l.at[pl.ds((peer // (1 << b)) * size, size)]
                target = vec_y.at[pl.ds(size, size)]
            else:
                source = vec_l.at[pl.ds(device // per, 1)]
                target = vec_y.at[pl.ds(slots + b, 1)]
            flight[b] = links.send(source, target, 1 << b)

        return run

    def vector_add(b):
        def run():
            if b >= own_bits:
                size = 1 << (b - own_bits)
                flight[b].wait_recv()
                mine = pl.ds((device // (1 << b)) * size, size)
                vec_l[mine] = vec_l[mine] + vec_y[size : 2 * size]
            else:
                links.swap_done(flight[b])
                mine = pl.ds(device // per, 1)
                vec_l[mine] = vec_l[mine] + vec_y[slots + b : slots + b + 1]

        return run

    def gate_return():
        for mask in layout.team + (0,):
            give(gate_sum.at[place_at(mask)], gate_back.at[place], mask)
            give(up_sum.at[place_at(mask)], up_back.at[place], mask)

    one = scatter_steps_light(links, one_parts, even_1, cores_1, taken_1, finish_one)
    two = scatter_steps_light(links, two_parts, even_2, cores_2, taken_2, finish_two)
    acts = one[1:] + [vector_begin]
    down_bits = list(range(layout.bits))[::-1]
    together = [(lambda b=b, a=a: ((a() if a else None), vector_send(b)())) for a, b in zip(
        [None] + [vector_add(b) for b in down_bits[:-1]], down_bits)]
    acts += [lambda: (together[0](), two[0](), gate_return())]
    for k in range(1, layout.bits):
        extra = two[k] if k < len(two) else (lambda: None)
        acts.append(lambda k=k, extra=extra: (together[k](), extra()))
    acts += two[layout.bits :] + [vector_add(down_bits[-1])]
    one[0]()
    interleave(steps, acts, 0)
    vector_sum[...] = vec_l[device // per]
    for copy in backs:
        copy.wait_recv()
    for copy in kept:
        copy.wait()
    links.finish()


def closing_call(layout, attn_p, out_q, gate_sum, up_sum, one_parts, two_parts, tokens, hidden_grad,
                 gains, vectors, back_widths):
    reps, shard = layout.reps, layout.shard
    half, width = hidden_grad.shape[1:]
    attn_block, up_block, out_block = attn_p.shape[1:], up_sum.shape, out_q.shape[1:]
    per = LANES // shard
    slots = layout.count // per
    stay = reps // 2
    rows = jax.ShapeDtypeStruct((2, half, width), F32)
    copies = 20 * (reps - 1) + 7 * 6 + 2 * SCATTER_COPIES + layout.bits
    return pl.pallas_call(
        functools.partial(closing_kernel, layout),
        out_shape=tuple(jax.ShapeDtypeStruct((shard, w), BF) for w in back_widths)
        + (
            jax.ShapeDtypeStruct(up_block, BF),
            jax.ShapeDtypeStruct(up_block, BF),
            jax.ShapeDtypeStruct(out_block, F32),
            rows,
            rows,
            jax.ShapeDtypeStruct((8, LANES), F32),
        ),
        in_specs=[HBM, HBM, VMEM, VMEM, HBM, HBM, VMEM, VMEM, VMEM, VMEM],
        out_specs=(HBM,) * 6 + (VMEM,) * 4,
        scratch_shapes=scatter_scratch(half, width)
        + scatter_scratch(half, width)
        + [
            pltpu.VMEM((half, width), F32),
            pltpu.VMEM((8, width), F32),
            pltpu.VMEM((slots, 8, LANES), F32),
            pltpu.VMEM((slots + per, 8, LANES), F32),
            pltpu.VMEM((stay,) + attn_block, BF),
            pltpu.VMEM((reps - 1,) + attn_block, BF),
            pltpu.VMEM(attn_block, BF),
            pltpu.VMEM((stay,) + out_block, BF),
            pltpu.VMEM((reps - 1,) + out_block, BF),
        ]
        + semaphores(copies, 20 * stay + 8),
        compiler_params=kernel_params(3),
        name="closing",
    )(
        attn_p, out_q, gate_sum, up_sum, one_parts.reshape(16, half, width),
        two_parts.reshape(16, half, width), tokens.reshape(2, half, width), hidden_grad, gains, vectors,
    )


def seq_layout(seq_lens, row_count):
    row_ids = jnp.arange(row_count, dtype=jnp.int32)
    seq_ends = jnp.cumsum(seq_lens)
    passed = row_ids[:, None] >= seq_ends[None, :]
    segment = jnp.sum(passed.astype(jnp.int32), axis=1)
    seq_start = jnp.sum(jnp.where(passed, seq_lens[None, :], 0), axis=1)
    position = row_ids - seq_start
    live_rows = row_ids < seq_ends[-1]
    return (segment, position, live_rows)


def group_norm(values):
    center = values - jnp.mean(values, axis=-1, keepdims=True)
    spread = jnp.mean(center * center, axis=-1, keepdims=True)
    return center * lax.rsqrt(spread + GROUP_EPS)


def dot(left, right):
    return jnp.dot(left, right, preferred_element_type=F32)


def dot_nt(left, right):
    return lax.dot_general(left, right, (((1,), (1,)), ((), ())), preferred_element_type=F32)


def dot_tn(left, right):
    return lax.dot_general(left, right, (((0,), (0,)), ((), ())), preferred_element_type=F32)


def make_body(count):
    def on_device(
        tokens,
        seq_lengths,
        attn_gain,
        attn_shift,
        query_weight,
        key_weight,
        value_weight,
        gate_weight,
        out_weight,
        mlp_gain,
        mlp_shift,
        mlp_gate,
        mlp_up,
        mlp_down,
        cotangent,
    ):
        local_rows, width = tokens.shape
        shard = width // count
        layout = Layout(count, shard)
        reps = layout.reps
        device = lax.axis_index("dp")
        rep, pos_t = layout.rep(device), layout.place(device)
        micro_count, seq_slots = seq_lengths.shape[1:]
        row_count = local_rows // micro_count
        key_size = query_weight.shape[1] // HEADS
        value_size = value_weight.shape[1] // HEADS
        hidden_size = mlp_gate.shape[1]
        ff_block = hidden_size // count
        group_rows = 8 * local_rows
        home = [layout.device(d % reps, d // reps) for d in range(count)]
        head_perm = [(d, home[d]) for d in range(count)]
        head_back = [(b, a) for a, b in head_perm]

        high, mid = 1 << (layout.bits - 1 - layout.far_bit), 1 << (layout.far_bit - 2)

        def ff_first(weight):
            v = weight.reshape(shard, high, 2, mid, 4, ff_block)
            return v.transpose(2, 4, 0, 1, 3, 5).reshape(8, shard, reps * ff_block)

        def ff_back(grad):
            v = grad.reshape(2, 4, shard, high, mid, ff_block)
            return v.transpose(2, 3, 0, 4, 1, 5).reshape(shard, hidden_size)

        per = LANES // shard
        lane_on = jnp.arange(LANES, dtype=jnp.int32) // shard == device % per

        def in_lanes(values):
            return jnp.where(lane_on, jnp.tile(values, per), jnp.zeros((), BF))[None]

        own_lens = seq_lengths.reshape(-1).astype(BF)
        small = jnp.concatenate(
            [in_lanes(v) for v in (attn_gain, attn_shift, mlp_gain, mlp_shift)]
            + [jnp.pad(own_lens, (0, LANES - own_lens.shape[0]))[None], jnp.zeros((3, LANES), BF)]
        )
        own_live = jax.vmap(lambda v: seq_layout(v, row_count)[2])(seq_lengths[0])
        own_live = own_live.reshape(local_rows).astype(F32)[:, None]
        out_grad_low = (cotangent.astype(F32) * own_live).astype(BF)

        out_own = lax.ppermute(out_weight, "dp", head_perm)
        small, normed_one, cot_all, attn_w, gate_in, up_in, out_w = opening_call(
            layout, small[None], tokens, out_grad_low,
            (query_weight, key_weight, value_weight, gate_weight),
            ff_first(mlp_gate), ff_first(mlp_up), out_own,
        )
        normed_one = normed_one.reshape(group_rows, width)
        cot_all = cot_all.reshape(group_rows, width)
        attn_w = attn_w.reshape(width, -1)
        out_w = out_w.reshape(-1, width)

        def flip_rep(values, bit):
            mask = 1 << layout.rep_bits[bit]
            return lax.ppermute(values, "dp", [(d, d ^ mask) for d in range(count)])

        down_even = [lax.optimization_barrier((mlp_down, small))[0]]
        for k in range(1, reps // 2):
            low = layout.low(k)
            down_even.append(flip_rep(down_even[k & ~(1 << low)], low + 1))

        def pair_sums(parts):
            sums = []
            for rel in range(0, reps, 2):
                other = lax.dynamic_index_in_dim(parts, rep ^ (rel + 1), 0, keepdims=False)
                own = lax.dynamic_index_in_dim(parts, rep ^ rel, 0, keepdims=False)
                sums.append((own.astype(F32) + flip_rep(other, 0).astype(F32)).astype(BF))
            return jnp.stack(sums)

        def finish_pairs(first, rest):
            sums = [first] + [rest[k] for k in range(reps // 2 - 1)]
            for k in range(reps // 2 - 1, 0, -1):
                low = layout.low(k)
                got = flip_rep(sums[k].astype(BF), low + 1).astype(F32)
                sums[k & ~(1 << low)] = sums[k & ~(1 << low)].astype(F32) + got
            return sums[0]

        vecs = small[:, :4, :].astype(F32).reshape(-1, per, 4, LANES).sum(1)
        vecs = vecs.transpose(1, 0, 2).reshape(4, width)
        gains_one = jnp.pad(vecs[:2], ((0, 6), (0, 0)))
        gains_two = jnp.pad(vecs[2:], ((0, 6), (0, 0)))
        lens = small[:, 4, : own_lens.shape[0]].astype(jnp.int32)
        order = [c + 2 * n + 4 * f for c in range(2) for f in range(2) for n in range(2)]
        members = jnp.stack(
            [flip_device(device, (j & 3) + (j >> 2) * layout.far) for j in order]
        )
        lens = jnp.take(lens, members, axis=0).reshape(8 * micro_count, seq_slots)

        segment, position, live = jax.vmap(lambda s: seq_layout(s, row_count))(lens)
        head_log = jnp.log(1.0 - 2.0 ** (-5.0 - jnp.arange(HEADS, dtype=F32)))
        head_log = lax.dynamic_index_in_dim(head_log, pos_t, 0, keepdims=False)
        ids = jnp.arange(row_count, dtype=jnp.int32)
        same_seq = (
            (segment[:, :, None] == segment[:, None, :])
            & live[:, :, None]
            & live[:, None, :]
            & (ids[:, None] >= ids[None, :])[None]
        )
        distance = jnp.maximum(position[:, :, None] - position[:, None, :], 0).astype(F32)
        decay = jnp.where(same_seq, jnp.exp(distance * head_log), 0.0)
        half_size = key_size // 2
        pair_index = jnp.arange(half_size, dtype=F32)
        frequency = 10000.0 ** (-pair_index / half_size)
        row_place = position.reshape(-1).astype(F32)[:, None]
        angles = row_place * frequency[None, :]
        growth = (pair_index * 2.0 / key_size + 0.4) / 1.4
        stretch = growth[None, :] ** (row_place / 512.0)
        key_factor = key_size ** (-0.5) / stretch
        cosine, sine, stretch, key_factor = lax.optimization_barrier(
            (jnp.cos(angles), jnp.sin(angles), stretch, key_factor)
        )

        def rotate(values, factor):
            a, b = values[:, :half_size], values[:, half_size:]
            return jnp.concatenate(
                [(a * cosine - b * sine) * factor, (b * cosine + a * sine) * factor], axis=1
            )

        def rotate_back(grads, factor):
            a, b = grads[:, :half_size] * factor, grads[:, half_size:] * factor
            return jnp.concatenate([a * cosine + b * sine, b * cosine - a * sine], axis=1)

        def micro(values):
            return values.reshape(-1, row_count, values.shape[-1])

        qkvg = dot(normed_one, attn_w)
        query_raw = qkvg[:, :key_size]
        key_raw = qkvg[:, key_size : 2 * key_size]
        value_low = qkvg[:, 2 * key_size : 2 * key_size + value_size].astype(BF)
        gate_raw = qkvg[:, 2 * key_size + value_size :]
        query_turned = micro(rotate(query_raw, stretch).astype(BF))
        key_turned = micro(rotate(key_raw, key_factor).astype(BF))
        value_m = micro(value_low)
        scores = jnp.einsum("mqd,mkd->mqk", query_turned, key_turned, preferred_element_type=F32)
        weights_low = (scores * decay).astype(BF)
        retained = jnp.einsum("mqk,mke->mqe", weights_low, value_m, preferred_element_type=F32)
        retained = retained.reshape(group_rows, value_size)

        def mix(gate_in, retained_in):
            return jax.nn.silu(gate_in) * group_norm(retained_in)

        mixed = mix(gate_raw, retained).astype(BF)
        hidden, normed_two, gate_w, up_w, down_w = turn_call(
            layout, dot(mixed, out_w).astype(BF), tokens, gains_two, gate_in, up_in,
            jnp.stack(down_even),
        )
        down_w = down_w.reshape(-1, width)
        normed_two = normed_two.reshape(group_rows, width)
        gate_w, up_w = gate_w.reshape(width, -1), up_w.reshape(width, -1)

        def act(gate_in, up_in):
            return jax.nn.gelu(gate_in, approximate=True) * up_in

        product, pull_act = jax.vjp(act, dot(normed_two, gate_w), dot(normed_two, up_w))
        product = product.astype(BF)
        gate_low, up_low = (g.astype(BF) for g in pull_act(dot_nt(cot_all, down_w)))
        two_parts = dot(product, down_w).astype(BF)
        down_parts = dot_tn(product, cot_all).astype(BF)
        gate_parts = dot_tn(normed_two, gate_low).astype(BF)
        up_parts = dot_tn(normed_two, up_low).astype(BF)
        normed_parts = (dot_nt(gate_low, gate_w) + dot_nt(up_low, up_w)).astype(BF)
        hidden_grad, branch_one_grad, vectors, mlp_down_grad, gate_sum, up_first, up_rest = turn_back_call(
            layout, normed_parts, hidden, out_grad_low, gains_two,
            down_parts.reshape(reps, 4, -1, width), gate_parts.reshape(reps, 8, shard, -1),
            up_parts.reshape(reps, 8, shard, -1),
        )
        branch_one_grad = branch_one_grad.reshape(group_rows, width)
        up_sum = finish_pairs(up_first, up_rest).astype(BF)

        mixed_grad = dot_nt(branch_one_grad, out_w)
        out_parts = dot_tn(mixed, branch_one_grad).astype(BF)
        out_pairs = pair_sums(out_parts.reshape(reps, 4, -1, width))
        _, pull_mix = jax.vjp(mix, gate_raw, retained)
        gate_grad, retained_grad = pull_mix(mixed_grad)
        gate_grad = gate_grad.astype(BF)
        retained_low = micro(retained_grad.astype(BF))
        weights_grad = jnp.einsum("mqe,mke->mqk", retained_low, value_m, preferred_element_type=F32)
        value_grad = jnp.einsum(
            "mqk,mqe->mke", weights_low, retained_low, preferred_element_type=F32
        )
        value_grad = value_grad.reshape(group_rows, value_size).astype(BF)
        score_low = (weights_grad * decay).astype(BF)
        query_turn_grad = jnp.einsum("mqk,mkd->mqd", score_low, key_turned, preferred_element_type=F32)
        key_turn_grad = jnp.einsum("mqk,mqd->mkd", score_low, query_turned, preferred_element_type=F32)
        query_grad = rotate_back(query_turn_grad.reshape(group_rows, key_size), stretch).astype(BF)
        key_grad = rotate_back(key_turn_grad.reshape(group_rows, key_size), key_factor).astype(BF)
        attn_grads = jnp.concatenate([query_grad, key_grad, value_grad, gate_grad], axis=1)
        attn_parts = dot_tn(normed_one, attn_grads).astype(BF)
        one_parts = dot_nt(attn_grads, attn_w).astype(BF)
        q_back, k_back, v_back, g_back, gate_back, up_back, out_sum, branch_two, tokens_grad, vectors = (
            closing_call(
                layout,
                attn_parts.reshape(reps, 8, shard, -1),
                out_pairs, gate_sum, up_sum, one_parts, two_parts, tokens, hidden_grad, gains_one, vectors,
                [w.shape[1] for w in (query_weight, key_weight, value_weight, gate_weight)],
            )
        )
        out_sum = out_sum.reshape(out_weight.shape).astype(BF)
        out_weight_grad = lax.ppermute(out_sum, "dp", head_back).astype(F32)
        output = ((hidden + branch_two).reshape(local_rows, width) * own_live).astype(BF)
        vectors = lax.dynamic_slice_in_dim(vectors, (device % per) * shard, shard, axis=1)
        return (
            output,
            tokens_grad.reshape(local_rows, width),
            vectors[0],
            vectors[1],
            q_back.astype(F32),
            k_back.astype(F32),
            v_back.astype(F32),
            g_back.astype(F32),
            out_weight_grad,
            vectors[2],
            vectors[3],
            ff_back(gate_back.astype(F32)),
            ff_back(up_back.astype(F32)),
            mlp_down_grad.reshape(mlp_down.shape),
        )

    return on_device


def solution(mesh):
    rows = P("dp", None)
    vec = P("dp")
    placed = (
        rows, P("dp", None, None), vec, vec, rows, rows, rows, rows, rows,
        vec, vec, rows, rows, rows, rows,
    )
    outs = (rows, rows, vec, vec, rows, rows, rows, rows, rows, vec, vec, rows, rows, rows)
    return jax.shard_map(
        make_body(mesh.shape["dp"]), mesh=mesh, in_specs=placed, out_specs=outs, check_vma=False
    )
```

```python
import functools

import jax
import jax.numpy as jnp
from jax import lax
from jax.experimental import pallas as pl
from jax.experimental.pallas import tpu as pltpu
from jax.sharding import PartitionSpec as P


HEADS = 8
NORM_EPS = 1e-05
GROUP_EPS = 1.0
BF = jnp.bfloat16
F32 = jnp.float32
MESH = pl.DeviceIdType.MESH
LANES = 128


CORE, NEAR = 1, 2
TILE = 16


class Layout:
    def __init__(self, count, shard):
        self.count, self.shard = count, shard
        self.far_bit = 3 if (4 * shard) % LANES == 0 and count >= 32 else 2
        self.far = 1 << self.far_bit
        self.bits = count.bit_length() - 1
        self.rep_bits = [b for b in range(2, self.bits) if b != self.far_bit]
        self.reps = count // 8
        self.team = (CORE, NEAR, self.far, CORE | NEAR, CORE | self.far, NEAR | self.far,
                     CORE | NEAR | self.far)
        self.masks = self.team + tuple(
            1 << b for b in range(self.bits) if (1 << b) not in self.team
        )

    def place(self, device):
        return ((device // self.far) % 2) * 4 + device % 4

    def rep(self, device):
        total = 0
        for i, b in enumerate(self.rep_bits):
            total = total + ((device // (1 << b)) % 2) * (1 << i)
        return total

    def device(self, rep, place):
        total = place % 4 + (place // 4) * self.far
        for i, b in enumerate(self.rep_bits):
            total += ((rep >> i) & 1) << b
        return total

    def head_part(self, rep):
        return (rep % (self.reps // 2)) * 2 + rep // (self.reps // 2)

    def head_rep(self, part):
        return (part % 2) * (self.reps // 2) + part // 2

    def low(self, rel):
        return (rel & -rel).bit_length() - 1 if rel else len(self.rep_bits)

    def mask(self, rel):
        return 1 << self.rep_bits[self.low(rel)]

    def sources(self, rel):
        return [rel | (1 << i) for i in range(self.low(rel))]

    def pieces(self, width):
        if self.far_bit == 2:
            return [(0, width)]
        size = 4 * self.shard
        order = []
        for hi in range(self.count // 16):
            for b2 in range(2):
                for b3 in range(2):
                    order.append(((hi * 4 + b3 * 2 + b2) * size, size))
        return order


def flip_device(device, mask):
    other, bit = device, 0
    while mask >> bit:
        if (mask >> bit) & 1:
            other = other + (1 - 2 * ((device // (1 << bit)) % 2)) * (1 << bit)
        bit += 1
    return other


def xor_index(static, own, size):
    total, bit = 0, 1
    while bit < size:
        own_bit = (own // bit) % 2
        total = total + bit * (1 - own_bit if static & bit else own_bit)
        bit *= 2
    return total


def layer_norm(values, gain_vec, shift_vec):
    center = values - jnp.mean(values, axis=-1, keepdims=True)
    spread = jnp.mean(center * center, axis=-1, keepdims=True)
    return center * lax.rsqrt(spread + NORM_EPS) * gain_vec + shift_vec


def layer_norm_back(values, gain_vec, grads):
    center = values - jnp.mean(values, axis=-1, keepdims=True)
    scale = lax.rsqrt(jnp.mean(center * center, axis=-1, keepdims=True) + NORM_EPS)
    z = center * scale
    e = grads * gain_vec
    part = scale * (
        e - jnp.mean(e, axis=-1, keepdims=True) - z * jnp.mean(e * z, axis=-1, keepdims=True)
    )
    gain_part = jnp.sum(grads * z, axis=0, keepdims=True)
    shift_part = jnp.sum(grads, axis=0, keepdims=True)
    return part, gain_part, shift_part


def to_weight_order(values, pieces):
    return jnp.concatenate([values[:, at : at + size] for at, size in pieces], axis=1)


def from_weight_order(values, pieces):
    size = pieces[0][1]
    where = {at: i * size for i, (at, _) in enumerate(pieces)}
    return jnp.concatenate([values[:, where[at] : where[at] + size] for at in sorted(where)], axis=1)


class Links:
    def __init__(self, layout, send_sems, recv_sems, local_sems):
        self.layout = layout
        self.device = lax.axis_index("dp")
        self.send_sems, self.recv_sems, self.local_sems = send_sems, recv_sems, local_sems
        self.made, self.locals, self.sent = [], [], []

    def greet(self, masks):
        barrier = pltpu.get_barrier_semaphore()
        for mask in masks:
            pl.semaphore_signal(
                barrier, inc=1, device_id=(flip_device(self.device, mask),), device_id_type=MESH
            )
        pl.semaphore_wait(barrier, len(masks))

    def send(self, source, target, mask):
        index = len(self.made)
        copy = pltpu.make_async_remote_copy(
            src_ref=source,
            dst_ref=target,
            send_sem=self.send_sems.at[index],
            recv_sem=self.recv_sems.at[index],
            device_id=(flip_device(self.device, mask),),
            device_id_type=MESH,
        )
        copy.start()
        self.made.append(copy)
        return copy

    def local(self, source, target):
        copy = pltpu.make_async_copy(source, target, self.local_sems.at[len(self.locals)])
        copy.start()
        self.locals.append(copy)
        return copy

    def swap_done(self, copy):
        copy.wait()
        self.sent.append(copy)

    def finish(self):
        for copy in self.made:
            if not any(copy is other for other in self.sent):
                copy.wait_send()


def gather_steps(links, own, out):
    got = {}
    far = links.layout.far

    def begin():
        got["an"] = links.send(own.at[0], out.at[2], NEAR)
        got["bf"] = links.send(own.at[1], out.at[5], far)
        got["bn"] = links.send(own.at[1], out.at[3], NEAR)
        got["af"] = links.send(own.at[0], out.at[4], far)
        got["c"] = [links.send(own.at[i], out.at[8 + i], CORE) for i in range(2)]

    def relay():
        got["an"].wait_recv()
        got["anf"] = links.send(out.at[2], out.at[6], far)
        got["c"].append(links.send(out.at[2], out.at[10], CORE))
        got["bf"].wait_recv()
        got["bnf"] = links.send(out.at[5], out.at[7], NEAR)
        got["c"].append(links.send(out.at[5], out.at[13], CORE))
        got["bn"].wait_recv()
        got["c"].append(links.send(out.at[3], out.at[11], CORE))
        got["af"].wait_recv()
        got["c"].append(links.send(out.at[4], out.at[12], CORE))

    def end():
        got["anf"].wait_recv()
        got["c"].append(links.send(out.at[6], out.at[14], CORE))
        got["bnf"].wait_recv()
        got["c"].append(links.send(out.at[7], out.at[15], CORE))
        for copy in got["c"]:
            copy.wait_recv()

    return [begin, relay, end]


def gather_steps_light(links, own, out):
    got = {}
    far = links.layout.far

    def begin():
        got["af"] = links.send(own.at[0], out.at[4], far)
        got["bf"] = links.send(own.at[1], out.at[5], far)
        got["an"] = links.send(own.at[0], out.at[2], NEAR)
        got["bn"] = links.send(own.at[1], out.at[3], NEAR)
        got["c"] = [links.send(own.at[i], out.at[8 + i], CORE) for i in range(2)]

    def relay():
        for i, name in enumerate(("af", "bf")):
            got[name].wait_recv()
            got[name + "n"] = links.send(out.at[4 + i], out.at[6 + i], NEAR)
            got["c"].append(links.send(out.at[4 + i], out.at[12 + i], CORE))
        for i, name in enumerate(("an", "bn")):
            got[name].wait_recv()
            got["c"].append(links.send(out.at[2 + i], out.at[10 + i], CORE))

    def end():
        for i, name in enumerate(("afn", "bfn")):
            got[name].wait_recv()
            got["c"].append(links.send(out.at[6 + i], out.at[14 + i], CORE))
        for copy in got["c"]:
            copy.wait_recv()

    return [begin, relay, end]


GATHER_COPIES = 14


def scatter_steps(links, parts, even, cores, taken, finish):
    got = {}
    far = links.layout.far

    def total(block):
        return even[block].astype(F32) + cores[block].astype(F32)

    def begin():
        got["load"] = links.local(parts.at[pl.ds(0, 8)], even)
        got["last"] = links.send(parts.at[pl.ds(14, 2)], cores.at[pl.ds(6, 2)], CORE)
        got["mid"] = links.send(parts.at[pl.ds(10, 4)], cores.at[pl.ds(2, 4)], CORE)
        got["own"] = links.send(parts.at[pl.ds(8, 2)], cores.at[pl.ds(0, 2)], CORE)

    def corners():
        got["load"].wait()
        got["last"].wait_recv()
        even[6] = total(6).astype(BF)
        got["anf"] = links.send(even.at[6], taken.at[0], far)
        even[7] = total(7).astype(BF)
        got["bnf"] = links.send(even.at[7], taken.at[1], NEAR)
        got["mid"].wait_recv()
        even[4] = total(4).astype(BF)
        got["af"] = links.send(even.at[4], taken.at[2], far)
        even[3] = total(3).astype(BF)
        got["bn"] = links.send(even.at[3], taken.at[3], NEAR)

    def relay():
        got["anf"].wait_recv()
        even[2] = (total(2) + taken[0].astype(F32)).astype(BF)
        got["an"] = links.send(even.at[2], taken.at[4], NEAR)
        got["bnf"].wait_recv()
        even[5] = (total(5) + taken[1].astype(F32)).astype(BF)
        got["bf"] = links.send(even.at[5], taken.at[5], far)

    def end():
        got["own"].wait_recv()
        for name in ("af", "an"):
            got[name].wait_recv()
        finish(0, total(0) + taken[2].astype(F32) + taken[4].astype(F32))
        for name in ("bn", "bf"):
            got[name].wait_recv()
        finish(1, total(1) + taken[3].astype(F32) + taken[5].astype(F32))

    return [begin, corners, relay, end]


def scatter_steps_light(links, parts, even, cores, taken, finish):
    got = {}
    far = links.layout.far

    def total(block):
        return even[block].astype(F32) + cores[block].astype(F32)

    def begin():
        got["load"] = links.local(parts.at[pl.ds(0, 8)], even)
        got["last"] = links.send(parts.at[pl.ds(14, 2)], cores.at[pl.ds(6, 2)], CORE)
        got["mid"] = links.send(parts.at[pl.ds(10, 4)], cores.at[pl.ds(2, 4)], CORE)
        got["own"] = links.send(parts.at[pl.ds(8, 2)], cores.at[pl.ds(0, 2)], CORE)

    def corners():
        got["load"].wait()
        got["last"].wait_recv()
        for i in range(2):
            even[6 + i] = total(6 + i).astype(BF)
            got["nf", i] = links.send(even.at[6 + i], taken.at[i], NEAR)
        got["mid"].wait_recv()
        for i in range(2):
            even[2 + i] = total(2 + i).astype(BF)
            got["n", i] = links.send(even.at[2 + i], taken.at[2 + i], NEAR)

    def relay():
        for i in range(2):
            got["nf", i].wait_recv()
            even[4 + i] = (total(4 + i) + taken[i].astype(F32)).astype(BF)
            got["f", i] = links.send(even.at[4 + i], taken.at[4 + i], far)

    def end():
        got["own"].wait_recv()
        for i in range(2):
            got["n", i].wait_recv()
            got["f", i].wait_recv()
            finish(i, total(i) + taken[2 + i].astype(F32) + taken[4 + i].astype(F32))

    return [begin, corners, relay, end]


SCATTER_COPIES = 9


def scatter_scratch(half, width):
    return [
        pltpu.VMEM((8, half, width), BF),
        pltpu.VMEM((8, half, width), BF),
        pltpu.VMEM((6, half, width), BF),
    ]


def gather_stream(links, items, lag):
    layout = links.layout
    made = [{} for _ in items]

    def spread(i, rel, source):
        slot = items[i][2]
        for bit in range(layout.low(rel)):
            goal = rel | (1 << bit)
            made[i][goal] = links.send(source, slot(rel), layout.mask(1 << bit))

    def step(k):
        def run():
            if k < len(items):
                ready, own, _ = items[k]
                ready()
                spread(k, 0, own)
            if k >= lag:
                i = k - lag
                for rel in range(2, layout.reps, 2):
                    made[i][rel].wait_recv()
                    spread(i, rel, items[i][2](rel))

        return run

    def end():
        for copies in made:
            for rel in range(1, layout.reps, 2):
                copies[rel].wait_recv()

    return [step(k) for k in range(len(items) + lag)], end


def scatter_stream(links, items, window, lag):
    layout = links.layout
    made = [{} for _ in items]
    loads = [None for _ in items]
    stay = range(0, layout.reps, 2)

    def begin(i):
        part, keep, taken, _, paired = items[i]
        loads[i] = [links.local(part(rel), keep(rel // 2)) for rel in stay]
        for rel in range(layout.reps - 1, 0, -2):
            if not paired:
                made[i][rel] = links.send(part(rel), taken(rel - 1), layout.mask(rel))

    def total(i, rel):
        _, keep, taken, _, paired = items[i]
        sources = [source for source in layout.sources(rel) if not (paired and source & 1)]
        for source in sources:
            made[i][source].wait_recv()
        value = keep(rel // 2)[...].astype(F32)
        for source in sources:
            value = value + taken(source - 1)[...].astype(F32)
        return value

    def pass_on(i):
        _, keep, taken, _, paired = items[i]
        for load in loads[i]:
            load.wait()
        for rel in stay[:0:-1]:
            if not (paired and layout.low(rel) == 1):
                keep(rel // 2)[...] = total(i, rel).astype(BF)
            made[i][rel] = links.send(keep(rel // 2), taken(rel - 1), layout.mask(rel))

    def step(k):
        def run():
            if k < len(items):
                begin(k)
            if window <= k < len(items) + window:
                pass_on(k - window)
            if k >= window + lag:
                items[k - window - lag][3](total(k - window - lag, 0))

        return run

    return [step(k) for k in range(len(items) + window + lag)]


def pair_stream(links, items, window):
    layout = links.layout
    made = [{} for _ in items]

    def begin(i):
        part, keep, taken, _ = items[i]
        for k in range(layout.reps // 2):
            made[i][k] = (
                links.local(part(2 * k), keep(k)),
                links.send(part(2 * k + 1), taken(k), layout.mask(1)),
            )

    def end(i):
        _, keep, taken, finish = items[i]
        for k, (load, copy) in made[i].items():
            load.wait()
            copy.wait_recv()
            finish(k, keep(k)[...].astype(F32) + taken(k)[...].astype(F32))

    def step(k):
        def run():
            if k < len(items):
                begin(k)
            if k >= window:
                end(k - window)

        return run

    return [step(k) for k in range(len(items) + window)]


def both(first, second):
    def run():
        first()
        second()

    return run


def interleave(stream, acts, first=1):
    acts = list(acts)
    for k, step in enumerate(stream):
        step()
        if k >= first and acts:
            acts.pop(0)()
    for act in acts:
        act()


def semaphores(copies, local_copies):
    return [
        pltpu.SemaphoreType.DMA((copies,)),
        pltpu.SemaphoreType.DMA((copies,)),
        pltpu.SemaphoreType.DMA((local_copies,)),
    ]


VMEM = pl.BlockSpec(memory_space=pltpu.VMEM)
HBM = pl.BlockSpec(memory_space=pl.ANY)


def kernel_params(call_id):
    return pltpu.CompilerParams(collective_id=call_id, has_side_effects=True)


def opening_kernel(
    layout, small, tokens, cot, query_w, key_w, value_w, gate_w, gate_src, up_src, out_src,
    small_all, x_all, cot_all, attn_w, gate_in, up_in, out_w,
    small_buf, gain_buf, normed_buf, attn_own, out_own, gate_own, up_own, send_sems, recv_sems, local_sems,
):
    links = Links(layout, send_sems, recv_sems, local_sems)
    device = links.device
    place, rep = layout.place(device), layout.rep(device)
    _, half, width = tokens.shape
    shard = layout.shard

    def place_at(mask):
        return layout.place(flip_device(device, mask)) if mask else place

    edges, columns = 0, []
    for weight in (query_w, key_w, value_w, gate_w):
        size = weight.shape[1] // HEADS
        columns.append((weight, size, edges))
        edges += size

    def column(weight, size, where):
        return weight.at[:, pl.ds(pl.multiple_of(where * size, LANES), size)]

    mine = links.local(small, small_buf.at[pl.ds(device, 1)])
    own_loads = [
        links.local(column(weight, size, place), attn_own.at[:, pl.ds(at, size)])
        for weight, size, at in columns
    ]
    out_load = links.local(out_src, out_own)
    gate_load = links.local(gate_src.at[place], gate_own)
    up_load = links.local(up_src.at[place], up_own)
    links.greet(layout.masks)
    mine.wait()

    def small_step(b):
        size = 1 << b
        part = small_buf.at[pl.ds((device // size) * size, size)]
        return links.send(part, part, size)

    attn_in, later_in = {}, []

    def attn_exchange(mask):
        attn_in[mask] = [
            links.send(
                column(weight, size, place_at(mask)),
                attn_w.at[rep, place, :, pl.ds(at, size)],
                mask,
            )
            for weight, size, at in columns
        ]

    def hidden_exchange(mask):
        for source, target in ((gate_src, gate_in), (up_src, up_in)):
            later_in.append(links.send(source.at[place_at(mask)], target.at[place], mask))

    small_copy = small_step(0)
    for mask in layout.team[:3]:
        attn_exchange(mask)
    for load in own_loads:
        load.wait()
    keeps = [links.local(attn_own, attn_w.at[rep, place])]

    def attn_item(mask):
        at = place_at(mask)

        def ready():
            for copy in attn_in.get(mask, ()):
                copy.wait_recv()

        own = attn_w.at[rep, at] if mask else attn_own
        return ready, own, lambda rel: attn_w.at[xor_index(rel, rep, layout.reps), at]

    def row_item(own, target, part):
        return (
            lambda: None,
            own.at[part],
            lambda rel: target(xor_index(rel, rep, layout.reps)).at[part],
        )

    def out_slot(owner):
        return out_w.at[layout.head_part(owner)]

    items = [attn_item(0)] + [row_item(out_own, out_slot, part) for part in range(4)]
    items += [attn_item(mask) for mask in layout.team]
    out_load.wait()
    keeps.append(links.local(out_own, out_slot(rep)))
    steps, stream_end = gather_stream(links, items, 3)
    steps[0]()
    for b in range(1, layout.bits):
        small_copy.wait_recv()
        small_copy = small_step(b)
        if b < 5:
            attn_exchange(layout.team[2 + b])
        if b == 2:
            steps[1]()
    steps[2]()
    small_copy.wait_recv()
    keeps.append(links.local(small_buf, small_all))

    per = LANES // shard
    for k in range(width // LANES):
        rows = small_buf[k * per].astype(F32)
        for i in range(1, per):
            rows = rows + small_buf[k * per + i].astype(F32)
        gain_buf[:, k * LANES : (k + 1) * LANES] = rows
    gain, shift = gain_buf[0:1, :], gain_buf[1:2, :]
    pieces = layout.pieces(width)

    def norm_rows(i, carry):
        part = i // (half // TILE)
        at = pl.ds(pl.multiple_of((i % (half // TILE)) * TILE, TILE), TILE)
        normed = layer_norm(tokens[part, at, :].astype(F32), gain, shift)
        normed_buf[part, at, :] = to_weight_order(normed, pieces).astype(BF)
        return carry

    lax.fori_loop(0, 2 * half // TILE, norm_rows, 0)
    keeps.append(links.local(normed_buf, x_all.at[pl.ds(0, 2)]))
    keeps.append(links.local(cot, cot_all.at[pl.ds(0, 2)]))
    for own, target, load in ((gate_own, gate_in, gate_load), (up_own, up_in, up_load)):
        load.wait()
        keeps.append(links.local(own, target.at[place]))

    def exchange_some(masks):
        return lambda: [hidden_exchange(mask) for mask in masks]

    x_steps = gather_steps_light(links, normed_buf, x_all)
    cot_steps = gather_steps_light(links, cot, cot_all)
    acts = x_steps[:1] + [lambda: None] + x_steps[1:2] + [lambda: None] + x_steps[2:]
    acts += [exchange_some(layout.team[:2]), exchange_some(layout.team[2:4])]
    acts += cot_steps[:1] + [exchange_some(layout.team[4:6])] + cot_steps[1:2]
    acts += [exchange_some(layout.team[6:])] + cot_steps[2:]
    interleave(steps[3:], acts, 0)
    stream_end()
    for copy in later_in:
        copy.wait_recv()
    for copy in keeps:
        copy.wait()
    links.finish()


def opening_call(layout, small, tokens, cot, attn_weights, gate_src, up_src, out_src):
    reps, shard = layout.reps, layout.shard
    rows, width = tokens.shape
    half = rows // 2
    attn_cols = sum(w.shape[1] for w in attn_weights) // HEADS
    ff_cols = gate_src.shape[2]
    out_shape = (4, out_src.shape[0] // 4, out_src.shape[1])
    copies = 7 * 4 + 7 * 2 + 12 * (reps - 1) + 2 * GATHER_COPIES + layout.bits
    return pl.pallas_call(
        functools.partial(opening_kernel, layout),
        out_shape=(
            jax.ShapeDtypeStruct((layout.count, 8, LANES), BF),
            jax.ShapeDtypeStruct((16, half, width), BF),
            jax.ShapeDtypeStruct((16, half, width), BF),
            jax.ShapeDtypeStruct((reps, 8, shard, attn_cols), BF),
            jax.ShapeDtypeStruct((8, shard, ff_cols), BF),
            jax.ShapeDtypeStruct((8, shard, ff_cols), BF),
            jax.ShapeDtypeStruct((reps,) + out_shape, BF),
        ),
        in_specs=[HBM, VMEM] + [HBM] * 8,
        out_specs=(HBM,) * 7,
        scratch_shapes=[
            pltpu.VMEM((layout.count, 8, LANES), BF),
            pltpu.VMEM((8, width), F32),
            pltpu.VMEM((2, half, width), BF),
            pltpu.VMEM((shard, attn_cols), BF),
            pltpu.VMEM(out_shape, BF),
            pltpu.VMEM((shard, ff_cols), BF),
            pltpu.VMEM((shard, ff_cols), BF),
        ]
        + semaphores(copies, 18),
        compiler_params=kernel_params(0),
        name="opening",
    )(
        small, tokens.reshape(2, half, width), cot.reshape(2, half, width), *attn_weights,
        gate_src, up_src, out_src.reshape(out_shape),
    )


def turn_kernel(
    layout, parts, tokens, gains, gate_in, up_in, down_in,
    hidden, all_rows, gate_w, up_w, down_w,
    even, cores, taken, normed_buf, send_sems, recv_sems, local_sems,
):
    links = Links(layout, send_sems, recv_sems, local_sems)
    rep = layout.rep(links.device)
    _, half, width = tokens.shape
    links.greet((CORE, NEAR, layout.far) + tuple(1 << b for b in layout.rep_bits))
    keeps = [links.local(gate_in, gate_w.at[rep]), links.local(up_in, up_w.at[rep])]
    downs = []
    for i in range(layout.reps // 2):
        slot = down_w.at[xor_index(2 * i, rep, layout.reps)]
        keeps.append(links.local(down_in.at[i], slot))
        downs.append(links.send(down_in.at[i], slot, layout.mask(1)))

    def item(own, target, part):
        at = pl.ds(part * 2, 2)
        return (
            lambda: None,
            own.at[at],
            lambda rel: target.at[xor_index(rel, rep, layout.reps), at],
        )

    items = [item(gate_in, gate_w, part) for part in range(4)]
    items += [item(up_in, up_w, part) for part in range(4)]
    steps, stream_end = gather_stream(links, items, 2)
    pieces = layout.pieces(width)

    def finish(part, value):
        hidden[part] = value + tokens[part].astype(F32)

        def norm_rows(i, carry):
            at = pl.ds(pl.multiple_of(i * TILE, TILE), TILE)
            normed = layer_norm(hidden[part, at, :], gains[0:1, :], gains[1:2, :])
            normed_buf[part, at, :] = to_weight_order(normed, pieces).astype(BF)
            return carry

        lax.fori_loop(0, half // TILE, norm_rows, 0)

    acts = scatter_steps_light(links, parts, even, cores, taken, finish)
    acts.append(lambda: keeps.append(links.local(normed_buf, all_rows.at[pl.ds(0, 2)])))
    acts += gather_steps_light(links, normed_buf, all_rows)
    acts.pop(0)()
    interleave(steps, acts, 0)
    stream_end()
    for copy in downs:
        copy.wait_recv()
    for copy in keeps:
        copy.wait()
    links.finish()


def turn_call(layout, parts, tokens, gains, gate_in, up_in, down_in):
    rows, width = tokens.shape
    half = rows // 2
    block = gate_in.shape
    return pl.pallas_call(
        functools.partial(turn_kernel, layout),
        out_shape=(
            jax.ShapeDtypeStruct((2, half, width), F32),
            jax.ShapeDtypeStruct((16, half, width), BF),
            jax.ShapeDtypeStruct((layout.reps,) + block, BF),
            jax.ShapeDtypeStruct((layout.reps,) + block, BF),
            jax.ShapeDtypeStruct((layout.reps,) + down_in.shape[1:], BF),
        ),
        in_specs=[HBM, VMEM, VMEM, VMEM, VMEM, VMEM],
        out_specs=(VMEM, HBM, HBM, HBM, HBM),
        scratch_shapes=scatter_scratch(half, width)
        + [pltpu.VMEM((2, half, width), BF)]
        + semaphores(
            8 * (layout.reps - 1) + layout.reps // 2 + SCATTER_COPIES + GATHER_COPIES,
            5 + layout.reps // 2,
        ),
        compiler_params=kernel_params(1),
        name="turn",
    )(parts.reshape(16, half, width), tokens.reshape(2, half, width), gains, gate_in, up_in, down_in)


def turn_back_kernel(
    layout, parts, hidden, out_grad, gains, down_p, hidden_p,
    hidden_grad, all_rows, vectors, down_sum, gate_sum, up_first, up_rest,
    even, cores, taken, low_buf, sum_buf, down_l, down_y, gate_l, gate_y, up_l, up_y,
    send_sems, recv_sems, local_sems,
):
    links = Links(layout, send_sems, recv_sems, local_sems)
    rep = layout.rep(links.device)
    _, half, width = hidden.shape
    links.greet((CORE, NEAR, layout.far) + tuple(1 << b for b in layout.rep_bits))

    columns = gate_sum.shape[2]

    def item(part, keep, taken, at, first, rest):
        def finish(k, value):
            if k:
                rest[k - 1, at] = value.astype(rest.dtype)
            else:
                first[at] = value.astype(first.dtype)

        return (
            lambda rel: part.at[xor_index(rel, rep, layout.reps), at, :, pl.ds(columns, columns)],
            lambda k: keep.at[k, at],
            lambda k: taken.at[k, at],
            finish,
        )

    pairs = [pl.ds(2 * part, 2) for part in range(4)]
    items = replica_items(layout, rep, down_p, down_l, down_y, range(4), down_sum)
    gates = replica_items(layout, rep, hidden_p, gate_l, gate_y, pairs, gate_sum)
    items += [
        ((lambda rel, part=g[0]: part(rel).at[:, :, pl.ds(0, columns)]),) + g[1:] for g in gates
    ]
    steps = scatter_stream(links, items, 2, 2)
    late = pair_stream(links, [item(hidden_p, up_l, up_y, at, up_first, up_rest) for at in pairs], 2)
    for k, more in enumerate(late):
        steps[min(k + 5, 11)] = both(steps[min(k + 5, 11)], more)
    pieces = layout.pieces(width)
    vectors[...] = jnp.zeros_like(vectors)

    def finish(part, value):
        sum_buf[...] = value

        def rows(i, carry):
            at = pl.ds(pl.multiple_of(i * TILE, TILE), TILE)
            grads = from_weight_order(sum_buf[at, :], pieces)
            back, gain_part, shift_part = layer_norm_back(
                hidden[part, at, :], gains[0:1, :], grads
            )
            total = out_grad[part, at, :].astype(F32) + back
            hidden_grad[part, at, :] = total
            low_buf[part, at, :] = total.astype(BF)
            vectors[0:1, :] += gain_part
            vectors[1:2, :] += shift_part
            return carry

        lax.fori_loop(0, half // TILE, rows, 0)

    keeps = []
    acts = scatter_steps(links, parts, even, cores, taken, finish)
    acts.append(lambda: keeps.append(links.local(low_buf, all_rows.at[pl.ds(0, 2)])))
    acts += gather_steps(links, low_buf, all_rows)
    acts.pop(0)()
    interleave(steps, acts, 0)
    for copy in keeps:
        copy.wait()
    links.finish()


def replica_items(layout, rep, part, keep, taken, places, sums, paired=False):
    def item(at):
        def finish(value):
            sums[at] = value.astype(sums.dtype)

        return (
            lambda rel: part.at[rel // 2 if paired else xor_index(rel, rep, layout.reps), at],
            lambda i: keep.at[i, at],
            lambda i: taken.at[i, at],
            finish,
            paired,
        )

    return [item(at) for at in places]


def turn_back_call(layout, parts, hidden, out_grad, gains, down_p, hidden_p):
    half, width = hidden.shape[1:]
    reps = layout.reps
    down_block = down_p.shape[1:]
    gate_block = hidden_p.shape[1:3] + (hidden_p.shape[3] // 2,)
    return pl.pallas_call(
        functools.partial(turn_back_kernel, layout),
        out_shape=(
            jax.ShapeDtypeStruct((2, half, width), F32),
            jax.ShapeDtypeStruct((16, half, width), BF),
            jax.ShapeDtypeStruct((8, width), F32),
            jax.ShapeDtypeStruct(down_block, F32),
            jax.ShapeDtypeStruct(gate_block, BF),
            jax.ShapeDtypeStruct(gate_block, F32),
            jax.ShapeDtypeStruct((reps // 2 - 1,) + gate_block, BF),
        ),
        in_specs=[HBM, VMEM, VMEM, VMEM, HBM, HBM],
        out_specs=(VMEM, HBM, VMEM, VMEM, VMEM, VMEM, VMEM),
        scratch_shapes=scatter_scratch(half, width)
        + [
            pltpu.VMEM((2, half, width), BF),
            pltpu.VMEM((half, width), F32),
            pltpu.VMEM((reps // 2,) + down_block, BF),
            pltpu.VMEM((reps - 1,) + down_block, BF),
            pltpu.VMEM((reps // 2,) + gate_block, BF),
            pltpu.VMEM((reps - 1,) + gate_block, BF),
            pltpu.VMEM((reps // 2,) + gate_block, BF),
            pltpu.VMEM((reps // 2,) + gate_block, BF),
        ]
        + semaphores(
            8 * (reps - 1) + 2 * reps + SCATTER_COPIES + GATHER_COPIES, 4 * reps + 2 * reps + 2
        ),
        compiler_params=kernel_params(2),
        name="turn_back",
    )(
        parts.reshape(16, half, width), hidden, out_grad.reshape(2, half, width), gains,
        down_p, hidden_p,
    )


def closing_kernel(
    layout, attn_p, out_q, gate_sum, up_sum, one_parts, two_parts, tokens, hidden_grad, gains, vectors,
    query_back, key_back, value_back, swish_back, gate_back, up_back, out_sum, branch_two,
    tokens_grad, vector_sum,
    even_1, cores_1, taken_1, even_2, cores_2, taken_2, sum_buf, rows_buf, vec_l, vec_y,
    attn_l, attn_y, attn_s, out_l, out_y, send_sems, recv_sems, local_sems,
):
    links = Links(layout, send_sems, recv_sems, local_sems)
    device = links.device
    place, rep = layout.place(device), layout.rep(device)
    _, half, width = tokens.shape
    links.greet(layout.masks)
    backs, kept = [], []

    def place_at(mask):
        return layout.place(flip_device(device, mask)) if mask else place

    def give(source, target, mask):
        if mask:
            backs.append(links.send(source, target, mask))
        else:
            kept.append(links.local(source, target))

    edges, columns = 0, []
    for target in (query_back, key_back, value_back, swish_back):
        size = target.shape[1] // HEADS
        columns.append((target, size, edges))
        edges += size

    def with_return(item, mask, give_back):
        part, keep, taken, finish, paired = item

        def finish_and_give(value):
            finish(value)
            give_back(mask)

        return part, keep, taken, finish_and_give, paired

    def attn_return(mask):
        for target, size, at in columns:
            goal = pl.ds(pl.multiple_of(place * size, LANES), size)
            give(attn_s.at[place_at(mask), :, pl.ds(at, size)], target.at[:, goal], mask)

    order = layout.team[::-1] + (0,)
    items = replica_items(layout, rep, out_q, out_l, out_y, range(4), out_sum, True)
    places = [place_at(m) for m in order]
    plain = replica_items(layout, rep, attn_p, attn_l, attn_y, places, attn_s)
    items += [with_return(item, m, attn_return) for item, m in zip(plain, order)]
    steps = scatter_stream(links, items, 2, 2)

    pieces = layout.pieces(width)
    rows_buf[...] = jnp.zeros_like(rows_buf)
    rows_buf[2:4, :] = vectors[0:2, :]

    def finish_one(part, value):
        sum_buf[...] = value

        def rows(i, carry):
            at = pl.ds(pl.multiple_of(i * TILE, TILE), TILE)
            grads = from_weight_order(sum_buf[at, :], pieces)
            back, gain_part, shift_part = layer_norm_back(
                tokens[part, at, :].astype(F32), gains[0:1, :], grads
            )
            tokens_grad[part, at, :] = hidden_grad[part, at, :] + back
            rows_buf[0:1, :] += gain_part
            rows_buf[1:2, :] += shift_part
            return carry

        lax.fori_loop(0, half // TILE, rows, 0)

    def finish_two(part, value):
        branch_two[part] = value

    per = LANES // layout.shard
    own_bits = per.bit_length() - 1
    slots = layout.count // per
    flight = {}

    def vector_begin():
        for slot in range(slots):
            vec_l[slot] = rows_buf[:, slot * LANES : (slot + 1) * LANES]

    def vector_send(b):
        def run():
            peer = flip_device(device, 1 << b)
            if b >= own_bits:
                size = 1 << (b - own_bits)
                source = vec_l.at[pl.ds((peer // (1 << b)) * size, size)]
                target = vec_y.at[pl.ds(size, size)]
            else:
                source = vec_l.at[pl.ds(device // per, 1)]
                target = vec_y.at[pl.ds(slots + b, 1)]
            flight[b] = links.send(source, target, 1 << b)

        return run

    def vector_add(b):
        def run():
            if b >= own_bits:
                size = 1 << (b - own_bits)
                flight[b].wait_recv()
                mine = pl.ds((device // (1 << b)) * size, size)
                vec_l[mine] = vec_l[mine] + vec_y[size : 2 * size]
            else:
                links.swap_done(flight[b])
                mine = pl.ds(device // per, 1)
                vec_l[mine] = vec_l[mine] + vec_y[slots + b : slots + b + 1]

        return run

    def gate_return():
        for mask in layout.team + (0,):
            give(gate_sum.at[place_at(mask)], gate_back.at[place], mask)
            give(up_sum.at[place_at(mask)], up_back.at[place], mask)

    one = scatter_steps_light(links, one_parts, even_1, cores_1, taken_1, finish_one)
    two = scatter_steps_light(links, two_parts, even_2, cores_2, taken_2, finish_two)
    acts = one[1:] + [vector_begin]
    down_bits = list(range(layout.bits))[::-1]
    together = [(lambda b=b, a=a: ((a() if a else None), vector_send(b)())) for a, b in zip(
        [None] + [vector_add(b) for b in down_bits[:-1]], down_bits)]
    acts += [lambda: (together[0](), two[0](), gate_return())]
    for k in range(1, layout.bits):
        extra = two[k] if k < len(two) else (lambda: None)
        acts.append(lambda k=k, extra=extra: (together[k](), extra()))
    acts += two[layout.bits :] + [vector_add(down_bits[-1])]
    one[0]()
    interleave(steps, acts, 0)
    vector_sum[...] = vec_l[device // per]
    for copy in backs:
        copy.wait_recv()
    for copy in kept:
        copy.wait()
    links.finish()


def closing_call(layout, attn_p, out_q, gate_sum, up_sum, one_parts, two_parts, tokens, hidden_grad,
                 gains, vectors, back_widths):
    reps, shard = layout.reps, layout.shard
    half, width = hidden_grad.shape[1:]
    attn_block, up_block, out_block = attn_p.shape[1:], up_sum.shape, out_q.shape[1:]
    per = LANES // shard
    slots = layout.count // per
    stay = reps // 2
    rows = jax.ShapeDtypeStruct((2, half, width), F32)
    copies = 20 * (reps - 1) + 7 * 6 + 2 * SCATTER_COPIES + layout.bits
    return pl.pallas_call(
        functools.partial(closing_kernel, layout),
        out_shape=tuple(jax.ShapeDtypeStruct((shard, w), BF) for w in back_widths)
        + (
            jax.ShapeDtypeStruct(up_block, BF),
            jax.ShapeDtypeStruct(up_block, BF),
            jax.ShapeDtypeStruct(out_block, F32),
            rows,
            rows,
            jax.ShapeDtypeStruct((8, LANES), F32),
        ),
        in_specs=[HBM, HBM, VMEM, VMEM, HBM, HBM, VMEM, VMEM, VMEM, VMEM],
        out_specs=(HBM,) * 6 + (VMEM,) * 4,
        scratch_shapes=scatter_scratch(half, width)
        + scatter_scratch(half, width)
        + [
            pltpu.VMEM((half, width), F32),
            pltpu.VMEM((8, width), F32),
            pltpu.VMEM((slots, 8, LANES), F32),
            pltpu.VMEM((slots + per, 8, LANES), F32),
            pltpu.VMEM((stay,) + attn_block, BF),
            pltpu.VMEM((reps - 1,) + attn_block, BF),
            pltpu.VMEM(attn_block, BF),
            pltpu.VMEM((stay,) + out_block, BF),
            pltpu.VMEM((reps - 1,) + out_block, BF),
        ]
        + semaphores(copies, 20 * stay + 8),
        compiler_params=kernel_params(3),
        name="closing",
    )(
        attn_p, out_q, gate_sum, up_sum, one_parts.reshape(16, half, width),
        two_parts.reshape(16, half, width), tokens.reshape(2, half, width), hidden_grad, gains, vectors,
    )


def seq_layout(seq_lens, row_count):
    row_ids = jnp.arange(row_count, dtype=jnp.int32)
    seq_ends = jnp.cumsum(seq_lens)
    passed = row_ids[:, None] >= seq_ends[None, :]
    segment = jnp.sum(passed.astype(jnp.int32), axis=1)
    seq_start = jnp.sum(jnp.where(passed, seq_lens[None, :], 0), axis=1)
    position = row_ids - seq_start
    live_rows = row_ids < seq_ends[-1]
    return (segment, position, live_rows)


def group_norm(values):
    center = values - jnp.mean(values, axis=-1, keepdims=True)
    spread = jnp.mean(center * center, axis=-1, keepdims=True)
    return center * lax.rsqrt(spread + GROUP_EPS)


def dot(left, right):
    return jnp.dot(left, right, preferred_element_type=F32)


def dot_nt(left, right):
    return lax.dot_general(left, right, (((1,), (1,)), ((), ())), preferred_element_type=F32)


def dot_tn(left, right):
    return lax.dot_general(left, right, (((0,), (0,)), ((), ())), preferred_element_type=F32)


def make_body(count):
    def on_device(
        tokens,
        seq_lengths,
        attn_gain,
        attn_shift,
        query_weight,
        key_weight,
        value_weight,
        gate_weight,
        out_weight,
        mlp_gain,
        mlp_shift,
        mlp_gate,
        mlp_up,
        mlp_down,
        cotangent,
    ):
        local_rows, width = tokens.shape
        shard = width // count
        layout = Layout(count, shard)
        reps = layout.reps
        device = lax.axis_index("dp")
        rep, pos_t = layout.rep(device), layout.place(device)
        micro_count, seq_slots = seq_lengths.shape[1:]
        row_count = local_rows // micro_count
        key_size = query_weight.shape[1] // HEADS
        value_size = value_weight.shape[1] // HEADS
        hidden_size = mlp_gate.shape[1]
        ff_block = hidden_size // count
        group_rows = 8 * local_rows
        home = [layout.device(layout.head_rep(d % reps), d // reps) for d in range(count)]
        head_perm = [(d, home[d]) for d in range(count)]
        head_back = [(b, a) for a, b in head_perm]

        high, mid = 1 << (layout.bits - 1 - layout.far_bit), 1 << (layout.far_bit - 2)

        def ff_first(weight):
            v = weight.reshape(shard, high, 2, mid, 4, ff_block)
            return v.transpose(2, 4, 0, 1, 3, 5).reshape(8, shard, reps * ff_block)

        def ff_back(grad):
            v = grad.reshape(2, 4, shard, high, mid, ff_block)
            return v.transpose(2, 3, 0, 4, 1, 5).reshape(shard, hidden_size)

        per = LANES // shard
        lane_on = jnp.arange(LANES, dtype=jnp.int32) // shard == device % per

        def in_lanes(values):
            return jnp.where(lane_on, jnp.tile(values, per), jnp.zeros((), BF))[None]

        own_lens = seq_lengths.reshape(-1).astype(BF)
        small = jnp.concatenate(
            [in_lanes(v) for v in (attn_gain, attn_shift, mlp_gain, mlp_shift)]
            + [jnp.pad(own_lens, (0, LANES - own_lens.shape[0]))[None], jnp.zeros((3, LANES), BF)]
        )
        own_live = jax.vmap(lambda v: seq_layout(v, row_count)[2])(seq_lengths[0])
        own_live = own_live.reshape(local_rows).astype(F32)[:, None]
        out_grad_low = (cotangent.astype(F32) * own_live).astype(BF)

        out_own = lax.ppermute(out_weight, "dp", head_perm)
        small, normed_one, cot_all, attn_w, gate_in, up_in, out_w = opening_call(
            layout, small[None], tokens, out_grad_low,
            (query_weight, key_weight, value_weight, gate_weight),
            ff_first(mlp_gate), ff_first(mlp_up), out_own,
        )
        normed_one = normed_one.reshape(group_rows, width)
        cot_all = cot_all.reshape(group_rows, width)
        attn_w = attn_w.reshape(width, -1)
        out_w = out_w.reshape(-1, width)

        def flip_rep(values, bit):
            mask = 1 << layout.rep_bits[bit]
            return lax.ppermute(values, "dp", [(d, d ^ mask) for d in range(count)])

        down_even = [lax.optimization_barrier((mlp_down, small))[0]]
        for k in range(1, reps // 2):
            low = layout.low(k)
            down_even.append(flip_rep(down_even[k & ~(1 << low)], low + 1))

        def pair_sums(parts):
            sums = []
            for rel in range(0, reps, 2):
                other = lax.dynamic_index_in_dim(
                    parts, layout.head_part(rep ^ (rel + 1)), 0, keepdims=False
                )
                own = lax.dynamic_index_in_dim(parts, layout.head_part(rep ^ rel), 0, keepdims=False)
                sums.append((own.astype(F32) + flip_rep(other, 0).astype(F32)).astype(BF))
            return jnp.stack(sums)

        def finish_pairs(first, rest):
            sums = [first] + [rest[k] for k in range(reps // 2 - 1)]
            for k in range(reps // 2 - 1, 0, -1):
                low = layout.low(k)
                got = flip_rep(sums[k].astype(BF), low + 1).astype(F32)
                sums[k & ~(1 << low)] = sums[k & ~(1 << low)].astype(F32) + got
            return sums[0]

        vecs = small[:, :4, :].astype(F32).reshape(-1, per, 4, LANES).sum(1)
        vecs = vecs.transpose(1, 0, 2).reshape(4, width)
        gains_one = jnp.pad(vecs[:2], ((0, 6), (0, 0)))
        gains_two = jnp.pad(vecs[2:], ((0, 6), (0, 0)))
        lens = small[:, 4, : own_lens.shape[0]].astype(jnp.int32)
        order = [c + 2 * n + 4 * f for c in range(2) for f in range(2) for n in range(2)]
        members = jnp.stack(
            [flip_device(device, (j & 3) + (j >> 2) * layout.far) for j in order]
        )
        lens = jnp.take(lens, members, axis=0).reshape(8 * micro_count, seq_slots)

        segment, position, live = jax.vmap(lambda s: seq_layout(s, row_count))(lens)
        head_log = jnp.log(1.0 - 2.0 ** (-5.0 - jnp.arange(HEADS, dtype=F32)))
        head_log = lax.dynamic_index_in_dim(head_log, pos_t, 0, keepdims=False)
        ids = jnp.arange(row_count, dtype=jnp.int32)
        same_seq = (
            (segment[:, :, None] == segment[:, None, :])
            & live[:, :, None]
            & live[:, None, :]
            & (ids[:, None] >= ids[None, :])[None]
        )
        distance = jnp.maximum(position[:, :, None] - position[:, None, :], 0).astype(F32)
        decay = jnp.where(same_seq, jnp.exp(distance * head_log), 0.0)
        half_size = key_size // 2
        pair_index = jnp.arange(half_size, dtype=F32)
        frequency = 10000.0 ** (-pair_index / half_size)
        row_place = position.reshape(-1).astype(F32)[:, None]
        angles = row_place * frequency[None, :]
        growth = (pair_index * 2.0 / key_size + 0.4) / 1.4
        stretch = growth[None, :] ** (row_place / 512.0)
        key_factor = key_size ** (-0.5) / stretch
        cosine, sine, stretch, key_factor = lax.optimization_barrier(
            (jnp.cos(angles), jnp.sin(angles), stretch, key_factor)
        )

        def rotate(values, factor):
            a, b = values[:, :half_size], values[:, half_size:]
            return jnp.concatenate(
                [(a * cosine - b * sine) * factor, (b * cosine + a * sine) * factor], axis=1
            )

        def rotate_back(grads, factor):
            a, b = grads[:, :half_size] * factor, grads[:, half_size:] * factor
            return jnp.concatenate([a * cosine + b * sine, b * cosine - a * sine], axis=1)

        def micro(values):
            return values.reshape(-1, row_count, values.shape[-1])

        qkvg = dot(normed_one, attn_w)
        query_raw = qkvg[:, :key_size]
        key_raw = qkvg[:, key_size : 2 * key_size]
        value_low = qkvg[:, 2 * key_size : 2 * key_size + value_size].astype(BF)
        gate_raw = qkvg[:, 2 * key_size + value_size :]
        query_turned = micro(rotate(query_raw, stretch).astype(BF))
        key_turned = micro(rotate(key_raw, key_factor).astype(BF))
        value_m = micro(value_low)
        scores = jnp.einsum("mqd,mkd->mqk", query_turned, key_turned, preferred_element_type=F32)
        weights_low = (scores * decay).astype(BF)
        retained = jnp.einsum("mqk,mke->mqe", weights_low, value_m, preferred_element_type=F32)
        retained = retained.reshape(group_rows, value_size)

        def mix(gate_in, retained_in):
            return jax.nn.silu(gate_in) * group_norm(retained_in)

        mixed = mix(gate_raw, retained).astype(BF)
        hidden, normed_two, gate_w, up_w, down_w = turn_call(
            layout, dot(mixed, out_w).astype(BF), tokens, gains_two, gate_in, up_in,
            jnp.stack(down_even),
        )
        down_w = down_w.reshape(-1, width)
        normed_two = normed_two.reshape(group_rows, width)
        gate_w, up_w = gate_w.reshape(width, -1), up_w.reshape(width, -1)

        def act(gate_in, up_in):
            return jax.nn.gelu(gate_in, approximate=True) * up_in

        product, pull_act = jax.vjp(act, dot(normed_two, gate_w), dot(normed_two, up_w))
        product = product.astype(BF)
        gate_low, up_low = (g.astype(BF) for g in pull_act(dot_nt(cot_all, down_w)))
        two_parts = dot(product, down_w).astype(BF)
        down_parts = dot_tn(product, cot_all).astype(BF)
        hidden_parts = dot_tn(normed_two, jnp.concatenate([gate_low, up_low], axis=1)).astype(BF)
        normed_parts = (dot_nt(gate_low, gate_w) + dot_nt(up_low, up_w)).astype(BF)
        hidden_grad, branch_one_grad, vectors, mlp_down_grad, gate_sum, up_first, up_rest = turn_back_call(
            layout, normed_parts, hidden, out_grad_low, gains_two,
            down_parts.reshape(reps, 4, -1, width), hidden_parts.reshape(reps, 8, shard, -1),
        )
        branch_one_grad = branch_one_grad.reshape(group_rows, width)
        up_sum = finish_pairs(up_first, up_rest).astype(BF)

        mixed_grad = dot_nt(branch_one_grad, out_w)
        out_parts = dot_tn(mixed, branch_one_grad).astype(BF)
        out_pairs = pair_sums(out_parts.reshape(reps, 4, -1, width))
        _, pull_mix = jax.vjp(mix, gate_raw, retained)
        gate_grad, retained_grad = pull_mix(mixed_grad)
        gate_grad = gate_grad.astype(BF)
        retained_low = micro(retained_grad.astype(BF))
        weights_grad = jnp.einsum("mqe,mke->mqk", retained_low, value_m, preferred_element_type=F32)
        value_grad = jnp.einsum(
            "mqk,mqe->mke", weights_low, retained_low, preferred_element_type=F32
        )
        value_grad = value_grad.reshape(group_rows, value_size).astype(BF)
        score_low = (weights_grad * decay).astype(BF)
        query_turn_grad = jnp.einsum("mqk,mkd->mqd", score_low, key_turned, preferred_element_type=F32)
        key_turn_grad = jnp.einsum("mqk,mqd->mkd", score_low, query_turned, preferred_element_type=F32)
        query_grad = rotate_back(query_turn_grad.reshape(group_rows, key_size), stretch).astype(BF)
        key_grad = rotate_back(key_turn_grad.reshape(group_rows, key_size), key_factor).astype(BF)
        attn_grads = jnp.concatenate([query_grad, key_grad, value_grad, gate_grad], axis=1)
        attn_parts = dot_tn(normed_one, attn_grads).astype(BF)
        one_parts = dot_nt(attn_grads, attn_w).astype(BF)
        q_back, k_back, v_back, g_back, gate_back, up_back, out_sum, branch_two, tokens_grad, vectors = (
            closing_call(
                layout,
                attn_parts.reshape(reps, 8, shard, -1),
                out_pairs, gate_sum, up_sum, one_parts, two_parts, tokens, hidden_grad, gains_one, vectors,
                [w.shape[1] for w in (query_weight, key_weight, value_weight, gate_weight)],
            )
        )
        out_sum = out_sum.reshape(out_weight.shape).astype(BF)
        out_weight_grad = lax.ppermute(out_sum, "dp", head_back).astype(F32)
        output = ((hidden + branch_two).reshape(local_rows, width) * own_live).astype(BF)
        vectors = lax.dynamic_slice_in_dim(vectors, (device % per) * shard, shard, axis=1)
        return (
            output,
            tokens_grad.reshape(local_rows, width),
            vectors[0],
            vectors[1],
            q_back.astype(F32),
            k_back.astype(F32),
            v_back.astype(F32),
            g_back.astype(F32),
            out_weight_grad,
            vectors[2],
            vectors[3],
            ff_back(gate_back.astype(F32)),
            ff_back(up_back.astype(F32)),
            mlp_down_grad.reshape(mlp_down.shape),
        )

    return on_device


def solution(mesh):
    rows = P("dp", None)
    vec = P("dp")
    placed = (
        rows, P("dp", None, None), vec, vec, rows, rows, rows, rows, rows,
        vec, vec, rows, rows, rows, rows,
    )
    outs = (rows, rows, vec, vec, rows, rows, rows, rows, rows, vec, vec, rows, rows, rows)
    return jax.shard_map(
        make_body(mesh.shape["dp"]), mesh=mesh, in_specs=placed, out_specs=outs, check_vma=False
    )
```
